8 devices in a mesh: stage: 8 (over z, y, x, core).
Axes of the slice: x: 2, y: 2, z: 1, core: 2. Of those that a mesh axis runs over, the one named last changes fastest.
Arguments:
- tokens: bfloat16 [8, 1024, 512], P('stage')
- seq_lens: int32 [8], P('stage')
- cotangent: bfloat16 [8, 1024, 512], P('stage')
- w_qkv: bfloat16 [8, 512, 1536], P('stage')
- w_out: bfloat16 [8, 512, 512], P('stage')
- w_up: bfloat16 [8, 512, 2048], P('stage')
- w_down: bfloat16 [8, 2048, 512], P('stage')
- gain_attn: bfloat16 [8, 512], P('stage')
- gain_mlp: bfloat16 [8, 512], P('stage')
Outputs:
- output 1: bfloat16 [8, 1024, 512], P('stage')
- output 2: float32 [8, 512, 1536], P('stage')
- output 3: float32 [8, 512, 512], P('stage')
- output 4: float32 [8, 512, 2048], P('stage')
- output 5: float32 [8, 2048, 512], P('stage')
- output 6: float32 [8, 512], P('stage')
- output 7: float32 [8, 512], P('stage')
All inputs are finite; a program needn't handle non-finite values.
Results may differ from the reference program's by a relative error of at most 0.02.
Values are sent between devices in bfloat16 or wider.
A program may use at most 1 GiB of HBM per device.

```python
import jax
import jax.numpy as jnp
from jax import lax

STAGES = 8
MICRO_BATCHES = 1
SEQ_LEN = 1024
D_MODEL = 512
N_HEADS = 8
HEAD_DIM = D_MODEL // N_HEADS
FFN_DIM = 4 * D_MODEL
EPS = 1e-5
NEG_BIG = -1e9


def draw_lengths(len_key):
    key_cap, key_len, key_top = jax.random.split(len_key, 3)
    shrink = jax.random.randint(key_cap, (STAGES, 1), 0, 4)
    cap_lens = SEQ_LEN // (2 ** shrink)
    low_lens = jnp.maximum(cap_lens // 4, 1)
    lengths = jax.random.randint(key_len, (STAGES, MICRO_BATCHES), low_lens, cap_lens + 1).reshape(-1)
    longest = jax.random.randint(key_top, (), 0, STAGES * MICRO_BATCHES)
    return jnp.where(jnp.arange(STAGES * MICRO_BATCHES) == longest, SEQ_LEN, lengths).astype(jnp.int32)


def setup_inputs(seed: int = 0) -> dict:
    key_list = jax.random.split(jax.random.key(seed), 9)
    n_rows = STAGES * MICRO_BATCHES
    act_shape = (n_rows, SEQ_LEN, D_MODEL)
    tokens = jax.random.normal(key_list[0], act_shape, jnp.float32)
    seq_lens = draw_lengths(key_list[1])
    is_valid = jnp.arange(SEQ_LEN)[None, :, None] < seq_lens[:, None, None]
    cot_scale = (n_rows * SEQ_LEN) ** -0.5
    cotangent = jnp.where(is_valid, jax.random.normal(key_list[2], act_shape, jnp.float32) * cot_scale, 0.0)
    w_qkv = jax.random.normal(key_list[3], (STAGES, D_MODEL, 3 * D_MODEL), jnp.float32) * D_MODEL ** -0.5
    w_out = jax.random.normal(key_list[4], (STAGES, D_MODEL, D_MODEL), jnp.float32) * D_MODEL ** -0.5
    w_up = jax.random.normal(key_list[5], (STAGES, D_MODEL, FFN_DIM), jnp.float32) * D_MODEL ** -0.5
    w_down = jax.random.normal(key_list[6], (STAGES, FFN_DIM, D_MODEL), jnp.float32) * FFN_DIM ** -0.5
    gain_attn = 1.0 + 0.4 * jax.random.normal(key_list[7], (STAGES, D_MODEL), jnp.float32)
    gain_mlp = 1.0 + 0.4 * jax.random.normal(key_list[8], (STAGES, D_MODEL), jnp.float32)
    return {'tokens': tokens.astype(jnp.bfloat16), 'seq_lens': seq_lens, 'cotangent': cotangent.astype(jnp.bfloat16), 'w_qkv': w_qkv.astype(jnp.bfloat16), 'w_out': w_out.astype(jnp.bfloat16), 'w_up': w_up.astype(jnp.bfloat16), 'w_down': w_down.astype(jnp.bfloat16), 'gain_attn': gain_attn.astype(jnp.bfloat16), 'gain_mlp': gain_mlp.astype(jnp.bfloat16)}


def rms_norm(hidden, gain_vec):
    hid_f32 = hidden.astype(jnp.float32)
    inv_rms = lax.rsqrt(jnp.mean(hid_f32 * hid_f32, axis=-1, keepdims=True) + EPS)
    return (hid_f32 * inv_rms * gain_vec.astype(jnp.float32)).astype(jnp.bfloat16), inv_rms


def rms_norm_bwd(hidden, inv_rms, gain_vec, d_normed):
    scaled = hidden.astype(jnp.float32) * inv_rms
    d_gain = jnp.sum(d_normed * scaled, axis=(0, 1))
    gain_dn = d_normed * gain_vec.astype(jnp.float32)
    d_hidden = inv_rms * (gain_dn - scaled * jnp.mean(gain_dn * scaled, axis=-1, keepdims=True))
    return d_hidden, d_gain


def gelu_tanh(pre_act):
    return jax.nn.gelu(pre_act, approximate=True)


def attention_weights(q_heads, k_heads, seq_lens):
    positions = jnp.arange(q_heads.shape[1])
    scores = jnp.einsum('nqhd,nkhd->nhqk', q_heads.astype(jnp.float32), k_heads.astype(jnp.float32)) * (HEAD_DIM ** -0.5)
    allowed = (positions[None, None, None, :] <= positions[None, None, :, None]) & (positions[None, None, None, :] < seq_lens[:, None, None, None])
    return jax.nn.softmax(jnp.where(allowed, scores, NEG_BIG), axis=-1)


def layer_parts(hidden, seq_lens, weights):
    w_qkv, w_out, w_up, w_down, gain_attn, gain_mlp = weights
    n_seq, seq_len, model_dim = hidden.shape
    normed1, inv_rms1 = rms_norm(hidden, gain_attn)
    qkv_proj = jnp.dot(normed1, w_qkv, preferred_element_type=jnp.float32).astype(jnp.bfloat16)
    qkv_proj = qkv_proj.reshape(n_seq, seq_len, 3, N_HEADS, HEAD_DIM)
    q_heads = qkv_proj[:, :, 0]
    k_heads = qkv_proj[:, :, 1]
    v_heads = qkv_proj[:, :, 2]
    attn_probs = attention_weights(q_heads, k_heads, seq_lens)
    probs16 = attn_probs.astype(jnp.bfloat16)
    context = jnp.einsum('nhqk,nkhd->nqhd', probs16.astype(jnp.float32), v_heads.astype(jnp.float32)).astype(jnp.bfloat16)
    context = context.reshape(n_seq, seq_len, model_dim)
    attn_out = jnp.dot(context, w_out, preferred_element_type=jnp.float32)
    mid_resid = (hidden.astype(jnp.float32) + attn_out).astype(jnp.bfloat16)
    normed2, inv_rms2 = rms_norm(mid_resid, gain_mlp)
    pre_act = jnp.dot(normed2, w_up, preferred_element_type=jnp.float32)
    act16 = gelu_tanh(pre_act).astype(jnp.bfloat16)
    mlp_out = jnp.dot(act16, w_down, preferred_element_type=jnp.float32)
    layer_out = (mid_resid.astype(jnp.float32) + mlp_out).astype(jnp.bfloat16)
    saved_acts = (normed1, inv_rms1, q_heads, k_heads, v_heads, attn_probs, probs16, context, mid_resid, normed2, inv_rms2, pre_act, act16)
    return layer_out, saved_acts


def layer_backward(hidden, seq_lens, weights, d_out):
    w_qkv, w_out, w_up, w_down, gain_attn, gain_mlp = weights
    n_seq, seq_len, model_dim = hidden.shape
    saved_acts = layer_parts(hidden, seq_lens, weights)[1]
    normed1, inv_rms1, q_heads, k_heads, v_heads, attn_probs, probs16, context, mid_resid, normed2, inv_rms2, pre_act, act16 = saved_acts
    d_out16 = d_out.astype(jnp.bfloat16)
    g_down = jnp.einsum('nsf,nsd->fd', act16.astype(jnp.float32), d_out16.astype(jnp.float32))
    d_act = jnp.einsum('nsd,fd->nsf', d_out16.astype(jnp.float32), w_down.astype(jnp.float32))
    gelu_pullback = jax.vjp(gelu_tanh, pre_act)[1]
    d_pre16 = gelu_pullback(d_act)[0].astype(jnp.bfloat16)
    g_up = jnp.einsum('nsd,nsf->df', normed2.astype(jnp.float32), d_pre16.astype(jnp.float32))
    d_normed2 = jnp.einsum('nsf,df->nsd', d_pre16.astype(jnp.float32), w_up.astype(jnp.float32))
    d_mid_norm, g_gain_mlp = rms_norm_bwd(mid_resid, inv_rms2, gain_mlp, d_normed2)
    d_mid = d_out + d_mid_norm
    d_mid16 = d_mid.astype(jnp.bfloat16)
    g_out = jnp.einsum('nsd,nse->de', context.astype(jnp.float32), d_mid16.astype(jnp.float32))
    d_context = jnp.einsum('nse,de->nsd', d_mid16.astype(jnp.float32), w_out.astype(jnp.float32)).astype(jnp.bfloat16)
    d_context = d_context.reshape(n_seq, seq_len, N_HEADS, HEAD_DIM)
    d_probs = jnp.einsum('nqhd,nkhd->nhqk', d_context.astype(jnp.float32), v_heads.astype(jnp.float32))
    d_value = jnp.einsum('nhqk,nqhd->nkhd', probs16.astype(jnp.float32), d_context.astype(jnp.float32))
    d_scores = attn_probs * (d_probs - jnp.sum(attn_probs * d_probs, axis=-1, keepdims=True))
    d_scores16 = (d_scores * (HEAD_DIM ** -0.5)).astype(jnp.bfloat16)
    d_query = jnp.einsum('nhqk,nkhd->nqhd', d_scores16.astype(jnp.float32), k_heads.astype(jnp.float32))
    d_key = jnp.einsum('nhqk,nqhd->nkhd', d_scores16.astype(jnp.float32), q_heads.astype(jnp.float32))
    d_qkv = jnp.stack([d_query.astype(jnp.bfloat16), d_key.astype(jnp.bfloat16), d_value.astype(jnp.bfloat16)], axis=2).reshape(n_seq, seq_len, 3 * model_dim)
    g_qkv = jnp.einsum('nsd,nse->de', normed1.astype(jnp.float32), d_qkv.astype(jnp.float32))
    d_normed1 = jnp.einsum('nse,de->nsd', d_qkv.astype(jnp.float32), w_qkv.astype(jnp.float32))
    d_in_norm, g_gain_attn = rms_norm_bwd(hidden, inv_rms1, gain_attn, d_normed1)
    return d_mid + d_in_norm, (g_qkv, g_out, g_up, g_down, g_gain_attn, g_gain_mlp)


def device_pass(dev_tokens, dev_lens, dev_cot, weights):
    def fwd_layer(hidden, layer_w):
        return layer_parts(hidden, dev_lens, layer_w)[0], hidden

    dev_out, saved_in = lax.scan(fwd_layer, dev_tokens, weights)

    def bwd_layer(d_hidden, layer_in):
        layer_w, hid_in = layer_in
        return layer_backward(hid_in, dev_lens, layer_w, d_hidden)

    dev_grads = lax.scan(bwd_layer, dev_cot.astype(jnp.float32), (weights, saved_in), reverse=True)[1]
    return dev_out, dev_grads


def reference(tokens, seq_lens, cotangent, w_qkv, w_out, w_up, w_down, gain_attn, gain_mlp):
    weights = (w_qkv, w_out, w_up, w_down, gain_attn, gain_mlp)
    dev_shape = (STAGES, MICRO_BATCHES, SEQ_LEN, D_MODEL)
    per_dev = (tokens.reshape(dev_shape), seq_lens.reshape(STAGES, MICRO_BATCHES), cotangent.reshape(dev_shape))

    def over_devices(grad_sum, dev_in):
        dev_out, dev_grads = device_pass(dev_in[0], dev_in[1], dev_in[2], weights)
        return tuple(acc_val + grad_val for acc_val, grad_val in zip(grad_sum, dev_grads)), dev_out

    zero_sum = tuple(jnp.zeros(weight.shape, jnp.float32) for weight in weights)
    grad_sum, all_out = lax.scan(over_devices, zero_sum, per_dev)
    return (all_out.reshape(tokens.shape), grad_sum[0], grad_sum[1], grad_sum[2], grad_sum[3], grad_sum[4], grad_sum[5])
```

```python
import functools
import jax
import jax.numpy as jnp
from jax import lax
from jax.experimental import pallas as pl
from jax.experimental.pallas import tpu as pltpu
from jax.sharding import PartitionSpec as P

bf16, f32 = jnp.bfloat16, jnp.float32
EPS = 1e-5
NEG = -1e30
NT = (((1,), (1,)), ((), ()))
MESH = pl.DeviceIdType.MESH
S, D, F, NH = 1024, 512, 2048, 8
C = 256
NC = S // C
NP = 4
KB = 128
ND = 8
LAST = ND - 1


def rms(h, g):
    r = lax.rsqrt(jnp.mean(h * h, axis=-1, keepdims=True) + EPS)
    return (h * r * g).astype(bf16)


def gelu(x):
    t = jnp.tanh(x * (0.7978845608028654 + 0.7978845608028654 * 0.044715 * (x * x)))
    hx = 0.5 * x
    return hx * t + hx


def fwd_kernel(tok, cot, ltile, wqkv, wo, w1, w2, g1, g2,
               y, cot_all, lens, sv_qkv, sv_h, sv_cx, sv_u, sv_lse,
               hbuf, st, cx_s, u_s, o_s, lse_s, k_s, vt_s, ct_s, bias, e_s, p_s,
               recv_sem, send_sem, tok_sem, len_ssem, len_rsem, cot_ssem, cot_rsem, y_sem, loc_sem, yl_sem):
    me = lax.axis_index('stage')

    barrier = pltpu.get_barrier_semaphore()
    for k in range(1, ND):
        pl.semaphore_signal(barrier, inc=1, device_id=(lax.rem(me + k, ND),), device_id_type=MESH)
    pl.semaphore_wait(barrier, ND - 1)

    def tok_copy(c):
        return pltpu.make_async_remote_copy(
            src_ref=tok.at[pl.ds(c * C, C)], dst_ref=hbuf.at[me * NC + c], send_sem=tok_sem.at[c],
            recv_sem=recv_sem.at[me * NC + c], device_id=(0,), device_id_type=MESH)

    def tok_local(c):
        return pltpu.make_async_copy(tok.at[pl.ds(c * C, C)], hbuf.at[c], recv_sem.at[c])

    def len_copy(k):
        return pltpu.make_async_remote_copy(
            src_ref=ltile, dst_ref=lens.at[me], send_sem=len_ssem.at[k - 1], recv_sem=len_rsem.at[me],
            device_id=(lax.rem(me + k, ND),), device_id_type=MESH)

    def len_wait(m):
        pltpu.make_async_remote_copy(
            src_ref=ltile, dst_ref=lens.at[m], send_sem=len_ssem.at[0], recv_sem=len_rsem.at[m],
            device_id=(0,), device_id_type=MESH).wait_recv()

    def cot_copy(m):
        return pltpu.make_async_remote_copy(
            src_ref=cot, dst_ref=cot_all.at[m], send_sem=cot_ssem.at[0], recv_sem=cot_rsem.at[m],
            device_id=(LAST,), device_id_type=MESH)

    def cot_local():
        return pltpu.make_async_copy(cot, cot_all.at[LAST], cot_ssem.at[0])

    def pass_copy(t, slot):
        return pltpu.make_async_remote_copy(
            src_ref=o_s.at[slot], dst_ref=hbuf.at[t], send_sem=send_sem.at[slot], recv_sem=recv_sem.at[t],
            device_id=(lax.rem(me + 1, ND),), device_id_type=MESH)

    def y_copy(m, c):
        return pltpu.make_async_remote_copy(
            src_ref=o_s.at[c % 2], dst_ref=y.at[pl.ds(c * C, C)], send_sem=send_sem.at[c % 2],
            recv_sem=y_sem.at[c], device_id=(m,), device_id_type=MESH)

    def y_local(c):
        return pltpu.make_async_copy(o_s.at[c % 2], y.at[pl.ds(c * C, C)], yl_sem.at[c % 2])

    def saves(m, c):
        t, slot = m * NC + c, c % 2
        rows = pl.ds(c * C, C)
        return [
            pltpu.make_async_copy(st.at[slot], sv_qkv.at[m, :, rows], loc_sem.at[slot, 0]),
            pltpu.make_async_copy(hbuf.at[t], sv_h.at[m, rows], loc_sem.at[slot, 1]),
            pltpu.make_async_copy(cx_s.at[slot], sv_cx.at[m, rows], loc_sem.at[slot, 2]),
            pltpu.make_async_copy(u_s.at[slot], sv_u.at[m, rows], loc_sem.at[slot, 3]),
            pltpu.make_async_copy(lse_s.at[slot], sv_lse.at[m, c], loc_sem.at[slot, 4]),
        ]

    def out_wait(m, c):
        @pl.when(me < LAST)
        def _():
            pass_copy(m * NC + c, c % 2).wait_send()

        @pl.when(me == LAST)
        def _():
            @pl.when(m < LAST)
            def _():
                y_copy(m, c).wait_send()

            @pl.when(m == LAST)
            def _():
                y_local(c).wait()

    @pl.when(me == 0)
    def _():
        for c in range(NC):
            tok_local(c).start()

    @pl.when(me > 0)
    def _():
        for c in range(NC):
            tok_copy(c).start()

    for k in range(1, ND):
        len_copy(k).start()
    lens[me] = ltile[...]

    def step(m, c):
        t, slot = m * NC + c, c % 2

        if c == 0:
            @pl.when(m != me)
            def _():
                len_wait(m)

        @pl.when(jnp.logical_and(me == 0, m == 0))
        def _():
            tok_local(c).wait()

        @pl.when(jnp.logical_or(me > 0, m > 0))
        def _():
            pass_copy(t, slot).wait_recv()

        def reuse(mm):
            for cp in saves(mm, (c - 2) % NC):
                cp.wait()
            out_wait(mm, (c - 2) % NC)

        if c < 2:
            @pl.when(m > 0)
            def _():
                reuse(m - 1)
        else:
            reuse(m)

        h = hbuf[t].astype(f32)
        a = rms(h, g1[...].astype(f32))
        nk = (c + 1) * C
        q = jnp.dot(a, wqkv[:, :D], preferred_element_type=f32)
        kk = jnp.dot(a, wqkv[:, D:2 * D], preferred_element_type=f32).astype(bf16)
        vv = jnp.dot(a, wqkv[:, 2 * D:], preferred_element_type=f32).astype(bf16)
        q = (q * 0.125).astype(bf16)
        for p in range(NP):
            lanes = slice(p * 128, (p + 1) * 128)
            st[slot, p] = q[:, lanes]
            st[slot, NP + p] = kk[:, lanes]
            st[slot, 2 * NP + p] = vv[:, lanes]
            k_s[p, c * C:nk] = kk[:, lanes]
            vt_s[p, :, c * C:nk] = vv[:, lanes].T

        row = lax.broadcasted_iota(jnp.int32, (C, C), 0)
        col = lax.broadcasted_iota(jnp.int32, (C, C), 1)
        ln = lens[m][0:1, :]
        for b in range(c + 1):
            ok = (row + b * C) < ln
            if b == c:
                ok = ok & (row <= col)
            bias[b * C:(b + 1) * C] = jnp.where(ok, 0.0, NEG)

        lane = lax.broadcasted_iota(jnp.int32, (C, 128), 1)

        def pair(p, carry):
            qp = st[slot, p]
            for hh in range(2):
                qm = jnp.where((lane >= 64) == (hh == 1), qp, jnp.zeros_like(qp))
                ms, ls = [], []
                nb = nk // KB
                for b in range(nb):
                    ks = slice(b * KB, (b + 1) * KB)
                    s = lax.dot_general(k_s[p, ks], qm, NT, preferred_element_type=f32) + bias[ks]
                    mb = jnp.max(s, axis=0, keepdims=True)
                    e = jnp.exp(s - mb)
                    ls.append(jnp.sum(e, axis=0, keepdims=True))
                    ms.append(mb)
                    e_s[hh, ks] = e
                mx = functools.reduce(jnp.maximum, ms)
                fs = [jnp.exp(mb - mx) for mb in ms]
                tot = sum(lb * fb for lb, fb in zip(ls, fs))
                inv = 1.0 / tot
                lse_s[slot, p, hh:hh + 1] = mx + jnp.log(tot)
                for b in range(nb):
                    ks = slice(b * KB, (b + 1) * KB)
                    p_s[hh, ks] = (e_s[hh, ks] * (fs[b] * inv)).astype(bf16)
                o = jnp.dot(vt_s[p, hh * 64:(hh + 1) * 64, 0:nk], p_s[hh, 0:nk], preferred_element_type=f32)
                ct_s[p, hh * 64:(hh + 1) * 64] = o.astype(bf16)
            return carry

        lax.fori_loop(0, NP, pair, 0, unroll=True)
        cx = jnp.concatenate([ct_s[p].T for p in range(NP)], axis=1)
        cx_s[slot] = cx
        u = (h + jnp.dot(cx, wo[...], preferred_element_type=f32)).astype(bf16)
        u_s[slot] = u
        for cp in saves(m, c):
            cp.start()
        u = u.astype(f32)
        a2 = rms(u, g2[...].astype(f32))
        z = gelu(jnp.dot(a2, w1[...], preferred_element_type=f32)).astype(bf16)
        o_s[slot] = (u + jnp.dot(z, w2[...], preferred_element_type=f32)).astype(bf16)

        @pl.when(me < LAST)
        def _():
            pass_copy(t, slot).start()

        @pl.when(me == LAST)
        def _():
            @pl.when(m < LAST)
            def _():
                y_copy(m, c).start()

            @pl.when(m == LAST)
            def _():
                y_local(c).start()

    def seq(m, carry):
        @pl.when(m == 2)
        def _():
            @pl.when(me < LAST)
            def _():
                cot_copy(me).start()

            @pl.when(me == LAST)
            def _():
                cot_local().start()

        for c in range(NC):
            step(m, c)
        return carry

    lax.fori_loop(0, ND, seq, 0)

    for c in (NC - 2, NC - 1):
        for cp in saves(LAST, c):
            cp.wait()
        out_wait(LAST, c)
    for k in range(1, ND):
        len_copy(k).wait_send()

    @pl.when(me > 0)
    def _():
        for c in range(NC):
            tok_copy(c).wait_send()

    @pl.when(me < LAST)
    def _():
        cot_copy(me).wait_send()
        for c in range(NC):
            y_copy(0, c).wait_recv()

    @pl.when(me == LAST)
    def _():
        cot_local().wait()
        for m in range(LAST):
            cot_copy(m).wait_recv()


def forward(tok, cot, ltile, wqkv, wo, w1, w2, g1, g2):
    V = pl.BlockSpec(memory_space=pltpu.VMEM)
    A = pl.BlockSpec(memory_space=pltpu.HBM)
    dma = pltpu.SemaphoreType.DMA
    sd = jax.ShapeDtypeStruct
    return pl.pallas_call(
        fwd_kernel,
        out_shape=(sd((S, D), bf16), sd((ND, S, D), bf16), sd((ND, 8, C), jnp.int32),
                   sd((ND, 3 * NP, S, 128), bf16), sd((ND, S, D), bf16), sd((ND, S, D), bf16), sd((ND, S, D), bf16),
                   sd((ND, NC, NP, 2, C), f32)),
        in_specs=[A] + [V] * 8,
        out_specs=(A, A, V, A, A, A, A, A),
        scratch_shapes=[
            pltpu.VMEM((ND * NC, C, D), bf16), pltpu.VMEM((2, 3 * NP, C, 128), bf16), pltpu.VMEM((2, C, D), bf16),
            pltpu.VMEM((2, C, D), bf16), pltpu.VMEM((2, C, D), bf16), pltpu.VMEM((2, NP, 2, C), f32),
            pltpu.VMEM((NP, S, 128), bf16), pltpu.VMEM((NP, 128, S), bf16), pltpu.VMEM((NP, 128, C), bf16),
            pltpu.VMEM((S, C), f32), pltpu.VMEM((2, S, C), f32), pltpu.VMEM((2, S, C), bf16),
            dma((ND * NC,)), dma((2,)), dma((NC,)), dma((ND - 1,)), dma((ND,)), dma((1,)), dma((ND,)), dma((NC,)),
            dma((2, 5)), dma((2,))],
        compiler_params=pltpu.CompilerParams(collective_id=0, has_side_effects=True, vmem_limit_bytes=48 * 1024 * 1024),
        cost_estimate=pl.CostEstimate(flops=80 * 10 ** 9, bytes_accessed=10 ** 8, transcendentals=10 ** 7),
    )(tok, cot, ltile, wqkv, wo, w1, w2, g1, g2)

TN = (((0,), (0,)), ((), ()))
K0 = 0.7978845608028654
K1 = K0 * 0.044715


def bwd_kernel(groups, cot_all, lens, sv_qkv, sv_h, sv_u, sv_lse, wqkv, wo, w1, w2, g1, g2,
               z_o, dpre_o, d16_o, a2_o, a_o, dmid_o, dqkv_o, gg1_o, gg2_o,
               dbuf, cbuf, qkv_b, h_b, u_b, lse_b, kt_s, dk_s, dv_s,
               z_s, dpre_s, d16_s, a2_s, a_s, dmid_s, dqkv_s, o_s, dc_s, bias, p_s, dp_s, p16_s, ds_s, dqt_s,
               recv_sem, send_sem, ld_sem, st_sem):
    me = lax.axis_index('stage')
    barrier = pltpu.get_barrier_semaphore()
    pl.semaphore_signal(barrier, inc=1, device_id=(lax.rem(me + 1, ND),), device_id_type=MESH)
    pl.semaphore_wait(barrier, 1)

    def loads(r, par, n):
        rows = pl.ds(0, n * C)
        return [
            pltpu.make_async_copy(sv_qkv.at[r, :, rows], qkv_b.at[par, :, rows], ld_sem.at[par, 0]),
            pltpu.make_async_copy(sv_h.at[r, rows], h_b.at[par, rows], ld_sem.at[par, 1]),
            pltpu.make_async_copy(sv_u.at[r, rows], u_b.at[par, rows], ld_sem.at[par, 2]),
            pltpu.make_async_copy(sv_lse.at[r, pl.ds(0, n)], lse_b.at[par, pl.ds(0, n)], ld_sem.at[par, 3]),
            pltpu.make_async_copy(cot_all.at[r, rows], cbuf.at[par, rows], ld_sem.at[par, 4]),
        ]

    def stores(row, slot):
        rows = pl.ds(row, C)
        pairs = [(z_s, z_o), (dpre_s, dpre_o), (d16_s, d16_o), (a2_s, a2_o), (a_s, a_o), (dmid_s, dmid_o), (dqkv_s, dqkv_o)]
        return [pltpu.make_async_copy(s.at[slot], o.at[rows], st_sem.at[slot, i]) for i, (s, o) in enumerate(pairs)]

    def send(t, slot):
        return pltpu.make_async_remote_copy(
            src_ref=o_s.at[slot], dst_ref=dbuf.at[t], send_sem=send_sem.at[slot], recv_sem=recv_sem.at[t],
            device_id=(lax.rem(me + ND - 1, ND),), device_id_type=MESH)

    gg1_o[...] = jnp.zeros_like(gg1_o)
    gg2_o[...] = jnp.zeros_like(gg2_o)
    for cp in loads(0, 0, groups[0][0]):
        cp.start()

    def step(r, par, c, n, base, t, slot):
        row0 = pl.multiple_of(base + c * C, C)

        def reuse():
            for cp in stores(0, slot):
                cp.wait()

            @pl.when(me > 0)
            def _():
                send(t, slot).wait_send()

        @pl.when(t >= 2)
        def _():
            reuse()

        @pl.when(me == LAST)
        def _():
            dbuf[t] = cbuf[par, c * C:(c + 1) * C].astype(f32)

        @pl.when(me < LAST)
        def _():
            send(t, slot).wait_recv()

        d = dbuf[t]
        d16 = d.astype(bf16)
        d16_s[slot] = d16
        u = u_b[par, c * C:(c + 1) * C].astype(f32)
        gm = g2[...].astype(f32)
        r2 = lax.rsqrt(jnp.mean(u * u, axis=-1, keepdims=True) + EPS)
        su = u * r2
        a2 = (su * gm).astype(bf16)
        a2_s[slot] = a2
        FB = 512
        for fb in range(F // FB):
            cols = slice(fb * FB, (fb + 1) * FB)
            x = jnp.dot(a2, w1[:, cols], preferred_element_type=f32)
            dz = lax.dot_general(d16, w2[cols], NT, preferred_element_type=f32)
            x2 = x * x
            th = jnp.tanh(x * (K0 + K1 * x2))
            hx = 0.5 * x
            z_s[slot, :, cols] = (hx * th + hx).astype(bf16)
            gp = (0.5 + 0.5 * th) + hx * (1.0 - th * th) * (K0 + 3.0 * K1 * x2)
            dpre_s[slot, :, cols] = (dz * gp).astype(bf16)
        da2 = lax.dot_general(dpre_s[slot], w1[...], NT, preferred_element_type=f32)
        gg2_o[...] += jnp.sum((da2 * su).reshape(C // 8, 8, D), axis=0)
        gd = da2 * gm
        dmid = d + r2 * (gd - su * jnp.mean(gd * su, axis=-1, keepdims=True))
        dmid16 = dmid.astype(bf16)
        dmid_s[slot] = dmid16
        o_s[slot] = dmid
        dc_s[...] = lax.dot_general(dmid16, wo[...], NT, preferred_element_type=f32).astype(bf16)

        nk = (c + 1) * C
        row = lax.broadcasted_iota(jnp.int32, (C, C), 0)
        col = lax.broadcasted_iota(jnp.int32, (C, C), 1)
        ln = lens[r][0:1, :]
        for b in range(c + 1):
            ok = (row + b * C) < ln
            if b == c:
                ok = ok & (row <= col)
            bias[b * C:(b + 1) * C] = jnp.where(ok, 0.0, NEG)
        lane = lax.broadcasted_iota(jnp.int32, (C, 128), 1)
        top = c == n - 1

        for p in range(NP):
            lanes = slice(p * 128, (p + 1) * 128)
            qp = qkv_b[par, p, c * C:(c + 1) * C]
            dcp = dc_s[:, lanes]
            for hh in range(2):
                keep = (lane >= 64) == (hh == 1)
                qm = jnp.where(keep, qp, jnp.zeros_like(qp))
                dom = jnp.where(keep, dcp, jnp.zeros_like(dcp))
                lse = lse_b[par, c, p, hh:hh + 1]
                acc = jnp.zeros((1, C), f32)
                nb = nk // KB
                for b in range(nb):
                    ks = slice(b * KB, (b + 1) * KB)
                    s = lax.dot_general(qkv_b[par, NP + p, ks], qm, NT, preferred_element_type=f32) + bias[ks]
                    pr = jnp.exp(s - lse)
                    dp = lax.dot_general(qkv_b[par, 2 * NP + p, ks], dom, NT, preferred_element_type=f32)
                    acc = acc + jnp.sum(pr * dp, axis=0, keepdims=True)
                    p16_s[hh, ks] = pr.astype(bf16)
                    p_s[hh, ks] = pr
                    dp_s[hh, ks] = dp
                for b in range(nb):
                    ks = slice(b * KB, (b + 1) * KB)
                    ds_s[hh, ks] = (p_s[hh, ks] * (dp_s[hh, ks] - acc)).astype(bf16)
                dvp = jnp.dot(p16_s[hh, 0:nk], dom, preferred_element_type=f32)
                dkp = jnp.dot(ds_s[hh, 0:nk], qm, preferred_element_type=f32)
                if top and hh == 0:
                    dv_s[p, 0:nk] = dvp
                    dk_s[p, 0:nk] = dkp
                else:
                    dv_s[p, 0:nk] += dvp
                    dk_s[p, 0:nk] += dkp
                dqt = jnp.dot(kt_s[p, hh * 64:(hh + 1) * 64, 0:nk], ds_s[hh, 0:nk], preferred_element_type=f32)
                dqt_s[p, hh * 64:(hh + 1) * 64] = dqt * 0.125
        for p in range(NP):
            for i, val in enumerate((dqt_s[p].T, dk_s[p, c * C:(c + 1) * C], dv_s[p, c * C:(c + 1) * C])):
                dqkv_s[slot, :, i * D + p * 128:i * D + (p + 1) * 128] = val.astype(bf16)
        da = lax.dot_general(dqkv_s[slot], wqkv[...], NT, preferred_element_type=f32)
        h = h_b[par, c * C:(c + 1) * C].astype(f32)
        gm = g1[...].astype(f32)
        r1 = lax.rsqrt(jnp.mean(h * h, axis=-1, keepdims=True) + EPS)
        sh = h * r1
        a_s[slot] = (sh * gm).astype(bf16)
        gg1_o[...] += jnp.sum((da * sh).reshape(C // 8, 8, D), axis=0)
        gd = da * gm
        o_s[slot] += r1 * (gd - sh * jnp.mean(gd * sh, axis=-1, keepdims=True))
        for cp in stores(row0, slot):
            cp.start()

        @pl.when(me > 0)
        def _():
            send(t, slot).start()

    r0 = t0 = 0
    for gi, (n, count) in enumerate(groups):
        nxt = groups[gi + 1][0] if gi + 1 < len(groups) else 0
        def one(i, carry, n=n, count=count, nxt=nxt, r0=r0, t0=t0):
            r = r0 + i
            par = lax.rem(r, 2)
            for cp in loads(r, par, n):
                cp.wait()

            if count > 1:
                @pl.when(i + 1 < count)
                def _():
                    for cp in loads(r + 1, 1 - par, n):
                        cp.start()
            if nxt:
                @pl.when(i + 1 == count)
                def _():
                    for cp in loads(r + 1, 1 - par, nxt):
                        cp.start()
            for p in range(NP):
                kt_s[p, :, 0:n * C] = qkv_b[par, NP + p, 0:n * C].T
            for j in range(n):
                t = t0 + i * n + j
                step(r, par, n - 1 - j, n, (t0 + i * n) * C, t, lax.rem(t, 2))
            return carry

        lax.fori_loop(0, count, one, 0)
        r0 += count
        t0 += n * count
    for t in (t0 - 2, t0 - 1):
        for cp in stores(0, t % 2):
            cp.wait()

        @pl.when(me > 0)
        def _():
            send(t, t % 2).wait_send()


def backward(groups, cid, cot_all, lens, sv_qkv, sv_h, sv_u, sv_lse, wqkv, wo, w1, w2, g1, g2):
    V = pl.BlockSpec(memory_space=pltpu.VMEM)
    A = pl.BlockSpec(memory_space=pltpu.HBM)
    dma = pltpu.SemaphoreType.DMA
    sd = jax.ShapeDtypeStruct
    T = sum(n * k for n, k in groups)
    R = T * C
    VM = pltpu.VMEM
    return pl.pallas_call(
        functools.partial(bwd_kernel, groups),
        out_shape=(sd((R, F), bf16), sd((R, F), bf16), sd((R, D), bf16), sd((R, D), bf16), sd((R, D), bf16), sd((R, D), bf16),
                   sd((R, 3 * D), bf16), sd((8, D), f32), sd((8, D), f32)),
        in_specs=[A, V] + [A] * 4 + [V] * 6,
        out_specs=(A,) * 7 + (V, V),
        scratch_shapes=[
            VM((T, C, D), f32), VM((2, S, D), bf16), VM((2, 3 * NP, S, 128), bf16), VM((2, S, D), bf16), VM((2, S, D), bf16),
            VM((2, NC, NP, 2, C), f32), VM((NP, 128, S), bf16), VM((NP, S, 128), f32), VM((NP, S, 128), f32),
            VM((2, C, F), bf16), VM((2, C, F), bf16), VM((2, C, D), bf16), VM((2, C, D), bf16), VM((2, C, D), bf16),
            VM((2, C, D), bf16), VM((2, C, 3 * D), bf16), VM((2, C, D), f32), VM((C, D), bf16), VM((S, C), f32),
            VM((2, S, C), f32), VM((2, S, C), f32), VM((2, S, C), bf16), VM((2, S, C), bf16), VM((NP, 128, C), f32),
            dma((T,)), dma((2,)), dma((2, 5)), dma((2, 7))],
        compiler_params=pltpu.CompilerParams(collective_id=cid, has_side_effects=True, vmem_limit_bytes=61 * 1024 * 1024),
        cost_estimate=pl.CostEstimate(flops=80 * 10 ** 9, bytes_accessed=10 ** 8, transcendentals=10 ** 7),
    )(cot_all, lens, sv_qkv, sv_h, sv_u, sv_lse, wqkv, wo, w1, w2, g1, g2)


def solution(mesh):
    def per_device(tokens, seq_lens, cot, wqkv, wo, w1, w2, g1, g2):
        lt = jnp.broadcast_to(seq_lens.reshape(1, 1), (8, C))
        wts = (wqkv[0], wo[0], w1[0], w2[0], g1, g2)
        y, cot_all, lens, sv_qkv, sv_h, sv_cx, sv_u, sv_lse = forward(tokens[0], cot[0], lt, *wts)
        z, dpre, d16, a2, a, dmid, dqkv, gg1, gg2 = backward(((NC, ND),), 1, cot_all, lens, sv_qkv, sv_h, sv_u, sv_lse, *wts)

        def wgrad(x, dy):
            return lax.dot_general(x, dy, TN, preferred_element_type=f32)[None]

        return (y[None], wgrad(a, dqkv), wgrad(sv_cx.reshape(-1, D), dmid), wgrad(a2, dpre), wgrad(z, d16),
                jnp.sum(gg1, axis=0, keepdims=True), jnp.sum(gg2, axis=0, keepdims=True))

    spec = P('stage')
    return jax.shard_map(per_device, mesh=mesh, in_specs=(spec,) * 9, out_specs=(spec,) * 7, check_vma=False)
```

```python
import functools
import jax
import jax.numpy as jnp
from jax import lax
from jax.experimental import pallas as pl
from jax.experimental.pallas import tpu as pltpu
from jax.sharding import PartitionSpec as P

bf16, f32 = jnp.bfloat16, jnp.float32
EPS = 1e-5
NEG = -1e30
BIG = 1e30
NT = (((1,), (1,)), ((), ()))
MESH = pl.DeviceIdType.MESH
S, D, F, NH = 1024, 512, 2048, 8
C = 128
C2 = 2 * C
NC = S // C
NP = 4
KB = 128
ND = 8
LAST = ND - 1
NT_ALL = ND * NC


def rms(h, g):
    r = lax.rsqrt(jnp.mean(h * h, axis=-1, keepdims=True) + EPS)
    return (h * r * g).astype(bf16)


def gelu(x):
    t = jnp.tanh(x * (0.7978845608028654 + 0.7978845608028654 * 0.044715 * (x * x)))
    hx = 0.5 * x
    return hx * t + hx


def fwd_kernel(tok, cot, ltile, wqkv, wo, w1, w2, g1, g2,
               y, cot_all, lens, sv_qkv, sv_h, sv_cx, sv_u, sv_lse, wqkv_t, wo_t, w1_t, w2_t,
               hbuf, st, cx_s, u_s, o_s, lse_s, k_s, vt_s, ct_s, bias, e_s, p_s, t1, t2, t3, t4,
               recv_sem, send_sem, tok_sem, len_ssem, len_rsem, cot_ssem, cot_rsem, y_sem, loc_sem, yl_sem, wt_sem):
    me = lax.axis_index('stage')

    barrier = pltpu.get_barrier_semaphore()
    for k in range(1, ND):
        pl.semaphore_signal(barrier, inc=1, device_id=(lax.rem(me + k, ND),), device_id_type=MESH)
    pl.semaphore_wait(barrier, ND - 1)

    def tok_copy(c):
        return pltpu.make_async_remote_copy(
            src_ref=tok.at[pl.ds(c * C, C)], dst_ref=hbuf.at[me * NC + c], send_sem=tok_sem.at[c],
            recv_sem=recv_sem.at[me * NC + c], device_id=(0,), device_id_type=MESH)

    def tok_local(c):
        return pltpu.make_async_copy(tok.at[pl.ds(c * C, C)], hbuf.at[c], recv_sem.at[c])

    def len_copy(k):
        return pltpu.make_async_remote_copy(
            src_ref=ltile, dst_ref=lens.at[me], send_sem=len_ssem.at[k - 1], recv_sem=len_rsem.at[me],
            device_id=(lax.rem(me + k, ND),), device_id_type=MESH)

    def len_wait(m):
        pltpu.make_async_remote_copy(
            src_ref=ltile, dst_ref=lens.at[m], send_sem=len_ssem.at[0], recv_sem=len_rsem.at[m],
            device_id=(0,), device_id_type=MESH).wait_recv()

    def cot_copy(m):
        return pltpu.make_async_remote_copy(
            src_ref=cot, dst_ref=cot_all.at[m], send_sem=cot_ssem.at[0], recv_sem=cot_rsem.at[m],
            device_id=(LAST,), device_id_type=MESH)

    def cot_local():
        return pltpu.make_async_copy(cot, cot_all.at[LAST], cot_ssem.at[0])

    def pass_copy(t, slot):
        return pltpu.make_async_remote_copy(
            src_ref=o_s.at[slot], dst_ref=hbuf.at[t], send_sem=send_sem.at[slot], recv_sem=recv_sem.at[t],
            device_id=(lax.rem(me + 1, ND),), device_id_type=MESH)

    def y_copy(m, c):
        return pltpu.make_async_remote_copy(
            src_ref=o_s.at[c % 2], dst_ref=y.at[pl.ds(c * C, C)], send_sem=send_sem.at[c % 2],
            recv_sem=y_sem.at[c], device_id=(m,), device_id_type=MESH)

    def y_local(c):
        return pltpu.make_async_copy(o_s.at[c % 2], y.at[pl.ds(c * C, C)], yl_sem.at[c % 2])

    def saves(m, c):
        t, slot = m * NC + c, c % 2
        return [
            pltpu.make_async_copy(st.at[slot], sv_qkv.at[t], loc_sem.at[slot, 0]),
            pltpu.make_async_copy(hbuf.at[t], sv_h.at[t], loc_sem.at[slot, 1]),
            pltpu.make_async_copy(cx_s.at[slot], sv_cx.at[t], loc_sem.at[slot, 2]),
            pltpu.make_async_copy(u_s.at[slot], sv_u.at[t], loc_sem.at[slot, 3]),
            pltpu.make_async_copy(lse_s.at[slot], sv_lse.at[t], loc_sem.at[slot, 4]),
        ]

    def out_wait(m, c):
        @pl.when(me < LAST)
        def _():
            pass_copy(m * NC + c, c % 2).wait_send()

        @pl.when(me == LAST)
        def _():
            @pl.when(m < LAST)
            def _():
                y_copy(m, c).wait_send()

            @pl.when(m == LAST)
            def _():
                y_local(c).wait()

    @pl.when(me == 0)
    def _():
        for c in range(NC):
            tok_local(c).start()

    @pl.when(jnp.logical_and(me > 0, me < 3))
    def _():
        for c in range(NC):
            tok_copy(c).start()

    turned = [pltpu.make_async_copy(a, b, wt_sem.at[i])
              for i, (a, b) in enumerate(((t1, wqkv_t), (t2, wo_t), (t3, w1_t), (t4, w2_t)))]

    def turn_weights():
        for src, dst in ((wqkv, t1), (wo, t2), (w1, t3), (w2, t4)):
            def block(i, carry, src=src, dst=dst):
                at = pl.ds(pl.multiple_of(i * 128, 128), 128)
                dst[at] = src[:, at].T
                return carry
            lax.fori_loop(0, src.shape[1] // 128, block, 0)
        for cp in turned:
            cp.start()

    for k in range(1, ND):
        len_copy(k).start()
    lens[me] = ltile[...]

    @pl.when(me >= 4)
    def _():
        turn_weights()

    def step(m, c):
        t, slot = m * NC + c, c % 2

        if c == 0:
            @pl.when(m != me)
            def _():
                len_wait(m)

        @pl.when(jnp.logical_and(me == 0, m == 0))
        def _():
            tok_local(c).wait()

        @pl.when(jnp.logical_or(me > 0, m > 0))
        def _():
            pass_copy(t, slot).wait_recv()

        if c == 0:
            @pl.when(jnp.logical_and(me > 2, m == 0))
            def _():
                for i in range(NC):
                    tok_copy(i).start()

        def reuse(mm):
            for cp in saves(mm, (c - 2) % NC):
                cp.wait()
            out_wait(mm, (c - 2) % NC)

        if c < 2:
            @pl.when(m > 0)
            def _():
                reuse(m - 1)
        else:
            reuse(m)

        h = hbuf[t].astype(f32)
        a = rms(h, g1[...].astype(f32))
        nk = (c + 1) * C
        q = jnp.dot(a, wqkv[:, :D], preferred_element_type=f32)
        kk = jnp.dot(a, wqkv[:, D:2 * D], preferred_element_type=f32).astype(bf16)
        vv = jnp.dot(a, wqkv[:, 2 * D:], preferred_element_type=f32).astype(bf16)
        q = (q * 0.125).astype(bf16)
        half = lax.broadcasted_iota(jnp.int32, (128, C), 0) < 64

        def q_of(p):
            qt = q[:, p * 128:(p + 1) * 128].T
            zero = jnp.zeros_like(qt)
            return jnp.concatenate([jnp.where(half, qt, zero), jnp.where(half, zero, qt)], axis=1)

        for p in range(NP):
            lanes = slice(p * 128, (p + 1) * 128)
            st[slot, p] = q[:, lanes]
            st[slot, NP + p] = kk[:, lanes]
            st[slot, 2 * NP + p] = vv[:, lanes]
            k_s[p, c * C:nk] = kk[:, lanes]
            vt_s[p, :, c * C:nk] = vv[:, lanes].T

        row = lax.broadcasted_iota(jnp.int32, (C, C2), 0)
        col = lax.rem(lax.broadcasted_iota(jnp.int32, (C, C2), 1), C)
        ln = lens[m][0:1, :]
        for b in range(c + 1):
            ok = (row + b * C) < ln
            if b == c:
                ok = ok & (row <= col)
            bias[b * C:(b + 1) * C] = jnp.where(ok, 0.0, NEG)
        here = (col[0:1] + c * C) < ln

        for p in range(NP):
            qt = q_of(p)
            ms, ls = [], []
            nb = nk // KB
            for b in range(nb):
                ks = slice(b * KB, (b + 1) * KB)
                s = jnp.dot(k_s[p, ks], qt, preferred_element_type=f32) + bias[ks]
                mb = jnp.max(s, axis=0, keepdims=True)
                e = jnp.exp(s - mb)
                ls.append(jnp.sum(e, axis=0, keepdims=True))
                ms.append(mb)
                e_s[p % 2, ks] = e
            mx = functools.reduce(jnp.maximum, ms)
            fs = [jnp.exp(mb - mx) for mb in ms]
            tot = sum(lb * fb for lb, fb in zip(ls, fs))
            inv = 1.0 / tot
            lse_s[slot, p:p + 1] = jnp.where(here, mx + jnp.log(tot), BIG)
            for b in range(nb):
                ks = slice(b * KB, (b + 1) * KB)
                p_s[p % 2, ks] = (e_s[p % 2, ks] * (fs[b] * inv)).astype(bf16)
            o = jnp.dot(vt_s[p, :, 0:nk], p_s[p % 2, 0:nk], preferred_element_type=f32)
            ct_s[p, 0:64] = o[0:64, 0:C].astype(bf16)
            ct_s[p, 64:128] = o[64:128, C:C2].astype(bf16)
        cx = jnp.concatenate([ct_s[p].T for p in range(NP)], axis=1)
        cx_s[slot] = cx
        u = (h + jnp.dot(cx, wo[...], preferred_element_type=f32)).astype(bf16)
        u_s[slot] = u
        for cp in saves(m, c):
            cp.start()
        u = u.astype(f32)
        a2 = rms(u, g2[...].astype(f32))
        z = gelu(jnp.dot(a2, w1[...], preferred_element_type=f32)).astype(bf16)
        o_s[slot] = (u + jnp.dot(z, w2[...], preferred_element_type=f32)).astype(bf16)

        @pl.when(me < LAST)
        def _():
            pass_copy(t, slot).start()

        @pl.when(me == LAST)
        def _():
            @pl.when(m < LAST)
            def _():
                y_copy(m, c).start()

            @pl.when(m == LAST)
            def _():
                y_local(c).start()

    def seq(m, carry):
        @pl.when(m == 2)
        def _():
            @pl.when(me < LAST)
            def _():
                cot_copy(me).start()

            @pl.when(me == LAST)
            def _():
                cot_local().start()

        for c in range(NC):
            step(m, c)
        return carry

    lax.fori_loop(0, ND, seq, 0)

    @pl.when(me < 4)
    def _():
        turn_weights()

    for cp in turned:
        cp.wait()
    for c in (NC - 2, NC - 1):
        for cp in saves(LAST, c):
            cp.wait()
        out_wait(LAST, c)
    for k in range(1, ND):
        len_copy(k).wait_send()

    @pl.when(me > 0)
    def _():
        for c in range(NC):
            tok_copy(c).wait_send()

    @pl.when(me < LAST)
    def _():
        cot_copy(me).wait_send()
        for c in range(NC):
            y_copy(0, c).wait_recv()

    @pl.when(me == LAST)
    def _():
        cot_local().wait()
        for m in range(LAST):
            cot_copy(m).wait_recv()


def forward(tok, cot, ltile, wqkv, wo, w1, w2, g1, g2):
    V = pl.BlockSpec(memory_space=pltpu.VMEM)
    A = pl.BlockSpec(memory_space=pltpu.HBM)
    dma = pltpu.SemaphoreType.DMA
    sd = jax.ShapeDtypeStruct
    return pl.pallas_call(
        fwd_kernel,
        out_shape=(sd((S, D), bf16), sd((ND, S, D), bf16), sd((ND, 8, C2), jnp.int32),
                   sd((NT_ALL, 3 * NP, C, 128), bf16), sd((NT_ALL, C, D), bf16), sd((NT_ALL, C, D), bf16), sd((NT_ALL, C, D), bf16),
                   sd((NT_ALL, NP, C2), f32), sd((3 * D, D), bf16), sd((D, D), bf16), sd((F, D), bf16), sd((D, F), bf16)),
        in_specs=[A] + [V] * 8,
        out_specs=(A, A, V) + (A,) * 9,
        scratch_shapes=[
            pltpu.VMEM((ND * NC, C, D), bf16), pltpu.VMEM((2, 3 * NP, C, 128), bf16), pltpu.VMEM((2, C, D), bf16),
            pltpu.VMEM((2, C, D), bf16), pltpu.VMEM((2, C, D), bf16), pltpu.VMEM((2, NP, C2), f32),
            pltpu.VMEM((NP, S, 128), bf16), pltpu.VMEM((NP, 128, S), bf16), pltpu.VMEM((NP, 128, C), bf16),
            pltpu.VMEM((S, C2), f32), pltpu.VMEM((2, S, C2), f32), pltpu.VMEM((2, S, C2), bf16),
            pltpu.VMEM((3 * D, D), bf16), pltpu.VMEM((D, D), bf16), pltpu.VMEM((F, D), bf16), pltpu.VMEM((D, F), bf16),
            dma((ND * NC,)), dma((2,)), dma((NC,)), dma((ND - 1,)), dma((ND,)), dma((1,)), dma((ND,)), dma((NC,)),
            dma((2, 5)), dma((2,)), dma((4,))],
        compiler_params=pltpu.CompilerParams(collective_id=0, has_side_effects=True, vmem_limit_bytes=48 * 1024 * 1024),
        cost_estimate=pl.CostEstimate(flops=80 * 10 ** 9, bytes_accessed=10 ** 8, transcendentals=10 ** 7),
    )(tok, cot, ltile, wqkv, wo, w1, w2, g1, g2)

TN = (((0,), (0,)), ((), ()))
K0 = 0.7978845608028654
K1 = K0 * 0.044715
LOG2E = 1.4426950408889634


def bwd_kernel(sizes, cot_all, sv_qkv, sv_h, sv_u, sv_lse, wqkv_t, wo_t, w1, w1_t, w2_t, g1, g2,
               z_o, dpre_o, d16_o, a2_o, a_o, dmid_o, dqkv_o, gg1_o, gg2_o,
               dbuf, cbuf, qkv_b, h_b, u_b, lse_b, kt_s, dk_s, dv_s,
               z_s, dpre_s, d16_s, a2_s, a_s, dmid_s, dqkv_s, o_s, qm_s, qt_s, dm_s, dt_s, p_s, dp_s, dsum_s, dqt_s,
               recv_sem, send_sem, ld_sem, st_sem):
    me = lax.axis_index('stage')
    barrier = pltpu.get_barrier_semaphore()
    pl.semaphore_signal(barrier, inc=1, device_id=(lax.rem(me + 1, ND),), device_id_type=MESH)
    pl.semaphore_wait(barrier, 1)
    starts = [sum(sizes[:i]) for i in range(len(sizes))]
    total = sum(sizes)

    def loads(r, par):
        dst, src = pl.ds(0, sizes[r]), pl.ds(starts[r], sizes[r])
        pairs = [(sv_qkv, qkv_b), (sv_h, h_b), (sv_u, u_b), (sv_lse, lse_b), (cot_all, cbuf)]
        return [pltpu.make_async_copy(a.at[src], b.at[par, dst], ld_sem.at[par, i]) for i, (a, b) in enumerate(pairs)]

    def stores(row, slot):
        rows = pl.ds(row, C)
        pairs = [(z_s, z_o), (dpre_s, dpre_o), (d16_s, d16_o), (a2_s, a2_o), (a_s, a_o), (dmid_s, dmid_o), (dqkv_s, dqkv_o)]
        return [pltpu.make_async_copy(s.at[slot], o.at[rows], st_sem.at[slot, i]) for i, (s, o) in enumerate(pairs)]

    def send(t, slot):
        return pltpu.make_async_remote_copy(
            src_ref=o_s.at[slot], dst_ref=dbuf.at[t], send_sem=send_sem.at[slot], recv_sem=recv_sem.at[t],
            device_id=(lax.rem(me + ND - 1, ND),), device_id_type=MESH)

    for cp in loads(0, 0):
        cp.start()
    gg1_o[...] = jnp.zeros_like(gg1_o)
    gg2_o[...] = jnp.zeros_like(gg2_o)
    dk_s[...] = jnp.zeros_like(dk_s)
    dv_s[...] = jnp.zeros_like(dv_s)
    causal = lax.broadcasted_iota(jnp.int32, (C, C2), 0) <= lax.rem(lax.broadcasted_iota(jnp.int32, (C, C2), 1), C)
    lane = lax.broadcasted_iota(jnp.int32, (C, 128), 1) < 64

    def stack(x):
        zero = jnp.zeros_like(x)
        return jnp.concatenate([jnp.where(lane, x, zero), jnp.where(lane, zero, x)], axis=0)

    def step(t, carry):
        r, n, first = 0, sizes[0], 0
        for i in range(1, len(sizes)):
            past = (t + 1024 - starts[i]) // 1024
            r = r + past
            n = n + past * (sizes[i] - sizes[i - 1])
            first = first + past * (starts[i] - starts[i - 1])
        c = n - 1 - (t - first)
        par, slot = lax.rem(r, 2), lax.rem(t, 2)
        row0 = pl.multiple_of((first + c) * C, C)
        rows = pl.ds(pl.multiple_of(c * C, C), C)

        for i in range(len(sizes)):
            @pl.when(t == starts[i])
            def _(i=i):
                for cp in loads(i, i % 2):
                    cp.wait()
                if i + 1 < len(sizes):
                    for cp in loads(i + 1, (i + 1) % 2):
                        cp.start()

                def turn(j, carry):
                    for p in range(NP):
                        kt_s[p, :, pl.ds(pl.multiple_of(j * C, C), C)] = qkv_b[i % 2, j, NP + p].T
                    return carry
                lax.fori_loop(0, sizes[i], turn, 0)

        @pl.when(t >= 2)
        def _():
            for cp in stores(0, slot):
                cp.wait()

            @pl.when(me > 0)
            def _():
                send(t, slot).wait_send()

        @pl.when(me == LAST)
        def _():
            dbuf[t] = cbuf[par, c].astype(f32)

        u = u_b[par, c].astype(f32)
        gm2 = g2[...].astype(f32)
        r2 = lax.rsqrt(jnp.mean(u * u, axis=-1, keepdims=True) + EPS)
        su = u * r2
        a2 = (su * gm2).astype(bf16)
        a2_s[slot] = a2
        for p in range(NP):
            qm = stack(qkv_b[par, c, p])
            qm_s[p] = qm
            qt_s[p] = qm.T

        @pl.when(me < LAST)
        def _():
            send(t, slot).wait_recv()

        d = dbuf[t]
        d16 = d.astype(bf16)
        d16_s[slot] = d16
        FB = 512
        for fb in range(F // FB):
            cols = slice(fb * FB, (fb + 1) * FB)
            x = jnp.dot(a2, w1[:, cols], preferred_element_type=f32)
            dz = jnp.dot(d16, w2_t[:, cols], preferred_element_type=f32)
            x2 = x * x
            th = jnp.tanh(x * (K0 + K1 * x2))
            hx = 0.5 * x
            z_s[slot, :, cols] = (hx * th + hx).astype(bf16)
            gp = (0.5 + 0.5 * th) + hx * (1.0 - th * th) * (K0 + 3.0 * K1 * x2)
            dpre_s[slot, :, cols] = (dz * gp).astype(bf16)
        da2 = jnp.dot(dpre_s[slot], w1_t[...], preferred_element_type=f32)
        gg2_o[...] += jnp.sum((da2 * su).reshape(C // 8, 8, D), axis=0)
        gd = da2 * gm2
        dmid = d + r2 * (gd - su * jnp.mean(gd * su, axis=-1, keepdims=True))
        dmid16 = dmid.astype(bf16)
        dmid_s[slot] = dmid16
        o_s[slot] = dmid
        dc = jnp.dot(dmid16, wo_t[...], preferred_element_type=f32).astype(bf16)
        for p in range(NP):
            dm = stack(dc[:, p * 128:(p + 1) * 128])
            dm_s[p] = dm
            dt_s[p] = dm.T
        dsum_s[...] = jnp.zeros_like(dsum_s)
        dqt_s[...] = jnp.zeros_like(dqt_s)

        def scores(b, diagonal):
            for p in range(NP):
                s = jnp.dot(qkv_b[par, b, NP + p], qt_s[p], preferred_element_type=f32) * LOG2E - lse_b[par, c, p:p + 1] * LOG2E
                if diagonal:
                    s = jnp.where(causal, s, NEG)
                pr = jnp.exp2(s)
                dp = jnp.dot(qkv_b[par, b, 2 * NP + p], dt_s[p], preferred_element_type=f32)
                dsum_s[p] += jnp.sum((pr * dp).reshape(C // 8, 8, C2), axis=0)
                p_s[b, p] = pr
                dp_s[b, p] = dp

        def grads(b):
            ks = pl.ds(pl.multiple_of(b * C, C), C)
            for p in range(NP):
                pr = p_s[b, p]
                ds = (pr * (dp_s[b, p] - jnp.sum(dsum_s[p], axis=0, keepdims=True))).astype(bf16)
                dv_s[p, ks] += jnp.dot(pr.astype(bf16), dm_s[p], preferred_element_type=f32)
                dk_s[p, ks] += jnp.dot(ds, qm_s[p], preferred_element_type=f32)
                dqt = jnp.dot(kt_s[p, :, ks], ds, preferred_element_type=f32)
                dqt_s[p, 0:64] += dqt[0:64, 0:C]
                dqt_s[p, 64:128] += dqt[64:128, C:C2]

        def loop1(b, carry):
            scores(b, False)
            return carry

        def loop2(b, carry):
            grads(b)
            return carry

        lax.fori_loop(0, c, loop1, 0)
        scores(c, True)
        grads(c)
        lax.fori_loop(0, c, loop2, 0)

        for p in range(NP):
            for i, val in enumerate((dqt_s[p].T * 0.125, dk_s[p, rows], dv_s[p, rows])):
                dqkv_s[slot, :, i * D + p * 128:i * D + (p + 1) * 128] = val.astype(bf16)
            dk_s[p, rows] = jnp.zeros((C, 128), f32)
            dv_s[p, rows] = jnp.zeros((C, 128), f32)
        da = jnp.dot(dqkv_s[slot], wqkv_t[...], preferred_element_type=f32)
        h = h_b[par, c].astype(f32)
        gm1 = g1[...].astype(f32)
        r1 = lax.rsqrt(jnp.mean(h * h, axis=-1, keepdims=True) + EPS)
        sh = h * r1
        a_s[slot] = (sh * gm1).astype(bf16)
        gg1_o[...] += jnp.sum((da * sh).reshape(C // 8, 8, D), axis=0)
        gd = da * gm1
        o_s[slot] += r1 * (gd - sh * jnp.mean(gd * sh, axis=-1, keepdims=True))
        for cp in stores(row0, slot):
            cp.start()

        @pl.when(me > 0)
        def _():
            send(t, slot).start()
        return carry

    lax.fori_loop(0, total, step, 0)
    for t in (total - 2, total - 1):
        for cp in stores(0, t % 2):
            cp.wait()

        @pl.when(me > 0)
        def _():
            send(t, t % 2).wait_send()


def backward(sizes, cid, cot_all, sv_qkv, sv_h, sv_u, sv_lse, wqkv_t, wo_t, w1, w1_t, w2_t, g1, g2):
    V = pl.BlockSpec(memory_space=pltpu.VMEM)
    A = pl.BlockSpec(memory_space=pltpu.HBM)
    dma = pltpu.SemaphoreType.DMA
    sd = jax.ShapeDtypeStruct
    T = sum(sizes)
    R = T * C
    VM = pltpu.VMEM
    return pl.pallas_call(
        functools.partial(bwd_kernel, sizes),
        out_shape=(sd((R, F), bf16), sd((R, F), bf16), sd((R, D), bf16), sd((R, D), bf16), sd((R, D), bf16), sd((R, D), bf16),
                   sd((R, 3 * D), bf16), sd((8, D), f32), sd((8, D), f32)),
        in_specs=[A] * 5 + [V] * 7,
        out_specs=(A,) * 7 + (V, V),
        scratch_shapes=[
            VM((T, C, D), f32), VM((2, NC, C, D), bf16), VM((2, NC, 3 * NP, C, 128), bf16), VM((2, NC, C, D), bf16), VM((2, NC, C, D), bf16),
            VM((2, NC, NP, C2), f32), VM((NP, 128, S), bf16), VM((NP, S, 128), f32), VM((NP, S, 128), f32),
            VM((2, C, F), bf16), VM((2, C, F), bf16), VM((2, C, D), bf16), VM((2, C, D), bf16), VM((2, C, D), bf16),
            VM((2, C, D), bf16), VM((2, C, 3 * D), bf16), VM((2, C, D), f32),
            VM((NP, C2, 128), bf16), VM((NP, 128, C2), bf16), VM((NP, C2, 128), bf16), VM((NP, 128, C2), bf16),
            VM((NC, NP, C, C2), f32), VM((NC, NP, C, C2), f32), VM((NP, 8, C2), f32), VM((NP, 128, C), f32),
            dma((T,)), dma((2,)), dma((2, 5)), dma((2, 7))],
        compiler_params=pltpu.CompilerParams(collective_id=cid, has_side_effects=True, vmem_limit_bytes=61 * 1024 * 1024),
        cost_estimate=pl.CostEstimate(flops=80 * 10 ** 9, bytes_accessed=10 ** 8, transcendentals=10 ** 7),
    )(cot_all, sv_qkv, sv_h, sv_u, sv_lse, wqkv_t, wo_t, w1, w1_t, w2_t, g1, g2)


def pack_kernel(plans, lens, qkv, h, u, lse, cot, cx, pick_o, qkv_o, h_o, u_o, lse_o, cot_o, cx_o,
                qkv_b, h_b, u_b, lse_b, cot_b, cx_b, order, src, ld_sem, st_sem):
    for m in range(ND):
        rank = 0
        for k in range(ND):
            longer = lens[k] > lens[m] if k >= m else lens[k] >= lens[m]
            rank = rank + jnp.where(longer, 1, 0)
        order[rank] = m
    pick = len(plans) - 1
    for i in reversed(range(len(plans) - 1)):
        fits = True
        for r in range(ND):
            fits = jnp.logical_and(fits, lens[order[r]] <= plans[i][r] * C)
        pick = jnp.where(fits, i, pick)
    pick_o[0] = pick
    count = 0
    for r in range(ND):
        n = 0
        for i, plan in enumerate(plans):
            n = n + jnp.where(pick == i, plan[r], 0)

        def put(j, carry, count=count, r=r):
            src[count + j] = order[r] * NC + j
            return carry
        lax.fori_loop(0, n, put, 0)
        count = count + n
    arrays = ((qkv, qkv_b, qkv_o), (h, h_b, h_o), (u, u_b, u_o), (lse, lse_b, lse_o), (cot, cot_b, cot_o), (cx, cx_b, cx_o))

    def load(t):
        s = lax.rem(t, RING)
        return [pltpu.make_async_copy(a.at[src[t]], b.at[s], ld_sem.at[s, i]) for i, (a, b, _) in enumerate(arrays)]

    def store(t):
        s = lax.rem(t, RING)
        return [pltpu.make_async_copy(b.at[s], o.at[t], st_sem.at[s, i]) for i, (_, b, o) in enumerate(arrays)]

    lag = RING // 2

    def go(t, carry):
        @pl.when(t < count)
        def _():
            @pl.when(t >= RING)
            def _():
                for cp in store(t - RING):
                    cp.wait()
            for cp in load(t):
                cp.start()

        @pl.when(t >= lag)
        def _():
            for cp in load(t - lag):
                cp.wait()
            for cp in store(t - lag):
                cp.start()
        return carry

    lax.fori_loop(0, count + lag, go, 0)

    def drain(t, carry):
        for cp in store(t):
            cp.wait()
        return carry

    lax.fori_loop(jnp.maximum(count - RING, 0), count, drain, 0)


RING = 12


def pack(plans, lens, *arrays):
    A = pl.BlockSpec(memory_space=pltpu.HBM)
    SM = pl.BlockSpec(memory_space=pltpu.SMEM)
    return pl.pallas_call(
        functools.partial(pack_kernel, plans),
        out_shape=(jax.ShapeDtypeStruct((1,), jnp.int32),) + tuple(jax.ShapeDtypeStruct(a.shape, a.dtype) for a in arrays),
        in_specs=[SM] + [A] * 6,
        out_specs=(SM,) + (A,) * 6,
        scratch_shapes=[pltpu.VMEM((RING,) + a.shape[1:], a.dtype) for a in arrays] + [
            pltpu.SMEM((ND,), jnp.int32), pltpu.SMEM((NT_ALL,), jnp.int32),
            pltpu.SemaphoreType.DMA((RING, 6)), pltpu.SemaphoreType.DMA((RING, 6))],
        compiler_params=pltpu.CompilerParams(vmem_limit_bytes=32 * 1024 * 1024),
        cost_estimate=pl.CostEstimate(flops=10 ** 9, bytes_accessed=5 * 10 ** 7, transcendentals=0),
    )(lens, *arrays)


PLANS = ((8, 4, 4, 3, 2, 2, 1, 1), (8, 7, 4, 3, 2, 2, 2, 1), (8, 8, 5, 4, 3, 2, 2, 1), (8, 8, 7, 5, 4, 3, 2, 2), (NC,) * ND)


def solution(mesh):
    def per_device(tokens, seq_lens, cot, wqkv, wo, w1, w2, g1, g2):
        lt = jnp.broadcast_to(seq_lens.reshape(1, 1), (8, C2))
        wqkv, wo, w1, w2 = wqkv[0], wo[0], w1[0], w2[0]
        y, cot_all, lens, qkv, h, cx, u, lse, wqkv_t, wo_t, w1_t, w2_t = forward(tokens[0], cot[0], lt, wqkv, wo, w1, w2, g1, g2)
        pick, qkv, h, u, lse, cot_all, cx = pack(PLANS, lens[:, 0, 0], qkv, h, u, lse, cot_all.reshape(NT_ALL, C, D), cx)

        def wgrad(x, dy):
            return lax.dot_general(x, dy, TN, preferred_element_type=f32)[None]

        def branch(i):
            def run(cot_all, qkv, h, u, lse, cx, wqkv_t, wo_t, w1, w1_t, w2_t, g1, g2):
                z, dpre, d16, a2, a, dmid, dqkv, gg1, gg2 = backward(
                    PLANS[i], i + 1, cot_all, qkv, h, u, lse, wqkv_t, wo_t, w1, w1_t, w2_t, g1, g2)
                cx = cx[:sum(PLANS[i])].reshape(-1, D)
                return (wgrad(a, dqkv), wgrad(cx, dmid), wgrad(a2, dpre), wgrad(z, d16),
                        jnp.sum(gg1, axis=0, keepdims=True), jnp.sum(gg2, axis=0, keepdims=True))
            return run

        return (y[None],) + lax.switch(pick[0], [branch(i) for i in range(len(PLANS))],
                                       cot_all, qkv, h, u, lse, cx, wqkv_t, wo_t, w1, w1_t, w2_t, g1, g2)

    spec = P('stage')
    return jax.shard_map(per_device, mesh=mesh, in_specs=(spec,) * 9, out_specs=(spec,) * 7, check_vma=False)
```

```python
import functools
import jax
import jax.numpy as jnp
from jax import lax
from jax.experimental import pallas as pl
from jax.experimental.pallas import tpu as pltpu
from jax.sharding import PartitionSpec as P

bf16, f32 = jnp.bfloat16, jnp.float32
EPS = 1e-5
NEG = -1e30
BIG = 1e30
NT = (((1,), (1,)), ((), ()))
MESH = pl.DeviceIdType.MESH
S, D, F, NH = 1024, 512, 2048, 8
C = 128
C2 = 2 * C
NC = S // C
NP = 4
KB = 128
ND = 8
LAST = ND - 1
NT_ALL = ND * NC
CF = 256
NF = S // CF
HALVES = CF // C
LOG2E = 1.4426950408889634


def rms(h, g):
    r = lax.rsqrt(jnp.mean(h * h, axis=-1, keepdims=True) + EPS)
    return (h * r * g).astype(bf16)


def gelu(x):
    t = jnp.tanh(x * (0.7978845608028654 + 0.7978845608028654 * 0.044715 * (x * x)))
    hx = 0.5 * x
    return hx * t + hx


def fwd_kernel(tok, cot, ltile, wqkv, wo, w1, w2, g1, g2,
               y, cot_all, lens, sv_qkv, sv_h, sv_cx, sv_u, sv_lse, wqkv_t, wo_t, w1_t, w2_t,
               hbuf, st, cx_s, u_s, o_s, lse_s, k_s, vt_s, ct_s, mask_s, causal, e_s, p_s, t1, t2, t3, t4,
               recv_sem, send_sem, tok_sem, len_ssem, len_rsem, cot_ssem, cot_rsem, y_sem, loc_sem, yl_sem, wt_sem):
    me = lax.axis_index('stage')

    barrier = pltpu.get_barrier_semaphore()
    for k in range(1, ND):
        pl.semaphore_signal(barrier, inc=1, device_id=(lax.rem(me + k, ND),), device_id_type=MESH)
    pl.semaphore_wait(barrier, ND - 1)

    def tok_copy(c):
        return pltpu.make_async_remote_copy(
            src_ref=tok.at[pl.ds(c * CF, CF)], dst_ref=hbuf.at[me * NF + c], send_sem=tok_sem.at[c],
            recv_sem=recv_sem.at[me * NF + c], device_id=(0,), device_id_type=MESH)

    def tok_local(c):
        return pltpu.make_async_copy(tok.at[pl.ds(c * CF, CF)], hbuf.at[c], recv_sem.at[c])

    def len_copy(k):
        return pltpu.make_async_remote_copy(
            src_ref=ltile, dst_ref=lens.at[me], send_sem=len_ssem.at[k - 1], recv_sem=len_rsem.at[me],
            device_id=(lax.rem(me + k, ND),), device_id_type=MESH)

    def len_wait(m):
        pltpu.make_async_remote_copy(
            src_ref=ltile, dst_ref=lens.at[m], send_sem=len_ssem.at[0], recv_sem=len_rsem.at[m],
            device_id=(0,), device_id_type=MESH).wait_recv()

    def cot_copy(m):
        return pltpu.make_async_remote_copy(
            src_ref=cot, dst_ref=cot_all.at[m], send_sem=cot_ssem.at[0], recv_sem=cot_rsem.at[m],
            device_id=(LAST,), device_id_type=MESH)

    def cot_local():
        return pltpu.make_async_copy(cot, cot_all.at[LAST], cot_ssem.at[0])

    def pass_copy(t, slot):
        return pltpu.make_async_remote_copy(
            src_ref=o_s.at[slot], dst_ref=hbuf.at[t], send_sem=send_sem.at[slot], recv_sem=recv_sem.at[t],
            device_id=(lax.rem(me + 1, ND),), device_id_type=MESH)

    def y_copy(m, c):
        return pltpu.make_async_remote_copy(
            src_ref=o_s.at[c % 2], dst_ref=y.at[pl.ds(c * CF, CF)], send_sem=send_sem.at[c % 2],
            recv_sem=y_sem.at[c], device_id=(m,), device_id_type=MESH)

    def y_local(c):
        return pltpu.make_async_copy(o_s.at[c % 2], y.at[pl.ds(c * CF, CF)], yl_sem.at[c % 2])

    def saves(m, c):
        t, slot = m * NF + c, c % 2
        return [
            pltpu.make_async_copy(st.at[slot], sv_qkv.at[t], loc_sem.at[slot, 0]),
            pltpu.make_async_copy(hbuf.at[t], sv_h.at[t], loc_sem.at[slot, 1]),
            pltpu.make_async_copy(cx_s.at[slot], sv_cx.at[t], loc_sem.at[slot, 2]),
            pltpu.make_async_copy(u_s.at[slot], sv_u.at[t], loc_sem.at[slot, 3]),
            pltpu.make_async_copy(lse_s.at[slot], sv_lse.at[t], loc_sem.at[slot, 4]),
        ]

    def out_wait(m, c):
        @pl.when(me < LAST)
        def _():
            pass_copy(m * NF + c, c % 2).wait_send()

        @pl.when(me == LAST)
        def _():
            @pl.when(m < LAST)
            def _():
                y_copy(m, c).wait_send()

            @pl.when(m == LAST)
            def _():
                y_local(c).wait()

    @pl.when(me == 0)
    def _():
        for c in range(NF):
            tok_local(c).start()

    @pl.when(jnp.logical_and(me > 0, me < 3))
    def _():
        for c in range(NF):
            tok_copy(c).start()

    turned = [pltpu.make_async_copy(a, b, wt_sem.at[i])
              for i, (a, b) in enumerate(((t1, wqkv_t), (t2, wo_t), (t3, w1_t), (t4, w2_t)))]

    def turn_weights():
        for src, dst in ((wqkv, t1), (wo, t2), (w1, t3), (w2, t4)):
            def block(i, carry, src=src, dst=dst):
                at = pl.ds(pl.multiple_of(i * 128, 128), 128)
                dst[at] = src[:, at].T
                return carry
            lax.fori_loop(0, src.shape[1] // 128, block, 0)
        for cp in turned:
            cp.start()

    for k in range(1, ND):
        len_copy(k).start()
    lens[me] = ltile[...]
    causal[...] = jnp.where(lax.broadcasted_iota(jnp.int32, (C, C2), 0)
                            <= lax.rem(lax.broadcasted_iota(jnp.int32, (C, C2), 1), C), 0.0, NEG)

    @pl.when(me >= 4)
    def _():
        turn_weights()

    def step(m, c):
        t, slot = m * NF + c, c % 2

        if c == 0:
            @pl.when(m != me)
            def _():
                len_wait(m)

        @pl.when(jnp.logical_and(me == 0, m == 0))
        def _():
            tok_local(c).wait()

        @pl.when(jnp.logical_or(me > 0, m > 0))
        def _():
            pass_copy(t, slot).wait_recv()

        if c == 0:
            @pl.when(jnp.logical_and(me > 2, m == 0))
            def _():
                for i in range(NF):
                    tok_copy(i).start()

        def reuse(mm):
            for cp in saves(mm, (c - 2) % NF):
                cp.wait()
            out_wait(mm, (c - 2) % NF)

        if c < 2:
            @pl.when(m > 0)
            def _():
                reuse(m - 1)
        else:
            reuse(m)

        h = hbuf[t].astype(f32)
        a = rms(h, g1[...].astype(f32))
        q = jnp.dot(a, wqkv[:, :D], preferred_element_type=f32)
        kk = jnp.dot(a, wqkv[:, D:2 * D], preferred_element_type=f32).astype(bf16)
        vv = jnp.dot(a, wqkv[:, 2 * D:], preferred_element_type=f32).astype(bf16)
        q = (q * 0.125).astype(bf16)
        own = slice(c * CF, (c + 1) * CF)
        for p in range(NP):
            lanes = slice(p * 128, (p + 1) * 128)
            for j in range(HALVES):
                rows = slice(j * C, (j + 1) * C)
                st[slot, j, p] = q[rows, lanes]
                st[slot, j, NP + p] = kk[rows, lanes]
                st[slot, j, 2 * NP + p] = vv[rows, lanes]
            k_s[p, own] = kk[:, lanes]
            vt_s[p, :, own] = vv[:, lanes].T
        ln = lens[m][0:1, :]
        key = lax.broadcasted_iota(jnp.int32, (CF, 128), 0) + c * CF
        off = jnp.logical_and(key >= ln[:, :128], lax.broadcasted_iota(jnp.int32, (CF, 128), 1) == 0)
        mask_s[own] = jnp.where(off, NEG, 0.0).astype(bf16)

        half = lax.broadcasted_iota(jnp.int32, (128, C), 0) < 64
        one = jnp.where(lax.broadcasted_iota(jnp.int32, (128, C2), 0) == 0, 1.0, 0.0).astype(bf16)

        def attend(j):
            i = c * HALVES + j
            nk = (i + 1) * C

            def scores(p):
                qt = q[j * C:(j + 1) * C, p * 128:(p + 1) * 128].T
                zero = jnp.zeros_like(qt)
                qt = jnp.concatenate([jnp.where(half, qt, zero), jnp.where(half, zero, qt)], axis=1)
                qt = jnp.concatenate([qt, one], axis=0)
                top = None
                for b in range(i + 1):
                    ks = slice(b * C, (b + 1) * C)
                    s = jnp.dot(jnp.concatenate([k_s[p, ks], mask_s[ks]], axis=1), qt, preferred_element_type=f32)
                    if b == i:
                        s = s + causal[...]
                    mb = jnp.max(s.reshape(C // 8, 8, C2), axis=0)
                    top = mb if top is None else jnp.maximum(top, mb)
                    e_s[p, ks] = s
                return jnp.max(top, axis=0, keepdims=True)

            def exps(p, top):
                total = None
                top2 = top * LOG2E
                for b in range(i + 1):
                    ks = slice(b * C, (b + 1) * C)
                    e = jnp.exp2(e_s[p, ks] * LOG2E - top2)
                    sb = jnp.sum(e.reshape(C // 8, 8, C2), axis=0)
                    total = sb if total is None else total + sb
                    e_s[p, ks] = e
                total = jnp.sum(total, axis=0, keepdims=True)
                here = (lax.rem(lax.broadcasted_iota(jnp.int32, (1, C2), 1), C) + i * C) < ln
                lse_s[slot, j, p:p + 1] = jnp.where(here, top + jnp.log(total), BIG)
                return 1.0 / total

            def context(p, inv):
                for b in range(i + 1):
                    ks = slice(b * C, (b + 1) * C)
                    p_s[p, ks] = (e_s[p, ks] * inv).astype(bf16)
                o = jnp.dot(vt_s[p, :, 0:nk], p_s[p, 0:nk], preferred_element_type=f32)
                ct_s[p, 0:64, j * C:(j + 1) * C] = o[0:64, 0:C].astype(bf16)
                ct_s[p, 64:128, j * C:(j + 1) * C] = o[64:128, C:C2].astype(bf16)

            tops = [scores(p) for p in range(NP)]
            invs = [exps(p, tops[p]) for p in range(NP)]
            for p in range(NP):
                context(p, invs[p])

        for j in range(HALVES):
            attend(j)
        cx = jnp.concatenate([ct_s[p].T for p in range(NP)], axis=1)
        cx_s[slot] = cx
        u = (h + jnp.dot(cx, wo[...], preferred_element_type=f32)).astype(bf16)
        u_s[slot] = u
        for cp in saves(m, c):
            cp.start()
        u = u.astype(f32)
        a2 = rms(u, g2[...].astype(f32))
        z = gelu(jnp.dot(a2, w1[...], preferred_element_type=f32)).astype(bf16)
        o_s[slot] = (u + jnp.dot(z, w2[...], preferred_element_type=f32)).astype(bf16)

        @pl.when(me < LAST)
        def _():
            pass_copy(t, slot).start()

        @pl.when(me == LAST)
        def _():
            @pl.when(m < LAST)
            def _():
                y_copy(m, c).start()

            @pl.when(m == LAST)
            def _():
                y_local(c).start()

    def seq(m, carry):
        @pl.when(m == 2)
        def _():
            @pl.when(me < LAST)
            def _():
                cot_copy(me).start()

            @pl.when(me == LAST)
            def _():
                cot_local().start()

        for c in range(NF):
            step(m, c)
        return carry

    lax.fori_loop(0, ND, seq, 0)

    @pl.when(me < 4)
    def _():
        turn_weights()

    for cp in turned:
        cp.wait()
    for c in (NF - 2, NF - 1):
        for cp in saves(LAST, c):
            cp.wait()
        out_wait(LAST, c)
    for k in range(1, ND):
        len_copy(k).wait_send()

    @pl.when(me > 0)
    def _():
        for c in range(NF):
            tok_copy(c).wait_send()

    @pl.when(me < LAST)
    def _():
        cot_copy(me).wait_send()
        for c in range(NF):
            y_copy(0, c).wait_recv()

    @pl.when(me == LAST)
    def _():
        cot_local().wait()
        for m in range(LAST):
            cot_copy(m).wait_recv()


def forward(tok, cot, ltile, wqkv, wo, w1, w2, g1, g2):
    V = pl.BlockSpec(memory_space=pltpu.VMEM)
    A = pl.BlockSpec(memory_space=pltpu.HBM)
    dma = pltpu.SemaphoreType.DMA
    sd = jax.ShapeDtypeStruct
    return pl.pallas_call(
        fwd_kernel,
        out_shape=(sd((S, D), bf16), sd((ND, S, D), bf16), sd((ND, 8, C2), jnp.int32),
                   sd((ND * NF, HALVES, 3 * NP, C, 128), bf16), sd((ND * NF, CF, D), bf16), sd((ND * NF, CF, D), bf16),
                   sd((ND * NF, CF, D), bf16), sd((ND * NF, HALVES, NP, C2), f32), sd((3 * D, D), bf16), sd((D, D), bf16), sd((F, D), bf16), sd((D, F), bf16)),
        in_specs=[A] + [V] * 8,
        out_specs=(A, A, V) + (A,) * 9,
        scratch_shapes=[
            pltpu.VMEM((ND * NF, CF, D), bf16), pltpu.VMEM((2, HALVES, 3 * NP, C, 128), bf16), pltpu.VMEM((2, CF, D), bf16),
            pltpu.VMEM((2, CF, D), bf16), pltpu.VMEM((2, CF, D), bf16), pltpu.VMEM((2, HALVES, NP, C2), f32),
            pltpu.VMEM((NP, S, 128), bf16), pltpu.VMEM((NP, 128, S), bf16), pltpu.VMEM((NP, 128, CF), bf16),
            pltpu.VMEM((S, 128), bf16), pltpu.VMEM((C, C2), f32), pltpu.VMEM((NP, S, C2), f32), pltpu.VMEM((NP, S, C2), bf16),
            pltpu.VMEM((3 * D, D), bf16), pltpu.VMEM((D, D), bf16), pltpu.VMEM((F, D), bf16), pltpu.VMEM((D, F), bf16),
            dma((ND * NF,)), dma((2,)), dma((NF,)), dma((ND - 1,)), dma((ND,)), dma((1,)), dma((ND,)), dma((NF,)),
            dma((2, 5)), dma((2,)), dma((4,))],
        compiler_params=pltpu.CompilerParams(collective_id=0, has_side_effects=True, vmem_limit_bytes=48 * 1024 * 1024),
        cost_estimate=pl.CostEstimate(flops=80 * 10 ** 9, bytes_accessed=10 ** 8, transcendentals=10 ** 7),
    )(tok, cot, ltile, wqkv, wo, w1, w2, g1, g2)

TN = (((0,), (0,)), ((), ()))
K0 = 0.7978845608028654
K1 = K0 * 0.044715


def bwd_kernel(sizes, cot_all, sv_qkv, sv_h, sv_u, sv_lse, wqkv_t, wo_t, w1, w1_t, w2_t, g1, g2,
               z_o, dpre_o, d16_o, a2_o, a_o, dmid_o, dqkv_o, gg1_o, gg2_o,
               dbuf, cbuf, qkv_b, h_b, u_b, lse_b, kt_s, dk_s, dv_s,
               z_s, dpre_s, d16_s, a2_s, a_s, dmid_s, dqkv_s, o_s, qm_s, qt_s, dm_s, dt_s, p_s, dp_s, dsum_s, dqt_s,
               recv_sem, send_sem, ld_sem, st_sem):
    me = lax.axis_index('stage')
    barrier = pltpu.get_barrier_semaphore()
    pl.semaphore_signal(barrier, inc=1, device_id=(lax.rem(me + 1, ND),), device_id_type=MESH)
    pl.semaphore_wait(barrier, 1)
    starts = [sum(sizes[:i]) for i in range(len(sizes))]
    total = sum(sizes)

    def loads(r, par):
        dst, src = pl.ds(0, sizes[r]), pl.ds(starts[r], sizes[r])
        pairs = [(sv_qkv, qkv_b), (sv_h, h_b), (sv_u, u_b), (sv_lse, lse_b), (cot_all, cbuf)]
        return [pltpu.make_async_copy(a.at[src], b.at[par, dst], ld_sem.at[par, i]) for i, (a, b) in enumerate(pairs)]

    def stores(row, slot):
        rows = pl.ds(row, C)
        pairs = [(z_s, z_o), (dpre_s, dpre_o), (d16_s, d16_o), (a2_s, a2_o), (a_s, a_o), (dmid_s, dmid_o), (dqkv_s, dqkv_o)]
        return [pltpu.make_async_copy(s.at[slot], o.at[rows], st_sem.at[slot, i]) for i, (s, o) in enumerate(pairs)]

    def send(t, slot):
        return pltpu.make_async_remote_copy(
            src_ref=o_s.at[slot], dst_ref=dbuf.at[t], send_sem=send_sem.at[slot], recv_sem=recv_sem.at[t],
            device_id=(lax.rem(me + ND - 1, ND),), device_id_type=MESH)

    for cp in loads(0, 0):
        cp.start()
    gg1_o[...] = jnp.zeros_like(gg1_o)
    gg2_o[...] = jnp.zeros_like(gg2_o)
    dk_s[...] = jnp.zeros_like(dk_s)
    dv_s[...] = jnp.zeros_like(dv_s)
    causal = lax.broadcasted_iota(jnp.int32, (C, C2), 0) <= lax.rem(lax.broadcasted_iota(jnp.int32, (C, C2), 1), C)
    lane = lax.broadcasted_iota(jnp.int32, (C, 128), 1) < 64

    def stack(x):
        zero = jnp.zeros_like(x)
        return jnp.concatenate([jnp.where(lane, x, zero), jnp.where(lane, zero, x)], axis=0)

    def step(t, carry):
        r, n, first = 0, sizes[0], 0
        for i in range(1, len(sizes)):
            past = (t + 1024 - starts[i]) // 1024
            r = r + past
            n = n + past * (sizes[i] - sizes[i - 1])
            first = first + past * (starts[i] - starts[i - 1])
        c = n - 1 - (t - first)
        par, slot = lax.rem(r, 2), lax.rem(t, 2)
        row0 = pl.multiple_of((first + c) * C, C)
        rows = pl.ds(pl.multiple_of(c * C, C), C)

        for i in range(len(sizes)):
            @pl.when(t == starts[i])
            def _(i=i):
                for cp in loads(i, i % 2):
                    cp.wait()
                if i + 1 < len(sizes):
                    for cp in loads(i + 1, (i + 1) % 2):
                        cp.start()

                def turn(j, carry):
                    for p in range(NP):
                        kt_s[p, :, pl.ds(pl.multiple_of(j * C, C), C)] = qkv_b[i % 2, j, NP + p].T
                    return carry
                lax.fori_loop(0, sizes[i], turn, 0)

        @pl.when(t >= 2)
        def _():
            for cp in stores(0, slot):
                cp.wait()

            @pl.when(me > 0)
            def _():
                send(t, slot).wait_send()

        @pl.when(me == LAST)
        def _():
            dbuf[t] = cbuf[par, c].astype(f32)

        u = u_b[par, c].astype(f32)
        gm2 = g2[...].astype(f32)
        r2 = lax.rsqrt(jnp.mean(u * u, axis=-1, keepdims=True) + EPS)
        su = u * r2
        a2 = (su * gm2).astype(bf16)
        a2_s[slot] = a2
        for p in range(NP):
            qm = stack(qkv_b[par, c, p])
            qm_s[p] = qm
            qt_s[p] = qm.T

        @pl.when(me < LAST)
        def _():
            send(t, slot).wait_recv()

        d = dbuf[t]
        d16 = d.astype(bf16)
        d16_s[slot] = d16
        FB = 512
        for fb in range(F // FB):
            cols = slice(fb * FB, (fb + 1) * FB)
            x = jnp.dot(a2, w1[:, cols], preferred_element_type=f32)
            dz = jnp.dot(d16, w2_t[:, cols], preferred_element_type=f32)
            x2 = x * x
            th = jnp.tanh(x * (K0 + K1 * x2))
            hx = 0.5 * x
            z_s[slot, :, cols] = (hx * th + hx).astype(bf16)
            gp = (0.5 + 0.5 * th) + hx * (1.0 - th * th) * (K0 + 3.0 * K1 * x2)
            dpre_s[slot, :, cols] = (dz * gp).astype(bf16)
        da2 = jnp.dot(dpre_s[slot], w1_t[...], preferred_element_type=f32)
        gg2_o[...] += jnp.sum((da2 * su).reshape(C // 8, 8, D), axis=0)
        gd = da2 * gm2
        dmid = d + r2 * (gd - su * jnp.mean(gd * su, axis=-1, keepdims=True))
        dmid16 = dmid.astype(bf16)
        dmid_s[slot] = dmid16
        o_s[slot] = dmid
        dc = jnp.dot(dmid16, wo_t[...], preferred_element_type=f32).astype(bf16)
        for p in range(NP):
            dm = stack(dc[:, p * 128:(p + 1) * 128])
            dm_s[p] = dm
            dt_s[p] = dm.T
        dsum_s[...] = jnp.zeros_like(dsum_s)
        dqt_s[...] = jnp.zeros_like(dqt_s)

        def scores(b, diagonal):
            for p in range(NP):
                s = jnp.dot(qkv_b[par, b, NP + p], qt_s[p], preferred_element_type=f32) * LOG2E - lse_b[par, c, p:p + 1] * LOG2E
                if diagonal:
                    s = jnp.where(causal, s, NEG)
                pr = jnp.exp2(s)
                dp = jnp.dot(qkv_b[par, b, 2 * NP + p], dt_s[p], preferred_element_type=f32)
                dsum_s[p] += jnp.sum((pr * dp).reshape(C // 8, 8, C2), axis=0)
                p_s[b, p] = pr
                dp_s[b, p] = dp

        def grads(b):
            ks = pl.ds(pl.multiple_of(b * C, C), C)
            for p in range(NP):
                pr = p_s[b, p]
                ds = (pr * (dp_s[b, p] - jnp.sum(dsum_s[p], axis=0, keepdims=True))).astype(bf16)
                dv_s[p, ks] += jnp.dot(pr.astype(bf16), dm_s[p], preferred_element_type=f32)
                dk_s[p, ks] += jnp.dot(ds, qm_s[p], preferred_element_type=f32)
                dqt = jnp.dot(kt_s[p, :, ks], ds, preferred_element_type=f32)
                dqt_s[p, 0:64] += dqt[0:64, 0:C]
                dqt_s[p, 64:128] += dqt[64:128, C:C2]

        def loop1(b, carry):
            scores(b, False)
            return carry

        def loop2(b, carry):
            grads(b)
            return carry

        lax.fori_loop(0, c, loop1, 0)
        scores(c, True)
        grads(c)
        lax.fori_loop(0, c, loop2, 0)

        for p in range(NP):
            for i, val in enumerate((dqt_s[p].T * 0.125, dk_s[p, rows], dv_s[p, rows])):
                dqkv_s[slot, :, i * D + p * 128:i * D + (p + 1) * 128] = val.astype(bf16)
            dk_s[p, rows] = jnp.zeros((C, 128), f32)
            dv_s[p, rows] = jnp.zeros((C, 128), f32)
        da = jnp.dot(dqkv_s[slot], wqkv_t[...], preferred_element_type=f32)
        h = h_b[par, c].astype(f32)
        gm1 = g1[...].astype(f32)
        r1 = lax.rsqrt(jnp.mean(h * h, axis=-1, keepdims=True) + EPS)
        sh = h * r1
        a_s[slot] = (sh * gm1).astype(bf16)
        gg1_o[...] += jnp.sum((da * sh).reshape(C // 8, 8, D), axis=0)
        gd = da * gm1
        o_s[slot] += r1 * (gd - sh * jnp.mean(gd * sh, axis=-1, keepdims=True))
        for cp in stores(row0, slot):
            cp.start()

        @pl.when(me > 0)
        def _():
            send(t, slot).start()
        return carry

    lax.fori_loop(0, total, step, 0)
    for t in (total - 2, total - 1):
        for cp in stores(0, t % 2):
            cp.wait()

        @pl.when(me > 0)
        def _():
            send(t, t % 2).wait_send()


def backward(sizes, cid, cot_all, sv_qkv, sv_h, sv_u, sv_lse, wqkv_t, wo_t, w1, w1_t, w2_t, g1, g2):
    V = pl.BlockSpec(memory_space=pltpu.VMEM)
    A = pl.BlockSpec(memory_space=pltpu.HBM)
    dma = pltpu.SemaphoreType.DMA
    sd = jax.ShapeDtypeStruct
    T = sum(sizes)
    R = NT_ALL * C
    VM = pltpu.VMEM
    return pl.pallas_call(
        functools.partial(bwd_kernel, sizes),
        out_shape=(sd((R, F), bf16), sd((R, F), bf16), sd((R, D), bf16), sd((R, D), bf16), sd((R, D), bf16), sd((R, D), bf16),
                   sd((R, 3 * D), bf16), sd((8, D), f32), sd((8, D), f32)),
        in_specs=[A] * 5 + [V] * 7,
        out_specs=(A,) * 7 + (V, V),
        scratch_shapes=[
            VM((T, C, D), f32), VM((2, NC, C, D), bf16), VM((2, NC, 3 * NP, C, 128), bf16), VM((2, NC, C, D), bf16), VM((2, NC, C, D), bf16),
            VM((2, NC, NP, C2), f32), VM((NP, 128, S), bf16), VM((NP, S, 128), f32), VM((NP, S, 128), f32),
            VM((2, C, F), bf16), VM((2, C, F), bf16), VM((2, C, D), bf16), VM((2, C, D), bf16), VM((2, C, D), bf16),
            VM((2, C, D), bf16), VM((2, C, 3 * D), bf16), VM((2, C, D), f32),
            VM((NP, C2, 128), bf16), VM((NP, 128, C2), bf16), VM((NP, C2, 128), bf16), VM((NP, 128, C2), bf16),
            VM((NC, NP, C, C2), f32), VM((NC, NP, C, C2), f32), VM((NP, 8, C2), f32), VM((NP, 128, C), f32),
            dma((T,)), dma((2,)), dma((2, 5)), dma((2, 7))],
        compiler_params=pltpu.CompilerParams(collective_id=cid, has_side_effects=True, vmem_limit_bytes=61 * 1024 * 1024),
        cost_estimate=pl.CostEstimate(flops=80 * 10 ** 9, bytes_accessed=10 ** 8, transcendentals=10 ** 7),
    )(cot_all, sv_qkv, sv_h, sv_u, sv_lse, wqkv_t, wo_t, w1, w1_t, w2_t, g1, g2)


def pack_kernel(plans, lens, qkv, h, u, lse, cot, pick_o, src, qkv_o, h_o, u_o, lse_o, cot_o,
                qkv_b, h_b, u_b, lse_b, cot_b, order, ld_sem, st_sem):
    for m in range(ND):
        rank = 0
        for k in range(ND):
            longer = lens[k] > lens[m] if k >= m else lens[k] >= lens[m]
            rank = rank + jnp.where(longer, 1, 0)
        order[rank] = m
    pick = len(plans) - 1
    for i in reversed(range(len(plans) - 1)):
        fits = True
        for r in range(ND):
            fits = jnp.logical_and(fits, lens[order[r]] <= plans[i][r] * C)
        pick = jnp.where(fits, i, pick)
    pick_o[0] = pick
    count = 0
    for r in range(ND):
        n = 0
        for i, plan in enumerate(plans):
            n = n + jnp.where(pick == i, plan[r], 0)

        def put(j, carry, count=count, r=r):
            src[count + j] = order[r] * NC + j
            return carry
        lax.fori_loop(0, n, put, 0)
        count = count + n
    pick_o[1] = count
    arrays = ((qkv, qkv_b, qkv_o), (h, h_b, h_o), (u, u_b, u_o), (lse, lse_b, lse_o), (cot, cot_b, cot_o))

    def load(t):
        s = lax.rem(t, RING)
        return [pltpu.make_async_copy(a.at[src[t]], b.at[s], ld_sem.at[s, i]) for i, (a, b, _) in enumerate(arrays)]

    def store(t):
        s = lax.rem(t, RING)
        return [pltpu.make_async_copy(b.at[s], o.at[t], st_sem.at[s, i]) for i, (_, b, o) in enumerate(arrays)]

    lag = RING // 2

    def go(t, carry):
        @pl.when(t < count)
        def _():
            @pl.when(t >= RING)
            def _():
                for cp in store(t - RING):
                    cp.wait()
            for cp in load(t):
                cp.start()

        @pl.when(t >= lag)
        def _():
            for cp in load(t - lag):
                cp.wait()
            for cp in store(t - lag):
                cp.start()
        return carry

    lax.fori_loop(0, count + lag, go, 0)

    def drain(t, carry):
        for cp in store(t):
            cp.wait()
        return carry

    lax.fori_loop(jnp.maximum(count - RING, 0), count, drain, 0)


RING = 16


def pack(plans, lens, *arrays):
    A = pl.BlockSpec(memory_space=pltpu.HBM)
    SM = pl.BlockSpec(memory_space=pltpu.SMEM)
    sd = jax.ShapeDtypeStruct
    return pl.pallas_call(
        functools.partial(pack_kernel, plans),
        out_shape=(sd((2,), jnp.int32), sd((NT_ALL,), jnp.int32)) + tuple(sd(a.shape, a.dtype) for a in arrays),
        in_specs=[SM] + [A] * 5,
        out_specs=(SM, SM) + (A,) * 5,
        scratch_shapes=[pltpu.VMEM((RING,) + a.shape[1:], a.dtype) for a in arrays] + [
            pltpu.SMEM((ND,), jnp.int32), pltpu.SemaphoreType.DMA((RING, 5)), pltpu.SemaphoreType.DMA((RING, 5))],
        compiler_params=pltpu.CompilerParams(vmem_limit_bytes=60 * 1024 * 1024),
        cost_estimate=pl.CostEstimate(flops=10 ** 9, bytes_accessed=5 * 10 ** 7, transcendentals=0),
    )(lens, *arrays)


def wgrad_kernel(pick, src, a, cx, a2, z, dqkv, dmid, dpre, d16, gg1, gg2,
                 g_qkv, g_out, g_up, g_down, g_g1, g_g2,
                 a_b, cx_b, a2_b, z_b, dqkv_b, dmid_b, dpre_b, d16_b, s_qkv, s_out, s_up, s_down, ld_sem, st_sem):
    count = pick[1]
    blocks = (count + 1) // 2
    bufs = ((a, a_b), (a2, a2_b), (z, z_b), (dqkv, dqkv_b), (dmid, dmid_b), (dpre, dpre_b), (d16, d16_b))

    def load(i, j, par):
        t = 2 * i + j
        rows = pl.ds(j * C, C)
        cps = [pltpu.make_async_copy(x.at[pl.ds(pl.multiple_of(t * C, C), C)], b.at[par, rows], ld_sem.at[par, j, k])
               for k, (x, b) in enumerate(bufs)]
        return cps + [pltpu.make_async_copy(cx.at[src[t]], cx_b.at[par, rows], ld_sem.at[par, j, len(bufs)])]

    def each(i, par, what):
        for cp in load(i, 0, par):
            what(cp)

        @pl.when(2 * i + 1 < count)
        def _():
            for cp in load(i, 1, par):
                what(cp)

    each(0, 0, lambda cp: cp.start())
    g_g1[...] = jnp.sum(gg1[...], axis=0, keepdims=True)
    g_g2[...] = jnp.sum(gg2[...], axis=0, keepdims=True)
    work = ((z_b, d16_b, s_down, g_down), (a2_b, dpre_b, s_up, g_up), (a_b, dqkv_b, s_qkv, g_qkv), (cx_b, dmid_b, s_out, g_out))
    for _, _, acc, _ in work:
        acc[...] = jnp.zeros_like(acc)

    def block(i, carry):
        par = lax.rem(i, 2)

        @pl.when(i + 1 < blocks)
        def _():
            each(i + 1, 1 - par, lambda cp: cp.start())
        each(i, par, lambda cp: cp.wait())

        @pl.when(2 * i + 1 == count)
        def _():
            for _, y, _, _ in work:
                y[par, C:] = jnp.zeros((C, y.shape[2]), bf16)
            for x, _, _, _ in work:
                x[par, C:] = jnp.zeros((C, x.shape[2]), bf16)
        for k, (x, y, acc, out) in enumerate(work):
            for m in range(0, acc.shape[0], 512):
                xt = x[par, :, m:m + 512].T
                for n in range(0, acc.shape[1], 512):
                    acc[m:m + 512, n:n + 512] += jnp.dot(xt, y[par, :, n:n + 512], preferred_element_type=f32)

            @pl.when(i + 1 == blocks)
            def _():
                pltpu.make_async_copy(acc, out, st_sem.at[k]).start()
        return carry

    lax.fori_loop(0, blocks, block, 0)
    for k, (_, _, acc, out) in enumerate(work):
        pltpu.make_async_copy(acc, out, st_sem.at[k]).wait()


def wgrad(pick, src, a, cx, a2, z, dqkv, dmid, dpre, d16, gg1, gg2):
    A = pl.BlockSpec(memory_space=pltpu.HBM)
    SM = pl.BlockSpec(memory_space=pltpu.SMEM)
    V = pl.BlockSpec(memory_space=pltpu.VMEM)
    sd = jax.ShapeDtypeStruct
    VM = pltpu.VMEM
    widths = (D, D, D, F, 3 * D, D, F, D)
    shapes = ((D, 3 * D), (D, D), (D, F), (F, D))
    return pl.pallas_call(
        wgrad_kernel,
        out_shape=tuple(sd(s, f32) for s in shapes) + (sd((1, D), f32),) * 2,
        in_specs=[SM, SM] + [A] * 8 + [V] * 2,
        out_specs=(A,) * 4 + (V, V),
        scratch_shapes=[VM((2, 2 * C, w), bf16) for w in widths] + [VM(s, f32) for s in shapes] + [
            pltpu.SemaphoreType.DMA((2, 2, 8)), pltpu.SemaphoreType.DMA((4,))],
        compiler_params=pltpu.CompilerParams(vmem_limit_bytes=60 * 1024 * 1024),
        cost_estimate=pl.CostEstimate(flops=25 * 10 ** 9, bytes_accessed=7 * 10 ** 7, transcendentals=0),
    )(pick, src, a, cx, a2, z, dqkv, dmid, dpre, d16, gg1, gg2)


PLANS = ((8, 4, 4, 3, 2, 2, 1, 1), (8, 7, 4, 3, 2, 2, 2, 1), (8, 8, 5, 4, 3, 2, 2, 1), (8, 8, 7, 5, 4, 3, 2, 2), (NC,) * ND)


def solution(mesh):
    def per_device(tokens, seq_lens, cot, wqkv, wo, w1, w2, g1, g2):
        lt = jnp.broadcast_to(seq_lens.reshape(1, 1), (8, C2))
        wqkv, wo, w1, w2 = wqkv[0], wo[0], w1[0], w2[0]
        y, cot_all, lens, qkv, h, cx, u, lse, wqkv_t, wo_t, w1_t, w2_t = forward(tokens[0], cot[0], lt, wqkv, wo, w1, w2, g1, g2)
        qkv, lse = qkv.reshape(NT_ALL, 3 * NP, C, 128), lse.reshape(NT_ALL, NP, C2)
        h, cx, u, cot_all = (x.reshape(NT_ALL, C, D) for x in (h, cx, u, cot_all))
        pick, src, *packed = pack(PLANS, lens[:, 0, 0], qkv, h, u, lse, cot_all)

        def branch(i):
            def run(qkv, h, u, lse, cot_all, wqkv_t, wo_t, w1, w1_t, w2_t, g1, g2):
                return backward(PLANS[i], i + 1, cot_all, qkv, h, u, lse, wqkv_t, wo_t, w1, w1_t, w2_t, g1, g2)
            return run

        z, dpre, d16, a2, a, dmid, dqkv, gg1, gg2 = lax.switch(
            pick[0], [branch(i) for i in range(len(PLANS))], *packed, wqkv_t, wo_t, w1, w1_t, w2_t, g1, g2)
        g_qkv, g_out, g_up, g_down, g_g1, g_g2 = wgrad(pick, src, a, cx, a2, z, dqkv, dmid, dpre, d16, gg1, gg2)
        return y[None], g_qkv[None], g_out[None], g_up[None], g_down[None], g_g1, g_g2

    spec = P('stage')
    return jax.shard_map(per_device, mesh=mesh, in_specs=(spec,) * 9, out_specs=(spec,) * 7, check_vma=False)
```

```python
import functools
import jax
import jax.numpy as jnp
from jax import lax
from jax.experimental import pallas as pl
from jax.experimental.pallas import tpu as pltpu
from jax.sharding import PartitionSpec as P

bf16, f32 = jnp.bfloat16, jnp.float32
EPS = 1e-5
NEG = -1e30
BIG = 1e30
NT = (((1,), (1,)), ((), ()))
MESH = pl.DeviceIdType.MESH
S, D, F, NH = 1024, 512, 2048, 8
C = 128
C2 = 2 * C
NC = S // C
NP = 4
KB = 128
ND = 8
LAST = ND - 1
NT_ALL = ND * NC
CF = 256
NF = S // CF
HALVES = CF // C
LOG2E = 1.4426950408889634


def rms(h, g):
    r = lax.rsqrt(jnp.mean(h * h, axis=-1, keepdims=True) + EPS)
    return (h * r * g).astype(bf16)


def gelu(x):
    t = jnp.tanh(x * (0.7978845608028654 + 0.7978845608028654 * 0.044715 * (x * x)))
    hx = 0.5 * x
    return hx * t + hx


def fwd_kernel(tok, cot, ltile, wqkv, wo, w1, w2, g1, g2,
               y, cot_all, lens, sv_qkv, sv_h, sv_cx, sv_u, sv_lse, wqkv_t, wo_t, w1_t, w2_t,
               hbuf, st, cx_s, u_s, o_s, lse_s, k_s, vt_s, ct_s, mask_s, causal, e_s, p_s, t1, t2, t3, t4,
               recv_sem, send_sem, tok_sem, len_ssem, len_rsem, cot_ssem, cot_rsem, y_sem, loc_sem, yl_sem, wt_sem):
    me = lax.axis_index('stage')

    barrier = pltpu.get_barrier_semaphore()
    for k in range(1, ND):
        pl.semaphore_signal(barrier, inc=1, device_id=(lax.rem(me + k, ND),), device_id_type=MESH)
    pl.semaphore_wait(barrier, ND - 1)

    def tok_copy(c):
        return pltpu.make_async_remote_copy(
            src_ref=tok.at[pl.ds(c * CF, CF)], dst_ref=hbuf.at[me * NF + c], send_sem=tok_sem.at[c],
            recv_sem=recv_sem.at[me * NF + c], device_id=(0,), device_id_type=MESH)

    def tok_local(c):
        return pltpu.make_async_copy(tok.at[pl.ds(c * CF, CF)], hbuf.at[c], recv_sem.at[c])

    def len_copy(k):
        return pltpu.make_async_remote_copy(
            src_ref=ltile, dst_ref=lens.at[me], send_sem=len_ssem.at[k - 1], recv_sem=len_rsem.at[me],
            device_id=(lax.rem(me + k, ND),), device_id_type=MESH)

    def len_wait(m):
        pltpu.make_async_remote_copy(
            src_ref=ltile, dst_ref=lens.at[m], send_sem=len_ssem.at[0], recv_sem=len_rsem.at[m],
            device_id=(0,), device_id_type=MESH).wait_recv()

    def cot_copy(m):
        return pltpu.make_async_remote_copy(
            src_ref=cot, dst_ref=cot_all.at[m], send_sem=cot_ssem.at[0], recv_sem=cot_rsem.at[m],
            device_id=(LAST,), device_id_type=MESH)

    def cot_local():
        return pltpu.make_async_copy(cot, cot_all.at[LAST], cot_ssem.at[0])

    def pass_copy(t, slot):
        return pltpu.make_async_remote_copy(
            src_ref=o_s.at[slot], dst_ref=hbuf.at[t], send_sem=send_sem.at[slot], recv_sem=recv_sem.at[t],
            device_id=(lax.rem(me + 1, ND),), device_id_type=MESH)

    def y_copy(m, c):
        return pltpu.make_async_remote_copy(
            src_ref=o_s.at[c % 2], dst_ref=y.at[pl.ds(c * CF, CF)], send_sem=send_sem.at[c % 2],
            recv_sem=y_sem.at[c], device_id=(m,), device_id_type=MESH)

    def y_local(c):
        return pltpu.make_async_copy(o_s.at[c % 2], y.at[pl.ds(c * CF, CF)], yl_sem.at[c % 2])

    def saves(m, c):
        t, slot = m * NF + c, c % 2
        return [
            pltpu.make_async_copy(st.at[slot], sv_qkv.at[t], loc_sem.at[slot, 0]),
            pltpu.make_async_copy(hbuf.at[t], sv_h.at[t], loc_sem.at[slot, 1]),
            pltpu.make_async_copy(cx_s.at[slot], sv_cx.at[t], loc_sem.at[slot, 2]),
            pltpu.make_async_copy(u_s.at[slot], sv_u.at[t], loc_sem.at[slot, 3]),
            pltpu.make_async_copy(lse_s.at[slot], sv_lse.at[t], loc_sem.at[slot, 4]),
        ]

    def out_wait(m, c):
        @pl.when(me < LAST)
        def _():
            pass_copy(m * NF + c, c % 2).wait_send()

        @pl.when(me == LAST)
        def _():
            @pl.when(m < LAST)
            def _():
                y_copy(m, c).wait_send()

            @pl.when(m == LAST)
            def _():
                y_local(c).wait()

    @pl.when(me == 0)
    def _():
        for c in range(NF):
            tok_local(c).start()

    @pl.when(jnp.logical_and(me > 0, me < 3))
    def _():
        for c in range(NF):
            tok_copy(c).start()

    turned = [pltpu.make_async_copy(a, b, wt_sem.at[i])
              for i, (a, b) in enumerate(((t1, wqkv_t), (t2, wo_t), (t3, w1_t), (t4, w2_t)))]

    def turn_weights():
        for src, dst in ((wqkv, t1), (wo, t2), (w1, t3), (w2, t4)):
            def block(i, carry, src=src, dst=dst):
                at = pl.ds(pl.multiple_of(i * 128, 128), 128)
                dst[at] = src[:, at].T
                return carry
            lax.fori_loop(0, src.shape[1] // 128, block, 0)
        for cp in turned:
            cp.start()

    for k in range(1, ND):
        len_copy(k).start()
    lens[me] = ltile[...]
    causal[...] = jnp.where(lax.broadcasted_iota(jnp.int32, (C, C2), 0)
                            <= lax.rem(lax.broadcasted_iota(jnp.int32, (C, C2), 1), C), 0.0, NEG)

    @pl.when(me >= 4)
    def _():
        turn_weights()

    def step(m, c):
        t, slot = m * NF + c, c % 2

        if c == 0:
            @pl.when(m != me)
            def _():
                len_wait(m)

        @pl.when(jnp.logical_and(me == 0, m == 0))
        def _():
            tok_local(c).wait()

        @pl.when(jnp.logical_or(me > 0, m > 0))
        def _():
            pass_copy(t, slot).wait_recv()

        if c == 0:
            @pl.when(jnp.logical_and(me > 2, m == 0))
            def _():
                for i in range(NF):
                    tok_copy(i).start()

        def reuse(mm):
            for cp in saves(mm, (c - 2) % NF):
                cp.wait()
            out_wait(mm, (c - 2) % NF)

        if c < 2:
            @pl.when(m > 0)
            def _():
                reuse(m - 1)
        else:
            reuse(m)

        h = hbuf[t].astype(f32)
        a = rms(h, g1[...].astype(f32))
        q = jnp.dot(a, wqkv[:, :D], preferred_element_type=f32)
        kk = jnp.dot(a, wqkv[:, D:2 * D], preferred_element_type=f32).astype(bf16)
        vv = jnp.dot(a, wqkv[:, 2 * D:], preferred_element_type=f32).astype(bf16)
        q = (q * 0.125).astype(bf16)
        own = slice(c * CF, (c + 1) * CF)
        for p in range(NP):
            lanes = slice(p * 128, (p + 1) * 128)
            for j in range(HALVES):
                rows = slice(j * C, (j + 1) * C)
                st[slot, j, p] = q[rows, lanes]
                st[slot, j, NP + p] = kk[rows, lanes]
                st[slot, j, 2 * NP + p] = vv[rows, lanes]
            k_s[p, own] = kk[:, lanes]
            vt_s[p, :, own] = vv[:, lanes].T
        ln = lens[m][0:1, :]
        key = lax.broadcasted_iota(jnp.int32, (CF, 128), 0) + c * CF
        off = jnp.logical_and(key >= ln[:, :128], lax.broadcasted_iota(jnp.int32, (CF, 128), 1) == 0)
        mask_s[own] = jnp.where(off, NEG, 0.0).astype(bf16)

        half = lax.broadcasted_iota(jnp.int32, (128, C), 0) < 64
        one = jnp.where(lax.broadcasted_iota(jnp.int32, (128, C2), 0) == 0, 1.0, 0.0).astype(bf16)

        def attend(j):
            i = c * HALVES + j
            nk = (i + 1) * C

            def scores(p):
                qt = q[j * C:(j + 1) * C, p * 128:(p + 1) * 128].T
                zero = jnp.zeros_like(qt)
                qt = jnp.concatenate([jnp.where(half, qt, zero), jnp.where(half, zero, qt)], axis=1)
                qt = jnp.concatenate([qt, one], axis=0)
                top = None
                for b in range(i + 1):
                    ks = slice(b * C, (b + 1) * C)
                    s = jnp.dot(jnp.concatenate([k_s[p, ks], mask_s[ks]], axis=1), qt, preferred_element_type=f32)
                    if b == i:
                        s = s + causal[...]
                    mb = jnp.max(s.reshape(C // 8, 8, C2), axis=0)
                    top = mb if top is None else jnp.maximum(top, mb)
                    e_s[p, ks] = s
                return jnp.max(top, axis=0, keepdims=True)

            def exps(p, top):
                total = None
                top2 = top * LOG2E
                for b in range(i + 1):
                    ks = slice(b * C, (b + 1) * C)
                    e = jnp.exp2(e_s[p, ks] * LOG2E - top2)
                    sb = jnp.sum(e.reshape(C // 8, 8, C2), axis=0)
                    total = sb if total is None else total + sb
                    e_s[p, ks] = e
                total = jnp.sum(total, axis=0, keepdims=True)
                here = (lax.rem(lax.broadcasted_iota(jnp.int32, (1, C2), 1), C) + i * C) < ln
                lse_s[slot, j, p:p + 1] = jnp.where(here, top + jnp.log(total), BIG)
                return 1.0 / total

            def context(p, inv):
                for b in range(i + 1):
                    ks = slice(b * C, (b + 1) * C)
                    p_s[p, ks] = (e_s[p, ks] * inv).astype(bf16)
                o = jnp.dot(vt_s[p, :, 0:nk], p_s[p, 0:nk], preferred_element_type=f32)
                ct_s[p, 0:64, j * C:(j + 1) * C] = o[0:64, 0:C].astype(bf16)
                ct_s[p, 64:128, j * C:(j + 1) * C] = o[64:128, C:C2].astype(bf16)

            tops = [scores(p) for p in range(NP)]
            invs = [exps(p, tops[p]) for p in range(NP)]
            for p in range(NP):
                context(p, invs[p])

        for j in range(HALVES):
            attend(j)
        cx = jnp.concatenate([ct_s[p].T for p in range(NP)], axis=1)
        cx_s[slot] = cx
        u = (h + jnp.dot(cx, wo[...], preferred_element_type=f32)).astype(bf16)
        u_s[slot] = u
        for cp in saves(m, c):
            cp.start()
        u = u.astype(f32)
        a2 = rms(u, g2[...].astype(f32))
        z = gelu(jnp.dot(a2, w1[...], preferred_element_type=f32)).astype(bf16)
        o_s[slot] = (u + jnp.dot(z, w2[...], preferred_element_type=f32)).astype(bf16)

        @pl.when(me < LAST)
        def _():
            pass_copy(t, slot).start()

        @pl.when(me == LAST)
        def _():
            @pl.when(m < LAST)
            def _():
                y_copy(m, c).start()

            @pl.when(m == LAST)
            def _():
                y_local(c).start()

    def seq(m, carry):
        @pl.when(m == 2)
        def _():
            @pl.when(me < LAST)
            def _():
                cot_copy(me).start()

            @pl.when(me == LAST)
            def _():
                cot_local().start()

        for c in range(NF):
            step(m, c)
        return carry

    lax.fori_loop(0, ND, seq, 0)

    @pl.when(me < 4)
    def _():
        turn_weights()

    for cp in turned:
        cp.wait()
    for c in (NF - 2, NF - 1):
        for cp in saves(LAST, c):
            cp.wait()
        out_wait(LAST, c)
    for k in range(1, ND):
        len_copy(k).wait_send()

    @pl.when(me > 0)
    def _():
        for c in range(NF):
            tok_copy(c).wait_send()

    @pl.when(me < LAST)
    def _():
        cot_copy(me).wait_send()
        for c in range(NF):
            y_copy(0, c).wait_recv()

    @pl.when(me == LAST)
    def _():
        cot_local().wait()
        for m in range(LAST):
            cot_copy(m).wait_recv()


def forward(tok, cot, ltile, wqkv, wo, w1, w2, g1, g2):
    V = pl.BlockSpec(memory_space=pltpu.VMEM)
    A = pl.BlockSpec(memory_space=pltpu.HBM)
    dma = pltpu.SemaphoreType.DMA
    sd = jax.ShapeDtypeStruct
    return pl.pallas_call(
        fwd_kernel,
        out_shape=(sd((S, D), bf16), sd((ND, S, D), bf16), sd((ND, 8, C2), jnp.int32),
                   sd((ND * NF, HALVES, 3 * NP, C, 128), bf16), sd((ND * NF, CF, D), bf16), sd((ND * NF, CF, D), bf16),
                   sd((ND * NF, CF, D), bf16), sd((ND * NF, HALVES, NP, C2), f32), sd((3 * D, D), bf16), sd((D, D), bf16), sd((F, D), bf16), sd((D, F), bf16)),
        in_specs=[A] + [V] * 8,
        out_specs=(A, A, V) + (A,) * 9,
        scratch_shapes=[
            pltpu.VMEM((ND * NF, CF, D), bf16), pltpu.VMEM((2, HALVES, 3 * NP, C, 128), bf16), pltpu.VMEM((2, CF, D), bf16),
            pltpu.VMEM((2, CF, D), bf16), pltpu.VMEM((2, CF, D), bf16), pltpu.VMEM((2, HALVES, NP, C2), f32),
            pltpu.VMEM((NP, S, 128), bf16), pltpu.VMEM((NP, 128, S), bf16), pltpu.VMEM((NP, 128, CF), bf16),
            pltpu.VMEM((S, 128), bf16), pltpu.VMEM((C, C2), f32), pltpu.VMEM((NP, S, C2), f32), pltpu.VMEM((NP, S, C2), bf16),
            pltpu.VMEM((3 * D, D), bf16), pltpu.VMEM((D, D), bf16), pltpu.VMEM((F, D), bf16), pltpu.VMEM((D, F), bf16),
            dma((ND * NF,)), dma((2,)), dma((NF,)), dma((ND - 1,)), dma((ND,)), dma((1,)), dma((ND,)), dma((NF,)),
            dma((2, 5)), dma((2,)), dma((4,))],
        compiler_params=pltpu.CompilerParams(collective_id=0, has_side_effects=True, vmem_limit_bytes=48 * 1024 * 1024),
        cost_estimate=pl.CostEstimate(flops=80 * 10 ** 9, bytes_accessed=10 ** 8, transcendentals=10 ** 7),
    )(tok, cot, ltile, wqkv, wo, w1, w2, g1, g2)

TN = (((0,), (0,)), ((), ()))
UN = 4
K0 = 0.7978845608028654
K1 = K0 * 0.044715


def bwd_kernel(sizes, cot_all, sv_qkv, sv_h, sv_u, sv_lse, wqkv_t, wo_t, w1, w1_t, w2_t, g1, g2,
               z_o, dpre_o, d16_o, a2_o, a_o, dmid_o, dqkv_o, gg1_o, gg2_o,
               dbuf, cbuf, qkv_b, h_b, u_b, lse_b, kt_s, dk_s, dv_s,
               z_s, dpre_s, d16_s, a2_s, a_s, dmid_s, dqkv_s, o_s, qm_s, qt_s, dm_s, dt_s, p_s, dp_s, dsum_s, dqt_s, sh_s, r1_s,
               recv_sem, send_sem, ld_sem, st_sem):
    me = lax.axis_index('stage')
    barrier = pltpu.get_barrier_semaphore()
    pl.semaphore_signal(barrier, inc=1, device_id=(lax.rem(me + 1, ND),), device_id_type=MESH)
    pl.semaphore_wait(barrier, 1)
    starts = [sum(sizes[:i]) for i in range(len(sizes))]
    total = sum(sizes)

    def loads(r, par):
        dst, src = pl.ds(0, sizes[r]), pl.ds(starts[r], sizes[r])
        pairs = [(sv_qkv, qkv_b), (sv_h, h_b), (sv_u, u_b), (sv_lse, lse_b), (cot_all, cbuf)]
        return [pltpu.make_async_copy(a.at[src], b.at[par, dst], ld_sem.at[par, i]) for i, (a, b) in enumerate(pairs)]

    def stores(row, slot):
        rows = pl.ds(row, C)
        pairs = [(z_s, z_o), (dpre_s, dpre_o), (d16_s, d16_o), (a2_s, a2_o), (a_s, a_o), (dmid_s, dmid_o), (dqkv_s, dqkv_o)]
        return [pltpu.make_async_copy(s.at[slot], o.at[rows], st_sem.at[slot, i]) for i, (s, o) in enumerate(pairs)]

    def send(t, slot):
        return pltpu.make_async_remote_copy(
            src_ref=o_s.at[slot], dst_ref=dbuf.at[t], send_sem=send_sem.at[slot], recv_sem=recv_sem.at[t],
            device_id=(lax.rem(me + ND - 1, ND),), device_id_type=MESH)

    for cp in loads(0, 0):
        cp.start()
    gg1_o[...] = jnp.zeros_like(gg1_o)
    gg2_o[...] = jnp.zeros_like(gg2_o)
    dk_s[...] = jnp.zeros_like(dk_s)
    dv_s[...] = jnp.zeros_like(dv_s)
    causal = lax.broadcasted_iota(jnp.int32, (C, C2), 0) <= lax.rem(lax.broadcasted_iota(jnp.int32, (C, C2), 1), C)
    lane = lax.broadcasted_iota(jnp.int32, (C, 128), 1) < 64

    def stack(x):
        zero = jnp.zeros_like(x)
        return jnp.concatenate([jnp.where(lane, x, zero), jnp.where(lane, zero, x)], axis=0)

    def step(t, carry):
        r, n, first = 0, sizes[0], 0
        for i in range(1, len(sizes)):
            past = (t + 1024 - starts[i]) // 1024
            r = r + past
            n = n + past * (sizes[i] - sizes[i - 1])
            first = first + past * (starts[i] - starts[i - 1])
        c = n - 1 - (t - first)
        par, slot = lax.rem(r, 2), lax.rem(t, 2)
        row0 = pl.multiple_of((first + c) * C, C)
        rows = pl.ds(pl.multiple_of(c * C, C), C)

        for i in range(len(sizes)):
            @pl.when(t == starts[i])
            def _(i=i):
                for cp in loads(i, i % 2):
                    cp.wait()
                if i + 1 < len(sizes):
                    for cp in loads(i + 1, (i + 1) % 2):
                        cp.start()

                def turn(j, carry):
                    for p in range(NP):
                        kt_s[p, :, pl.ds(pl.multiple_of(j * C, C), C)] = qkv_b[i % 2, j, NP + p].T
                    return carry
                lax.fori_loop(0, sizes[i], turn, 0)

        @pl.when(t >= 2)
        def _():
            for cp in stores(0, slot):
                cp.wait()

            @pl.when(me > 0)
            def _():
                send(t, slot).wait_send()

        @pl.when(me == LAST)
        def _():
            dbuf[t] = cbuf[par, c].astype(f32)

        @pl.when(me < LAST)
        def _():
            send(t, slot).wait_recv()

        d = dbuf[t]
        d16 = d.astype(bf16)
        d16_s[slot] = d16
        u = u_b[par, c].astype(f32)
        gm2 = g2[...].astype(f32)
        r2 = lax.rsqrt(jnp.mean(u * u, axis=-1, keepdims=True) + EPS)
        su = u * r2
        a2 = (su * gm2).astype(bf16)
        a2_s[slot] = a2
        FB = 256

        def ups(fb):
            cols = slice(fb * FB, (fb + 1) * FB)
            dz = jnp.dot(d16, w2_t[:, cols], preferred_element_type=f32)
            return jnp.dot(a2, w1[:, cols], preferred_element_type=f32), dz

        ahead = [ups(0)]
        for fb in range(F // FB):
            cols = slice(fb * FB, (fb + 1) * FB)
            if fb + 1 < F // FB:
                ahead.append(ups(fb + 1))
            x, dz = ahead[fb]
            x2 = x * x
            sg = 0.5 + 0.5 * jnp.tanh(x * (K0 + K1 * x2))
            zz = x * sg
            z_s[slot, :, cols] = zz.astype(bf16)
            gp = sg + (zz - zz * sg) * (2.0 * K0 + 6.0 * K1 * x2)
            dpre_s[slot, :, cols] = (dz * gp).astype(bf16)
        da2 = jnp.dot(dpre_s[slot], w1_t[...], preferred_element_type=f32)
        for p in range(NP):
            qm = stack(qkv_b[par, c, p])
            qm_s[p] = qm
            qt_s[p] = qm.T
        h = h_b[par, c].astype(f32)
        gm1 = g1[...].astype(f32)
        r1 = lax.rsqrt(jnp.mean(h * h, axis=-1, keepdims=True) + EPS)
        sh = h * r1
        sh_s[...] = sh
        r1_s[...] = jnp.broadcast_to(r1, (C, 128))
        a_s[slot] = (sh * gm1).astype(bf16)
        gg2_o[...] += jnp.sum((da2 * su).reshape(C // 8, 8, D), axis=0)
        gd = da2 * gm2
        dmid = d + r2 * (gd - su * jnp.mean(gd * su, axis=-1, keepdims=True))
        dmid16 = dmid.astype(bf16)
        dmid_s[slot] = dmid16
        o_s[slot] = dmid
        dc = jnp.dot(dmid16, wo_t[...], preferred_element_type=f32).astype(bf16)
        for p in range(NP):
            dm = stack(dc[:, p * 128:(p + 1) * 128])
            dm_s[p] = dm
            dt_s[p] = dm.T
        dsum_s[...] = jnp.zeros_like(dsum_s)
        dqt_s[...] = jnp.zeros_like(dqt_s)

        def scores(b, diagonal):
            for p in range(NP):
                s = jnp.dot(qkv_b[par, b, NP + p], qt_s[p], preferred_element_type=f32) * LOG2E - lse_b[par, c, p:p + 1] * LOG2E
                if diagonal:
                    s = jnp.where(causal, s, NEG)
                pr = jnp.exp2(s)
                dp = jnp.dot(qkv_b[par, b, 2 * NP + p], dt_s[p], preferred_element_type=f32)
                dsum_s[p] += jnp.sum((pr * dp).reshape(C // 8, 8, C2), axis=0)
                p_s[b, p] = pr
                dp_s[b, p] = dp

        def grads(b):
            ks = pl.ds(pl.multiple_of(b * C, C), C)
            for p in range(NP):
                pr = p_s[b, p]
                ds = (pr * (dp_s[b, p] - jnp.sum(dsum_s[p], axis=0, keepdims=True))).astype(bf16)
                dv_s[p, ks] += jnp.dot(pr.astype(bf16), dm_s[p], preferred_element_type=f32)
                dk_s[p, ks] += jnp.dot(ds, qm_s[p], preferred_element_type=f32)
                dqt = jnp.dot(kt_s[p, :, ks], ds, preferred_element_type=f32)
                dqt_s[p, 0:64] += dqt[0:64, 0:C]
                dqt_s[p, 64:128] += dqt[64:128, C:C2]

        def group(what):
            def run(b, carry):
                for i in range(UN):
                    what(UN * b + i)
                return carry
            lax.fori_loop(0, c // UN, run, 0)

        def rest(k):
            def run():
                for i in range(k):
                    scores(c - k + i, False)
                scores(c, True)
                grads(c)
                for i in range(k):
                    grads(c - k + i)
            return run

        group(lambda b: scores(b, False))
        for k in range(UN):
            pl.when(lax.rem(c, UN) == k)(rest(k))
        group(grads)

        for p in range(NP):
            for i, val in enumerate((dqt_s[p].T * 0.125, dk_s[p, rows], dv_s[p, rows])):
                dqkv_s[slot, :, i * D + p * 128:i * D + (p + 1) * 128] = val.astype(bf16)
            dk_s[p, rows] = jnp.zeros((C, 128), f32)
            dv_s[p, rows] = jnp.zeros((C, 128), f32)
        da = jnp.dot(dqkv_s[slot], wqkv_t[...], preferred_element_type=f32)
        gm1 = g1[...].astype(f32)
        sh, r1 = sh_s[...], r1_s[:, 0:1]
        gg1_o[...] += jnp.sum((da * sh).reshape(C // 8, 8, D), axis=0)
        gd = da * gm1
        o_s[slot] += r1 * (gd - sh * jnp.mean(gd * sh, axis=-1, keepdims=True))
        for cp in stores(row0, slot):
            cp.start()

        @pl.when(me > 0)
        def _():
            send(t, slot).start()
        return carry

    lax.fori_loop(0, total, step, 0)
    for t in (total - 2, total - 1):
        for cp in stores(0, t % 2):
            cp.wait()

        @pl.when(me > 0)
        def _():
            send(t, t % 2).wait_send()


def backward(sizes, cid, cot_all, sv_qkv, sv_h, sv_u, sv_lse, wqkv_t, wo_t, w1, w1_t, w2_t, g1, g2):
    V = pl.BlockSpec(memory_space=pltpu.VMEM)
    A = pl.BlockSpec(memory_space=pltpu.HBM)
    dma = pltpu.SemaphoreType.DMA
    sd = jax.ShapeDtypeStruct
    T = sum(sizes)
    R = NT_ALL * C
    VM = pltpu.VMEM
    return pl.pallas_call(
        functools.partial(bwd_kernel, sizes),
        out_shape=(sd((R, F), bf16), sd((R, F), bf16), sd((R, D), bf16), sd((R, D), bf16), sd((R, D), bf16), sd((R, D), bf16),
                   sd((R, 3 * D), bf16), sd((8, D), f32), sd((8, D), f32)),
        in_specs=[A] * 5 + [V] * 7,
        out_specs=(A,) * 7 + (V, V),
        scratch_shapes=[
            VM((T, C, D), f32), VM((2, NC, C, D), bf16), VM((2, NC, 3 * NP, C, 128), bf16), VM((2, NC, C, D), bf16), VM((2, NC, C, D), bf16),
            VM((2, NC, NP, C2), f32), VM((NP, 128, S), bf16), VM((NP, S, 128), f32), VM((NP, S, 128), f32),
            VM((2, C, F), bf16), VM((2, C, F), bf16), VM((2, C, D), bf16), VM((2, C, D), bf16), VM((2, C, D), bf16),
            VM((2, C, D), bf16), VM((2, C, 3 * D), bf16), VM((2, C, D), f32),
            VM((NP, C2, 128), bf16), VM((NP, 128, C2), bf16), VM((NP, C2, 128), bf16), VM((NP, 128, C2), bf16),
            VM((NC, NP, C, C2), f32), VM((NC, NP, C, C2), f32), VM((NP, 8, C2), f32), VM((NP, 128, C), f32),
            VM((C, D), f32), VM((C, 128), f32),
            dma((T,)), dma((2,)), dma((2, 5)), dma((2, 7))],
        compiler_params=pltpu.CompilerParams(collective_id=cid, has_side_effects=True, vmem_limit_bytes=61 * 1024 * 1024),
        cost_estimate=pl.CostEstimate(flops=80 * 10 ** 9, bytes_accessed=10 ** 8, transcendentals=10 ** 7),
    )(cot_all, sv_qkv, sv_h, sv_u, sv_lse, wqkv_t, wo_t, w1, w1_t, w2_t, g1, g2)


def pack_kernel(plans, lens, qkv, h, u, lse, cot, pick_o, src, qkv_o, h_o, u_o, lse_o, cot_o,
                qkv_b, h_b, u_b, lse_b, cot_b, order, ld_sem, st_sem):
    for m in range(ND):
        rank = 0
        for k in range(ND):
            longer = lens[k] > lens[m] if k >= m else lens[k] >= lens[m]
            rank = rank + jnp.where(longer, 1, 0)
        order[rank] = m
    pick = len(plans) - 1
    for i in reversed(range(len(plans) - 1)):
        fits = True
        for r in range(ND):
            fits = jnp.logical_and(fits, lens[order[r]] <= plans[i][r] * C)
        pick = jnp.where(fits, i, pick)
    pick_o[0] = pick
    count = 0
    for r in range(ND):
        n = 0
        for i, plan in enumerate(plans):
            n = n + jnp.where(pick == i, plan[r], 0)

        def put(j, carry, count=count, r=r):
            src[count + j] = order[r] * NC + j
            return carry
        lax.fori_loop(0, n, put, 0)
        count = count + n
    pick_o[1] = count
    arrays = ((qkv, qkv_b, qkv_o), (h, h_b, h_o), (u, u_b, u_o), (lse, lse_b, lse_o), (cot, cot_b, cot_o))

    def load(t):
        s = lax.rem(t, RING)
        return [pltpu.make_async_copy(a.at[src[t]], b.at[s], ld_sem.at[s, i]) for i, (a, b, _) in enumerate(arrays)]

    def store(t):
        s = lax.rem(t, RING)
        return [pltpu.make_async_copy(b.at[s], o.at[t], st_sem.at[s, i]) for i, (_, b, o) in enumerate(arrays)]

    lag = RING // 2

    def go(t, carry):
        @pl.when(t < count)
        def _():
            @pl.when(t >= RING)
            def _():
                for cp in store(t - RING):
                    cp.wait()
            for cp in load(t):
                cp.start()

        @pl.when(t >= lag)
        def _():
            for cp in load(t - lag):
                cp.wait()
            for cp in store(t - lag):
                cp.start()
        return carry

    lax.fori_loop(0, count + lag, go, 0)

    def drain(t, carry):
        for cp in store(t):
            cp.wait()
        return carry

    lax.fori_loop(jnp.maximum(count - RING, 0), count, drain, 0)


RING = 16


def pack(plans, lens, *arrays):
    A = pl.BlockSpec(memory_space=pltpu.HBM)
    SM = pl.BlockSpec(memory_space=pltpu.SMEM)
    sd = jax.ShapeDtypeStruct
    return pl.pallas_call(
        functools.partial(pack_kernel, plans),
        out_shape=(sd((2,), jnp.int32), sd((NT_ALL,), jnp.int32)) + tuple(sd(a.shape, a.dtype) for a in arrays),
        in_specs=[SM] + [A] * 5,
        out_specs=(SM, SM) + (A,) * 5,
        scratch_shapes=[pltpu.VMEM((RING,) + a.shape[1:], a.dtype) for a in arrays] + [
            pltpu.SMEM((ND,), jnp.int32), pltpu.SemaphoreType.DMA((RING, 5)), pltpu.SemaphoreType.DMA((RING, 5))],
        compiler_params=pltpu.CompilerParams(vmem_limit_bytes=60 * 1024 * 1024),
        cost_estimate=pl.CostEstimate(flops=10 ** 9, bytes_accessed=5 * 10 ** 7, transcendentals=0),
    )(lens, *arrays)


def wgrad_kernel(pick, src, a, cx, a2, z, dqkv, dmid, dpre, d16, gg1, gg2,
                 g_qkv, g_out, g_up, g_down, g_g1, g_g2,
                 a_b, cx_b, a2_b, z_b, dqkv_b, dmid_b, dpre_b, d16_b, s_qkv, s_out, s_up, s_down, ld_sem, st_sem):
    count = pick[1]
    blocks = (count + WB - 1) // WB
    bufs = ((z, z_b), (d16, d16_b), (a2, a2_b), (dpre, dpre_b), (a, a_b), (dqkv, dqkv_b), (dmid, dmid_b))

    def load(i, j, par):
        t = WB * i + j
        rows = pl.ds(j * C, C)
        cps = [pltpu.make_async_copy(x.at[pl.ds(pl.multiple_of(t * C, C), C)], b.at[par, rows], ld_sem.at[par, j, k])
               for k, (x, b) in enumerate(bufs)]
        return cps + [pltpu.make_async_copy(cx.at[src[t]], cx_b.at[par, rows], ld_sem.at[par, j, len(bufs)])]

    def each(i, par, what):
        for j in range(WB):
            @pl.when(WB * i + j < count)
            def _(j=j):
                for cp in load(i, j, par):
                    what(cp)

    each(0, 0, lambda cp: cp.start())
    g_g1[...] = jnp.sum(gg1[...], axis=0, keepdims=True)
    g_g2[...] = jnp.sum(gg2[...], axis=0, keepdims=True)
    work = ((z_b, d16_b, s_down, g_down), (a2_b, dpre_b, s_up, g_up), (a_b, dqkv_b, s_qkv, g_qkv), (cx_b, dmid_b, s_out, g_out))
    for _, _, acc, _ in work:
        acc[...] = jnp.zeros_like(acc)

    def block(i, carry):
        par = lax.rem(i, 2)

        @pl.when(i + 1 < blocks)
        def _():
            each(i + 1, 1 - par, lambda cp: cp.start())
        each(i, par, lambda cp: cp.wait())
        for j in range(1, WB):
            @pl.when(WB * i + j >= count)
            def _(j=j):
                rows = slice(j * C, (j + 1) * C)
                for x, y, _, _ in work:
                    x[par, rows] = jnp.zeros((C, x.shape[2]), bf16)
                    y[par, rows] = jnp.zeros((C, y.shape[2]), bf16)
        for k, (x, y, acc, out) in enumerate(work):
            for m in range(0, acc.shape[0], WM):
                xt = x[par, :, m:m + WM].T
                for n in range(0, acc.shape[1], 512):
                    acc[m:m + WM, n:n + 512] += jnp.dot(xt, y[par, :, n:n + 512], preferred_element_type=f32)

            @pl.when(i + 1 == blocks)
            def _():
                pltpu.make_async_copy(acc, out, st_sem.at[k]).start()
        return carry

    lax.fori_loop(0, blocks, block, 0)
    for k, (_, _, acc, out) in enumerate(work):
        pltpu.make_async_copy(acc, out, st_sem.at[k]).wait()


WB = 2
WM = 512


def wgrad(pick, src, a, cx, a2, z, dqkv, dmid, dpre, d16, gg1, gg2):
    A = pl.BlockSpec(memory_space=pltpu.HBM)
    SM = pl.BlockSpec(memory_space=pltpu.SMEM)
    V = pl.BlockSpec(memory_space=pltpu.VMEM)
    sd = jax.ShapeDtypeStruct
    VM = pltpu.VMEM
    widths = (D, D, D, F, 3 * D, D, F, D)
    shapes = ((D, 3 * D), (D, D), (D, F), (F, D))
    return pl.pallas_call(
        wgrad_kernel,
        out_shape=tuple(sd(s, f32) for s in shapes) + (sd((1, D), f32),) * 2,
        in_specs=[SM, SM] + [A] * 8 + [V] * 2,
        out_specs=(A,) * 4 + (V, V),
        scratch_shapes=[VM((2, WB * C, w), bf16) for w in widths] + [VM(s, f32) for s in shapes] + [
            pltpu.SemaphoreType.DMA((2, WB, 8)), pltpu.SemaphoreType.DMA((4,))],
        compiler_params=pltpu.CompilerParams(vmem_limit_bytes=60 * 1024 * 1024),
        cost_estimate=pl.CostEstimate(flops=25 * 10 ** 9, bytes_accessed=7 * 10 ** 7, transcendentals=0),
    )(pick, src, a, cx, a2, z, dqkv, dmid, dpre, d16, gg1, gg2)


PLANS = ((8, 4, 4, 3, 2, 2, 1, 1), (8, 7, 4, 3, 2, 2, 2, 1), (8, 8, 5, 4, 3, 2, 2, 1), (8, 8, 7, 5, 4, 3, 2, 2), (NC,) * ND)


def solution(mesh):
    def per_device(tokens, seq_lens, cot, wqkv, wo, w1, w2, g1, g2):
        lt = jnp.broadcast_to(seq_lens.reshape(1, 1), (8, C2))
        wqkv, wo, w1, w2 = wqkv[0], wo[0], w1[0], w2[0]
        y, cot_all, lens, qkv, h, cx, u, lse, wqkv_t, wo_t, w1_t, w2_t = forward(tokens[0], cot[0], lt, wqkv, wo, w1, w2, g1, g2)
        qkv, lse = qkv.reshape(NT_ALL, 3 * NP, C, 128), lse.reshape(NT_ALL, NP, C2)
        h, cx, u, cot_all = (x.reshape(NT_ALL, C, D) for x in (h, cx, u, cot_all))
        pick, src, *packed = pack(PLANS, lens[:, 0, 0], qkv, h, u, lse, cot_all)

        def branch(i):
            def run(qkv, h, u, lse, cot_all, wqkv_t, wo_t, w1, w1_t, w2_t, g1, g2):
                return backward(PLANS[i], i + 1, cot_all, qkv, h, u, lse, wqkv_t, wo_t, w1, w1_t, w2_t, g1, g2)
            return run

        z, dpre, d16, a2, a, dmid, dqkv, gg1, gg2 = lax.switch(
            pick[0], [branch(i) for i in range(len(PLANS))], *packed, wqkv_t, wo_t, w1, w1_t, w2_t, g1, g2)
        g_qkv, g_out, g_up, g_down, g_g1, g_g2 = wgrad(pick, src, a, cx, a2, z, dqkv, dmid, dpre, d16, gg1, gg2)
        return y[None], g_qkv[None], g_out[None], g_up[None], g_down[None], g_g1, g_g2

    spec = P('stage')
    return jax.shard_map(per_device, mesh=mesh, in_specs=(spec,) * 9, out_specs=(spec,) * 7, check_vma=False)
```

```python
import functools
import jax
import jax.numpy as jnp
from jax import lax
from jax.experimental import pallas as pl
from jax.experimental.pallas import tpu as pltpu
from jax.sharding import PartitionSpec as P

bf16, f32 = jnp.bfloat16, jnp.float32
EPS = 1e-5
K0 = 0.7978845608028654
K1 = K0 * 0.044715
W = 128
NEG = -1e30
BIG = 1e30
NT = (((1,), (1,)), ((), ()))
MESH = pl.DeviceIdType.MESH
S, D, F, NH = 1024, 512, 2048, 8
C = W
C2 = 2 * C
NC = S // C
NP = 4
KB = W
ND = 8
LAST = ND - 1
NT_ALL = ND * NC
CF = 256
NF = S // CF
HALVES = CF // C
LOG2E = 1.4426950408889634


def row_sum(x):
    return jnp.sum(x, axis=0, keepdims=True)


def cost(gflops, mbytes):
    return pl.CostEstimate(flops=gflops * 10 ** 9, bytes_accessed=mbytes * 10 ** 6, transcendentals=0)


def row_mean(x):
    return jnp.mean(x, axis=-1, keepdims=True)


def params(mib, **kw):
    return pltpu.CompilerParams(vmem_limit_bytes=mib * 2 ** 20, **kw)


def iota(rows, cols, dim):
    return lax.broadcasted_iota(jnp.int32, (rows, cols), dim)


def rms(h, g):
    r = lax.rsqrt(row_mean(h * h) + EPS)
    return (h * r * g).astype(bf16)


def gelu(x):
    return x * (0.5 + 0.5 * jnp.tanh(x * (K0 + K1 * (x * x))))


def fwd_kernel(tok, cot, ltile, wqkv_h, wo_h, w1_h, w2_h, g1, g2,
               y, cot_all, lens, sv_qkv, sv_h, sv_cx, sv_u, sv_lse, wqkv_t, wo_t, w1_t, w2_t,
               hbuf, st, cx_s, u_s, o_s, lse_s, k_s, vt_s, ct_s, mask_s, causal, e_s, p_s, t1, t2, t3, t4, wqkv, wo, w1, w2,
               recv_sem, send_sem, tok_sem, len_ssem, len_rsem, cot_ssem, cot_rsem, y_sem, loc_sem, yl_sem, wt_sem, w_sem):
    me = lax.axis_index('stage')
    weights = [pltpu.make_async_copy(a, b, w_sem.at[i])
               for i, (a, b) in enumerate(((wqkv_h, wqkv), (wo_h, wo), (w1_h, w1), (w2_h, w2)))]
    for cp in weights:
        cp.start()

    barrier = pltpu.get_barrier_semaphore()
    for k in range(1, ND):
        pl.semaphore_signal(barrier, inc=1, device_id=(lax.rem(me + k, ND),), device_id_type=MESH)
    pl.semaphore_wait(barrier, ND - 1)

    def tok_copy(c):
        return pltpu.make_async_remote_copy(
            src_ref=tok.at[pl.ds(c * CF, CF)], dst_ref=hbuf.at[me * NF + c], send_sem=tok_sem.at[c],
            recv_sem=recv_sem.at[me * NF + c], device_id=(0,), device_id_type=MESH)

    def tok_local(c):
        return pltpu.make_async_copy(tok.at[pl.ds(c * CF, CF)], hbuf.at[c], recv_sem.at[c])

    def len_copy(k):
        return pltpu.make_async_remote_copy(
            src_ref=ltile, dst_ref=lens.at[me], send_sem=len_ssem.at[k - 1], recv_sem=len_rsem.at[me],
            device_id=(lax.rem(me + k, ND),), device_id_type=MESH)

    def len_wait(m):
        pltpu.make_async_remote_copy(
            src_ref=ltile, dst_ref=lens.at[m], send_sem=len_ssem.at[0], recv_sem=len_rsem.at[m],
            device_id=(0,), device_id_type=MESH).wait_recv()

    def cot_copy(m, at, n):
        rows = pl.ds(at, n)
        return pltpu.make_async_remote_copy(
            src_ref=cot.at[rows], dst_ref=cot_all.at[m, rows], send_sem=cot_ssem.at[0], recv_sem=cot_rsem.at[m],
            device_id=(LAST,), device_id_type=MESH)

    def cot_local():
        return pltpu.make_async_copy(cot, cot_all.at[LAST], cot_ssem.at[0])

    def pass_copy(t, c):
        return pltpu.make_async_remote_copy(
            src_ref=o_s.at[c], dst_ref=hbuf.at[t], send_sem=send_sem.at[c], recv_sem=recv_sem.at[t],
            device_id=(lax.rem(me + 1, ND),), device_id_type=MESH)

    def y_copy(m, c):
        return pltpu.make_async_remote_copy(
            src_ref=o_s.at[c], dst_ref=y.at[pl.ds(c * CF, CF)], send_sem=send_sem.at[c],
            recv_sem=y_sem.at[c], device_id=(m,), device_id_type=MESH)

    def y_local(c):
        return pltpu.make_async_copy(o_s.at[c], y.at[pl.ds(c * CF, CF)], yl_sem.at[c])

    def saves(m, c):
        t, slot = m * NF + c, c % 2
        return [
            pltpu.make_async_copy(st.at[slot], sv_qkv.at[t], loc_sem.at[slot, 0]),
            pltpu.make_async_copy(hbuf.at[t], sv_h.at[t], loc_sem.at[slot, 1]),
            pltpu.make_async_copy(cx_s.at[slot], sv_cx.at[t], loc_sem.at[slot, 2]),
            pltpu.make_async_copy(u_s.at[slot], sv_u.at[t], loc_sem.at[slot, 3]),
            pltpu.make_async_copy(lse_s.at[slot], sv_lse.at[t], loc_sem.at[slot, 4]),
        ]

    def out_wait(m, c):
        @pl.when(me < LAST)
        def _():
            pass_copy(m * NF + c, c).wait_send()

        @pl.when(me == LAST)
        def _():
            @pl.when(m < LAST)
            def _():
                y_copy(m, c).wait_send()

            @pl.when(m == LAST)
            def _():
                y_local(c).wait()

    @pl.when(me == 0)
    def _():
        for c in range(NF):
            tok_local(c).start()

    @pl.when(me > 0)
    def _():
        for c in range(NF):
            tok_copy(c).start()

    turned = [pltpu.make_async_copy(a, b, wt_sem.at[i])
              for i, (a, b) in enumerate(((t1, wqkv_t), (t2, wo_t), (t3, w1_t), (t4, w2_t)))]

    def turn_weights():
        for src, dst in ((wqkv, t1), (wo, t2), (w1, t3), (w2, t4)):
            def block(i, carry, src=src, dst=dst):
                at = pl.ds(pl.multiple_of(i * W, W), W)
                dst[at] = src[:, at].T
                return carry
            lax.fori_loop(0, src.shape[1] // W, block, 0)
        for cp in turned:
            cp.start()

    for k in range(1, ND):
        len_copy(k).start()
    lens[me] = ltile[...]

    @pl.when(me == LAST)
    def _():
        cot_local().start()

    causal[...] = jnp.where(iota(C, C2, 0)
                            <= lax.rem(iota(C, C2, 1), C), 0.0, NEG)

    for cp in weights:
        cp.wait()

    @pl.when(me >= 4)
    def _():
        turn_weights()

    def step(m, c):
        t, slot = m * NF + c, c % 2

        if c == 0:
            @pl.when(m != me)
            def _():
                len_wait(m)

        @pl.when(jnp.logical_and(me == 0, m == 0))
        def _():
            tok_local(c).wait()

        @pl.when(jnp.logical_or(me > 0, m > 0))
        def _():
            pass_copy(t, c).wait_recv()

        @pl.when(m > 0)
        def _():
            out_wait(m - 1, c)

        def reuse(mm):
            for cp in saves(mm, (c - 2) % NF):
                cp.wait()

        if c < 2:
            @pl.when(m > 0)
            def _():
                reuse(m - 1)
        else:
            reuse(m)

        h = hbuf[t].astype(f32)
        a = rms(h, g1[...].astype(f32))
        q = jnp.dot(a, wqkv[:, :D], preferred_element_type=f32)
        kk = jnp.dot(a, wqkv[:, D:2 * D], preferred_element_type=f32).astype(bf16)
        vv = jnp.dot(a, wqkv[:, 2 * D:], preferred_element_type=f32).astype(bf16)
        q = (q * 0.125).astype(bf16)
        own = slice(c * CF, (c + 1) * CF)
        for p in range(NP):
            lanes = slice(p * W, (p + 1) * W)
            for j in range(HALVES):
                rows = slice(j * C, (j + 1) * C)
                st[slot, j, p] = q[rows, lanes]
                st[slot, j, NP + p] = kk[rows, lanes]
                st[slot, j, 2 * NP + p] = vv[rows, lanes]
            k_s[p, own] = kk[:, lanes]
            vt_s[p, :, own] = vv[:, lanes].T
        ln = lens[m][0:1, :]
        key = iota(CF, W, 0) + c * CF
        off = jnp.logical_and(key >= ln[:, :W], iota(CF, W, 1) == 0)
        mask_s[own] = jnp.where(off, NEG, 0.0).astype(bf16)

        half = iota(W, C, 0) < 64
        one = jnp.where(iota(W, C2, 0) == 0, 1.0, 0.0).astype(bf16)

        def attend(j):
            i = c * HALVES + j
            nk = (i + 1) * C

            def scores(p):
                qt = q[j * C:(j + 1) * C, p * W:(p + 1) * W].T
                zero = jnp.zeros_like(qt)
                qt = jnp.concatenate([jnp.where(half, qt, zero), jnp.where(half, zero, qt)], axis=1)
                qt = jnp.concatenate([qt, one], axis=0)
                top = None
                for b in range(i + 1):
                    ks = slice(b * C, (b + 1) * C)
                    s = jnp.dot(jnp.concatenate([k_s[p, ks], mask_s[ks]], axis=1), qt, preferred_element_type=f32)
                    if b == i:
                        s = s + causal[...]
                    mb = jnp.max(s.reshape(C // 8, 8, C2), axis=0)
                    top = mb if top is None else jnp.maximum(top, mb)
                    e_s[p, ks] = s
                return jnp.max(top, axis=0, keepdims=True)

            def exps(p, top):
                total = None
                top2 = top * LOG2E
                for b in range(i + 1):
                    ks = slice(b * C, (b + 1) * C)
                    e = jnp.exp2(e_s[p, ks] * LOG2E - top2)
                    sb = jnp.sum(e.reshape(C // 8, 8, C2), axis=0)
                    total = sb if total is None else total + sb
                    p_s[p, ks] = e.astype(bf16)
                total = row_sum(total)
                here = (lax.rem(iota(1, C2, 1), C) + i * C) < ln
                lse_s[slot, j, p:p + 1] = jnp.where(here, top + jnp.log(total), BIG)
                return 1.0 / total

            def context(p, inv):
                o = jnp.dot(vt_s[p, :, 0:nk], p_s[p, 0:nk], preferred_element_type=f32) * inv
                own = slice(j * C, (j + 1) * C)
                ct_s[p, 0:64, own] = o[0:64, 0:C].astype(bf16)
                ct_s[p, 64:, own] = o[64:, C:].astype(bf16)

            tops = [scores(p) for p in range(NP)]
            invs = [exps(p, tops[p]) for p in range(NP)]
            for p in range(NP):
                context(p, invs[p])

        for j in range(HALVES):
            attend(j)
        cx = jnp.concatenate([ct_s[p].T for p in range(NP)], axis=1)
        cx_s[slot] = cx
        u = (h + jnp.dot(cx, wo[...], preferred_element_type=f32)).astype(bf16)
        u_s[slot] = u
        u = u.astype(f32)
        a2 = rms(u, g2[...].astype(f32))
        z = gelu(jnp.dot(a2, w1[...], preferred_element_type=f32)).astype(bf16)
        o_s[c] = (u + jnp.dot(z, w2[...], preferred_element_type=f32)).astype(bf16)
        for cp in saves(m, c):
            cp.start()

        @pl.when(me < LAST)
        def _():
            pass_copy(t, c).start()
            piece = S // (ND * NF)
            cot_copy(me, pl.multiple_of(t * piece, piece), piece).start()

        @pl.when(me == LAST)
        def _():
            @pl.when(m < LAST)
            def _():
                y_copy(m, c).start()

            @pl.when(m == LAST)
            def _():
                y_local(c).start()

    def seq(m, carry):
        for c in range(NF):
            step(m, c)
        return carry

    lax.fori_loop(0, ND, seq, 0)

    @pl.when(me < 4)
    def _():
        turn_weights()

    for cp in turned:
        cp.wait()
    for c in (NF - 2, NF - 1):
        for cp in saves(LAST, c):
            cp.wait()
    for c in range(NF):
        out_wait(LAST, c)
    for k in range(1, ND):
        len_copy(k).wait_send()

    @pl.when(me > 0)
    def _():
        for c in range(NF):
            tok_copy(c).wait_send()

    @pl.when(me < LAST)
    def _():
        cot_copy(me, 0, S).wait_send()
        for c in range(NF):
            y_copy(0, c).wait_recv()

    @pl.when(me == LAST)
    def _():
        cot_local().wait()
        for m in range(LAST):
            cot_copy(m, 0, S).wait_recv()


def forward(tok, cot, ltile, wqkv, wo, w1, w2, g1, g2):
    V = pl.BlockSpec(memory_space=pltpu.VMEM)
    A = pl.BlockSpec(memory_space=pltpu.HBM)
    dma = pltpu.SemaphoreType.DMA
    sd = jax.ShapeDtypeStruct
    return pl.pallas_call(
        fwd_kernel,
        out_shape=(sd((S, D), bf16), sd((ND, S, D), bf16), sd((ND, 8, C2), jnp.int32),
                   sd((ND * NF, HALVES, 3 * NP, C, W), bf16), sd((ND * NF, CF, D), bf16), sd((ND * NF, CF, D), bf16),
                   sd((ND * NF, CF, D), bf16), sd((ND * NF, HALVES, 2 * NP, C2), f32), sd((3 * D, D), bf16), sd((D, D), bf16), sd((F, D), bf16), sd((D, F), bf16)),
        in_specs=[A, V, V] + [A] * 4 + [V] * 2,
        out_specs=(A, A, V) + (A,) * 9,
        scratch_shapes=[
            pltpu.VMEM((ND * NF, CF, D), bf16), pltpu.VMEM((2, HALVES, 3 * NP, C, W), bf16), pltpu.VMEM((2, CF, D), bf16),
            pltpu.VMEM((2, CF, D), bf16), pltpu.VMEM((NF, CF, D), bf16), pltpu.VMEM((2, HALVES, 2 * NP, C2), f32),
            pltpu.VMEM((NP, S, W), bf16), pltpu.VMEM((NP, W, S), bf16), pltpu.VMEM((NP, W, CF), bf16),
            pltpu.VMEM((S, W), bf16), pltpu.VMEM((C, C2), f32), pltpu.VMEM((NP, S, C2), f32), pltpu.VMEM((NP, S, C2), bf16),
            pltpu.VMEM((3 * D, D), bf16), pltpu.VMEM((D, D), bf16), pltpu.VMEM((F, D), bf16), pltpu.VMEM((D, F), bf16),
            pltpu.VMEM((D, 3 * D), bf16), pltpu.VMEM((D, D), bf16), pltpu.VMEM((D, F), bf16), pltpu.VMEM((F, D), bf16),
            dma((ND * NF,)), dma((NF,)), dma((NF,)), dma((ND - 1,)), dma((ND,)), dma((1,)), dma((ND,)), dma((NF,)),
            dma((2, 5)), dma((NF,)), dma((4,)), dma((4,))],
        compiler_params=params(56, collective_id=0, has_side_effects=True),
        cost_estimate=cost(80, 100),
    )(tok, cot, ltile, wqkv, wo, w1, w2, g1, g2)

TN = (((0,), (0,)), ((), ()))
UN = 4
OUT = 4


def bwd_kernel(sizes, cot_all, sv_qkv, sv_h, sv_u, sv_lse, wqkv_h, wo_h, w1_h, w1t_h, w2_h, g1, g2,
               z_o, dpre_o, d16_o, a2_o, a_o, dmid_o, dqkv_o, gg1_o, gg2_o,
               dbuf, cbuf, qkv_b, h_b, u_b, lse_b, kt_s, dk_s, dv_s,
               z_s, dpre_s, d16_s, a2_s, a_s, dmid_s, dqkv_s, o_s, qm_s, qt_s, dm_s, dt_s, p_s, dp_s, dsum_s, dqt_s, sh_s, r1_s,
               w2_t, w1, w1_t, wo_t, wqkv_t, recv_sem, send_sem, ld_sem, st_sem, w_sem):
    me = lax.axis_index('stage')
    weights = [pltpu.make_async_copy(a, b, w_sem.at[i]) for i, (a, b) in enumerate(
        ((w2_h, w2_t), (w1_h, w1), (w1t_h, w1_t), (wo_h, wo_t), (wqkv_h, wqkv_t)))]
    for cp in weights:
        cp.start()
    barrier = pltpu.get_barrier_semaphore()
    pl.semaphore_signal(barrier, inc=1, device_id=(lax.rem(me + 1, ND),), device_id_type=MESH)
    pl.semaphore_wait(barrier, 1)
    starts = [sum(sizes[:i]) for i in range(len(sizes))]
    total = sum(sizes)

    def loads(r, par):
        dst, src = pl.ds(0, sizes[r]), pl.ds(starts[r], sizes[r])
        pairs = [(sv_qkv, qkv_b), (sv_h, h_b), (sv_u, u_b), (sv_lse, lse_b), (cot_all, cbuf)]
        return [pltpu.make_async_copy(a.at[src], b.at[par, dst], ld_sem.at[par, i]) for i, (a, b) in enumerate(pairs)]

    def stores(row, slot):
        rows = pl.ds(row, C)
        pairs = [(z_s, z_o), (dpre_s, dpre_o), (d16_s, d16_o), (a2_s, a2_o), (a_s, a_o), (dmid_s, dmid_o), (dqkv_s, dqkv_o)]
        return [pltpu.make_async_copy(s.at[slot], o.at[rows], st_sem.at[slot, i]) for i, (s, o) in enumerate(pairs)]

    def send(t, slot):
        return pltpu.make_async_remote_copy(
            src_ref=o_s.at[slot], dst_ref=dbuf.at[t], send_sem=send_sem.at[slot], recv_sem=recv_sem.at[t],
            device_id=(lax.rem(me + ND - 1, ND),), device_id_type=MESH)

    for cp in loads(0, 0):
        cp.start()
    gg1_o[...] = jnp.zeros_like(gg1_o)
    gg2_o[...] = jnp.zeros_like(gg2_o)
    dk_s[...] = jnp.zeros_like(dk_s)
    dv_s[...] = jnp.zeros_like(dv_s)
    causal = iota(C, C2, 0) <= lax.rem(iota(C, C2, 1), C)
    lane = iota(C, W, 1) < 64

    def stack(x):
        zero = jnp.zeros_like(x)
        return jnp.concatenate([jnp.where(lane, x, zero), jnp.where(lane, zero, x)], axis=0)

    def step(t, carry):
        r, n, first = 0, sizes[0], 0
        for i in range(1, len(sizes)):
            past = (t + 1024 - starts[i]) // 1024
            r = r + past
            n = n + past * (sizes[i] - sizes[i - 1])
            first = first + past * (starts[i] - starts[i - 1])
        c = n - 1 - (t - first)
        par, slot, out = lax.rem(r, 2), lax.rem(t, 2), lax.rem(t, OUT)
        row0 = pl.multiple_of((first + c) * C, C)
        rows = pl.ds(pl.multiple_of(c * C, C), C)

        for i in range(len(sizes)):
            @pl.when(t == starts[i])
            def _(i=i):
                for cp in loads(i, i % 2):
                    cp.wait()
                if i + 1 < len(sizes):
                    for cp in loads(i + 1, (i + 1) % 2):
                        cp.start()

                def turn(j, carry):
                    for p in range(NP):
                        kt_s[p, :, pl.ds(pl.multiple_of(j * C, C), C)] = qkv_b[i % 2, j, NP + p].T
                    return carry
                lax.fori_loop(0, sizes[i], turn, 0)

        @pl.when(t >= 2)
        def _():
            for cp in stores(0, slot):
                cp.wait()

        @pl.when(jnp.logical_and(t >= OUT, me > 0))
        def _():
            send(t, out).wait_send()

        @pl.when(me == LAST)
        def _():
            dbuf[t] = cbuf[par, c].astype(f32)

        @pl.when(me < LAST)
        def _():
            send(t, out).wait_recv()

        d = dbuf[t]
        d16 = d.astype(bf16)
        d16_s[slot] = d16
        u = u_b[par, c].astype(f32)
        gm2 = g2[...].astype(f32)
        r2 = lax.rsqrt(row_mean(u * u) + EPS)
        su = u * r2
        a2 = (su * gm2).astype(bf16)
        a2_s[slot] = a2
        FB = 256

        def ups(fb):
            cols = slice(fb * FB, (fb + 1) * FB)
            dz = jnp.dot(d16, w2_t[:, cols], preferred_element_type=f32)
            return jnp.dot(a2, w1[:, cols], preferred_element_type=f32), dz

        ahead = [ups(0)]
        for fb in range(F // FB):
            cols = slice(fb * FB, (fb + 1) * FB)
            if fb + 1 < F // FB:
                ahead.append(ups(fb + 1))
            x, dz = ahead[fb]
            x2 = x * x
            sg = 0.5 + 0.5 * jnp.tanh(x * (K0 + K1 * x2))
            zz = x * sg
            z_s[slot, :, cols] = zz.astype(bf16)
            gp = sg + (zz - zz * sg) * (2.0 * K0 + 6.0 * K1 * x2)
            dpre_s[slot, :, cols] = (dz * gp).astype(bf16)
        da2 = jnp.dot(dpre_s[slot], w1_t[...], preferred_element_type=f32)
        for p in range(NP):
            qm = stack(qkv_b[par, c, p])
            qm_s[p] = qm
            qt_s[p] = qm.T
        h = h_b[par, c].astype(f32)
        gm1 = g1[...].astype(f32)
        r1 = lax.rsqrt(row_mean(h * h) + EPS)
        sh = h * r1
        sh_s[...] = sh
        r1_s[...] = jnp.broadcast_to(r1, (C, W))
        a_s[slot] = (sh * gm1).astype(bf16)
        gg2_o[...] += jnp.sum((da2 * su).reshape(C // 8, 8, D), axis=0)
        gd = da2 * gm2
        dmid = d + r2 * (gd - su * row_mean(gd * su))
        dmid16 = dmid.astype(bf16)
        dmid_s[slot] = dmid16
        o_s[out] = dmid
        dc = jnp.dot(dmid16, wo_t[...], preferred_element_type=f32).astype(bf16)
        for p in range(NP):
            dm = stack(dc[:, p * W:(p + 1) * W])
            dm_s[p] = dm
            dt_s[p] = dm.T
        dsum_s[...] = jnp.zeros_like(dsum_s)
        dqt_s[...] = jnp.zeros_like(dqt_s)

        def scores(b, diagonal):
            for p in range(NP):
                s = jnp.dot(qkv_b[par, b, NP + p], qt_s[p], preferred_element_type=f32) * LOG2E - lse_b[par, c, p:p + 1] * LOG2E
                if diagonal:
                    s = jnp.where(causal, s, NEG)
                pr = jnp.exp2(s)
                dp = jnp.dot(qkv_b[par, b, 2 * NP + p], dt_s[p], preferred_element_type=f32)
                dsum_s[p] += jnp.sum((pr * dp).reshape(C // 8, 8, C2), axis=0)
                p_s[b, p] = pr
                dp_s[b, p] = dp

        def grads(b):
            ks = pl.ds(pl.multiple_of(b * C, C), C)
            for p in range(NP):
                pr = p_s[b, p]
                ds = (pr * (dp_s[b, p] - row_sum(dsum_s[p]))).astype(bf16)
                dv_s[p, ks] += jnp.dot(pr.astype(bf16), dm_s[p], preferred_element_type=f32)
                dk_s[p, ks] += jnp.dot(ds, qm_s[p], preferred_element_type=f32)
                dqt = jnp.dot(kt_s[p, :, ks], ds, preferred_element_type=f32)
                dqt_s[p, 0:64] += dqt[0:64, 0:C]
                dqt_s[p, 64:W] += dqt[64:W, C:C2]

        def group(what):
            def run(b, carry):
                for i in range(UN):
                    what(UN * b + i)
                return carry
            lax.fori_loop(0, c // UN, run, 0)

        def rest(k):
            def run():
                for i in range(k):
                    scores(c - k + i, False)
                scores(c, True)
                grads(c)
                for i in range(k):
                    grads(c - k + i)
            return run

        group(lambda b: scores(b, False))
        for k in range(UN):
            pl.when(lax.rem(c, UN) == k)(rest(k))
        group(grads)

        for p in range(NP):
            for i, val in enumerate((dqt_s[p].T * 0.125, dk_s[p, rows], dv_s[p, rows])):
                dqkv_s[slot, :, i * D + p * W:i * D + (p + 1) * W] = val.astype(bf16)
            dk_s[p, rows] = jnp.zeros((C, W), f32)
            dv_s[p, rows] = jnp.zeros((C, W), f32)
        da = jnp.dot(dqkv_s[slot], wqkv_t[...], preferred_element_type=f32)
        gm1 = g1[...].astype(f32)
        sh, r1 = sh_s[...], r1_s[:, 0:1]
        gg1_o[...] += jnp.sum((da * sh).reshape(C // 8, 8, D), axis=0)
        gd = da * gm1
        o_s[out] += r1 * (gd - sh * row_mean(gd * sh))
        for cp in stores(row0, slot):
            cp.start()

        @pl.when(me > 0)
        def _():
            send(t, out).start()
        return carry

    for cp in weights:
        cp.wait()
    lax.fori_loop(0, total, step, 0)
    for t in (total - 2, total - 1):
        for cp in stores(0, t % 2):
            cp.wait()

    @pl.when(me > 0)
    def _():
        for t in range(total - OUT, total):
            send(t, t % OUT).wait_send()


def backward(sizes, cid, cot_all, sv_qkv, sv_h, sv_u, sv_lse, wqkv_t, wo_t, w1, w1_t, w2_t, g1, g2):
    V = pl.BlockSpec(memory_space=pltpu.VMEM)
    A = pl.BlockSpec(memory_space=pltpu.HBM)
    dma = pltpu.SemaphoreType.DMA
    sd = jax.ShapeDtypeStruct
    T = sum(sizes)
    R = NT_ALL * C
    VM = pltpu.VMEM
    return pl.pallas_call(
        functools.partial(bwd_kernel, sizes),
        out_shape=(sd((R, F), bf16), sd((R, F), bf16), sd((R, D), bf16), sd((R, D), bf16), sd((R, D), bf16), sd((R, D), bf16),
                   sd((R, 3 * D), bf16), sd((8, D), f32), sd((8, D), f32)),
        in_specs=[A] * 10 + [V] * 2,
        out_specs=(A,) * 7 + (V, V),
        scratch_shapes=[
            VM((T, C, D), f32), VM((2, NC, C, D), bf16), VM((2, NC, 3 * NP, C, W), bf16), VM((2, NC, C, D), bf16), VM((2, NC, C, D), bf16),
            VM((2, NC, 2 * NP, C2), f32), VM((NP, W, S), bf16), VM((NP, S, W), f32), VM((NP, S, W), f32),
            VM((2, C, F), bf16), VM((2, C, F), bf16), VM((2, C, D), bf16), VM((2, C, D), bf16), VM((2, C, D), bf16),
            VM((2, C, D), bf16), VM((2, C, 3 * D), bf16), VM((OUT, C, D), f32),
            VM((NP, C2, W), bf16), VM((NP, W, C2), bf16), VM((NP, C2, W), bf16), VM((NP, W, C2), bf16),
            VM((NC, NP, C, C2), f32), VM((NC, NP, C, C2), f32), VM((NP, 8, C2), f32), VM((NP, W, C), f32),
            VM((C, D), f32), VM((C, W), f32),
            VM((D, F), bf16), VM((D, F), bf16), VM((F, D), bf16), VM((D, D), bf16), VM((3 * D, D), bf16),
            dma((T,)), dma((OUT,)), dma((2, 5)), dma((2, 7)), dma((5,))],
        compiler_params=params(60, collective_id=cid, has_side_effects=True),
        cost_estimate=cost(60, 100),
    )(cot_all, sv_qkv, sv_h, sv_u, sv_lse, wqkv_t, wo_t, w1, w1_t, w2_t, g1, g2)


def pack_kernel(plans, lens, qkv, h, u, lse, cot, pick_o, src, live, qkv_o, h_o, u_o, lse_o, cot_o,
                qkv_b, h_b, u_b, lse_b, cot_b, order, ld_sem, st_sem):
    for m in range(ND):
        rank = 0
        for k in range(ND):
            longer = lens[k] > lens[m] if k >= m else lens[k] >= lens[m]
            rank = rank + jnp.where(longer, 1, 0)
        order[rank] = m
    pick = len(plans) - 1
    for i in reversed(range(len(plans) - 1)):
        fits = True
        for r in range(ND):
            fits = jnp.logical_and(fits, lens[order[r]] <= plans[i][r] * C)
        pick = jnp.where(fits, i, pick)
    pick_o[0] = pick
    count = 0
    for r in range(ND):
        n = 0
        for i, plan in enumerate(plans):
            n = n + jnp.where(pick == i, plan[r], 0)

        def put(j, carry, count=count, r=r):
            src[count + j] = order[r] * NC + j
            return carry
        lax.fori_loop(0, n, put, 0)
        count = count + n
    used = 0
    start = 0
    for r in range(ND):
        n = 0
        for i, plan in enumerate(plans):
            n = n + jnp.where(pick == i, plan[r], 0)
        k = (lens[order[r]] + C - 1) // C

        def mark(j, carry, used=used, start=start):
            live[used + j] = start + j
            return carry
        lax.fori_loop(0, k, mark, 0)
        used = used + k
        start = start + n
    pick_o[1] = used
    arrays = ((qkv, qkv_b, qkv_o), (h, h_b, h_o), (u, u_b, u_o), (lse, lse_b, lse_o), (cot, cot_b, cot_o))

    def load(t):
        s = lax.rem(t, RING)
        return [pltpu.make_async_copy(a.at[src[t]], b.at[s], ld_sem.at[s, i]) for i, (a, b, _) in enumerate(arrays)]

    def store(t):
        s = lax.rem(t, RING)
        return [pltpu.make_async_copy(b.at[s], o.at[t], st_sem.at[s, i]) for i, (_, b, o) in enumerate(arrays)]

    lag = RING // 2

    def go(t, carry):
        @pl.when(t < count)
        def _():
            @pl.when(t >= RING)
            def _():
                for cp in store(t - RING):
                    cp.wait()
            for cp in load(t):
                cp.start()

        @pl.when(t >= lag)
        def _():
            for cp in load(t - lag):
                cp.wait()
            for cp in store(t - lag):
                cp.start()
        return carry

    lax.fori_loop(0, count + lag, go, 0)

    def drain(t, carry):
        for cp in store(t):
            cp.wait()
        return carry

    lax.fori_loop(jnp.maximum(count - RING, 0), count, drain, 0)


RING = 16


def pack(plans, lens, *arrays):
    A = pl.BlockSpec(memory_space=pltpu.HBM)
    SM = pl.BlockSpec(memory_space=pltpu.SMEM)
    sd = jax.ShapeDtypeStruct
    return pl.pallas_call(
        functools.partial(pack_kernel, plans),
        out_shape=(sd((2,), jnp.int32), sd((NT_ALL,), jnp.int32), sd((NT_ALL,), jnp.int32)) + tuple(sd(a.shape, a.dtype) for a in arrays),
        in_specs=[SM] + [A] * 5,
        out_specs=(SM, SM, SM) + (A,) * 5,
        scratch_shapes=[pltpu.VMEM((RING,) + a.shape[1:], a.dtype) for a in arrays] + [
            pltpu.SMEM((ND,), jnp.int32), pltpu.SemaphoreType.DMA((RING, 5)), pltpu.SemaphoreType.DMA((RING, 5))],
        compiler_params=params(60),
        cost_estimate=cost(1, 50),
    )(lens, *arrays)


def wgrad_kernel(pick, src, live, a, cx, a2, z, dqkv, dmid, dpre, d16, gg1, gg2,
                 g_qkv, g_out, g_up, g_down, g_g1, g_g2,
                 a_b, cx_b, a2_b, z_b, dqkv_b, dmid_b, dpre_b, d16_b, s_qkv, s_out, s_up, s_down, ld_sem, st_sem):
    count = pick[1]
    blocks = (count + WB - 1) // WB
    bufs = ((z, z_b), (d16, d16_b), (a2, a2_b), (dpre, dpre_b), (a, a_b), (dqkv, dqkv_b), (dmid, dmid_b))

    def load(i, j, par):
        t = live[WB * i + j]
        rows = pl.ds(j * C, C)
        cps = [pltpu.make_async_copy(x.at[pl.ds(pl.multiple_of(t * C, C), C)], b.at[par, rows], ld_sem.at[par, j, k])
               for k, (x, b) in enumerate(bufs)]
        return cps + [pltpu.make_async_copy(cx.at[src[t]], cx_b.at[par, rows], ld_sem.at[par, j, len(bufs)])]

    def each(i, par, what):
        for j in range(WB):
            @pl.when(WB * i + j < count)
            def _(j=j):
                for cp in load(i, j, par):
                    what(cp)

    each(0, 0, lambda cp: cp.start())
    g_g1[...] = row_sum(gg1[...])
    g_g2[...] = row_sum(gg2[...])
    work = ((z_b, d16_b, s_down, g_down), (a2_b, dpre_b, s_up, g_up), (a_b, dqkv_b, s_qkv, g_qkv), (cx_b, dmid_b, s_out, g_out))
    for _, _, acc, _ in work:
        acc[...] = jnp.zeros_like(acc)

    def block(i, carry):
        par = lax.rem(i, 2)

        @pl.when(i + 1 < blocks)
        def _():
            each(i + 1, 1 - par, lambda cp: cp.start())
        each(i, par, lambda cp: cp.wait())
        for j in range(1, WB):
            @pl.when(WB * i + j >= count)
            def _(j=j):
                rows = slice(j * C, (j + 1) * C)
                for x, y, _, _ in work:
                    x[par, rows] = jnp.zeros((C, x.shape[2]), bf16)
                    y[par, rows] = jnp.zeros((C, y.shape[2]), bf16)
        for k, (x, y, acc, out) in enumerate(work):
            for m in range(0, acc.shape[0], WM):
                xt = x[par, :, m:m + WM].T
                for n in range(0, acc.shape[1], 512):
                    acc[m:m + WM, n:n + 512] += jnp.dot(xt, y[par, :, n:n + 512], preferred_element_type=f32)

            @pl.when(i + 1 == blocks)
            def _():
                pltpu.make_async_copy(acc, out, st_sem.at[k]).start()
        return carry

    lax.fori_loop(0, blocks, block, 0)
    for k, (_, _, acc, out) in enumerate(work):
        pltpu.make_async_copy(acc, out, st_sem.at[k]).wait()


WB = 2
WM = 512


def wgrad(pick, src, live, a, cx, a2, z, dqkv, dmid, dpre, d16, gg1, gg2):
    A = pl.BlockSpec(memory_space=pltpu.HBM)
    SM = pl.BlockSpec(memory_space=pltpu.SMEM)
    V = pl.BlockSpec(memory_space=pltpu.VMEM)
    sd = jax.ShapeDtypeStruct
    VM = pltpu.VMEM
    widths = (D, D, D, F, 3 * D, D, F, D)
    shapes = ((D, 3 * D), (D, D), (D, F), (F, D))
    return pl.pallas_call(
        wgrad_kernel,
        out_shape=tuple(sd(s, f32) for s in shapes) + (sd((1, D), f32),) * 2,
        in_specs=[SM] * 3 + [A] * 8 + [V] * 2,
        out_specs=(A,) * 4 + (V, V),
        scratch_shapes=[VM((2, WB * C, w), bf16) for w in widths] + [VM(s, f32) for s in shapes] + [
            pltpu.SemaphoreType.DMA((2, WB, 8)), pltpu.SemaphoreType.DMA((4,))],
        compiler_params=params(60),
        cost_estimate=cost(25, 70),
    )(pick, src, live, a, cx, a2, z, dqkv, dmid, dpre, d16, gg1, gg2)


PLANS = ((8, 4, 4, 3, 2, 2, 1, 1), (8, 7, 4, 3, 2, 2, 2, 1), (8, 8, 5, 4, 3, 2, 2, 1), (8, 8, 7, 5, 4, 3, 2, 2), (NC,) * ND)


def solution(mesh):
    def per_device(tokens, seq_lens, cot, wqkv, wo, w1, w2, g1, g2):
        lt = jnp.broadcast_to(seq_lens.reshape(1, 1), (8, C2))
        wqkv, wo, w1, w2 = wqkv[0], wo[0], w1[0], w2[0]
        y, cot_all, lens, qkv, h, cx, u, lse, wqkv_t, wo_t, w1_t, w2_t = forward(tokens[0], cot[0], lt, wqkv, wo, w1, w2, g1, g2)
        qkv, lse = qkv.reshape(NT_ALL, 3 * NP, C, 128), lse.reshape(NT_ALL, 2 * NP, C2)
        h, cx, u, cot_all = (x.reshape(NT_ALL, C, D) for x in (h, cx, u, cot_all))
        pick, src, live, *packed = pack(PLANS, lens[:, 0, 0], qkv, h, u, lse, cot_all)

        def branch(i):
            def run(qkv, h, u, lse, cot_all, wqkv_t, wo_t, w1, w1_t, w2_t, g1, g2):
                return backward(PLANS[i], i + 1, cot_all, qkv, h, u, lse, wqkv_t, wo_t, w1, w1_t, w2_t, g1, g2)
            return run

        z, dpre, d16, a2, a, dmid, dqkv, gg1, gg2 = lax.switch(
            pick[0], [branch(i) for i in range(len(PLANS))], *packed, wqkv_t, wo_t, w1, w1_t, w2_t, g1, g2)
        g_qkv, g_out, g_up, g_down, g_g1, g_g2 = wgrad(pick, src, live, a, cx, a2, z, dqkv, dmid, dpre, d16, gg1, gg2)
        return y[None], g_qkv[None], g_out[None], g_up[None], g_down[None], g_g1, g_g2

    spec = P('stage')
    return jax.shard_map(per_device, mesh=mesh, in_specs=(spec,) * 9, out_specs=(spec,) * 7, check_vma=False)
```

```python
import functools
import jax
import jax.numpy as jnp
from jax import lax
from jax.experimental import pallas as pl
from jax.experimental.pallas import tpu as pltpu
from jax.sharding import PartitionSpec as P

bf16, f32 = jnp.bfloat16, jnp.float32
EPS = 1e-5
K0 = 0.7978845608028654
K1 = K0 * 0.044715
W = 128
NEG = -1e30
BIG = 1e30
NT = (((1,), (1,)), ((), ()))
MESH = pl.DeviceIdType.MESH
S, D, F, NH = 1024, 512, 2048, 8
C = W
C2 = 2 * C
NC = S // C
NP = 4
KB = W
ND = 8
LAST = ND - 1
NT_ALL = ND * NC
CF = 256
NF = S // CF
HALVES = CF // C
LOG2E = 1.4426950408889634


def row_sum(x):
    return jnp.sum(x, axis=0, keepdims=True)


def cost(gflops, mbytes):
    return pl.CostEstimate(flops=gflops * 10 ** 9, bytes_accessed=mbytes * 10 ** 6, transcendentals=0)


def row_mean(x):
    return jnp.mean(x, axis=-1, keepdims=True)


def params(mib, **kw):
    return pltpu.CompilerParams(vmem_limit_bytes=mib * 2 ** 20, **kw)


def iota(rows, cols, dim):
    return lax.broadcasted_iota(jnp.int32, (rows, cols), dim)


def rms(h, g):
    r = lax.rsqrt(row_mean(h * h) + EPS)
    return (h * r * g).astype(bf16)


def gelu(x):
    return x * (0.5 + 0.5 * jnp.tanh(x * (K0 + K1 * (x * x))))


def fwd_kernel(tok, cot, own_len, wqkv_h, wo_h, w1_h, w2_h, g1, g2,
               y, cot_all, lens_o, sv_qkv, sv_h, sv_cx, sv_u, sv_lse, wqkv_t, wo_t, w1_t, w2_t,
               hbuf, st, cx_s, u_s, o_s, lse_s, k_s, vt_s, ct_s, mask_s, causal, e_s, p_s, t1, t2, t3, t4, wqkv, wo, w1, w2, ltile, lens,
               recv_sem, send_sem, tok_sem, len_ssem, len_rsem, cot_ssem, cot_rsem, y_sem, loc_sem, yl_sem, wt_sem, w_sem):
    me = lax.axis_index('stage')
    weights = [pltpu.make_async_copy(a, b, w_sem.at[i])
               for i, (a, b) in enumerate(((wqkv_h, wqkv), (wo_h, wo), (w1_h, w1), (w2_h, w2)))]
    for cp in weights:
        cp.start()
    ltile[...] = jnp.full(ltile.shape, own_len[0], jnp.int32)

    barrier = pltpu.get_barrier_semaphore()
    for k in range(1, ND):
        pl.semaphore_signal(barrier, inc=1, device_id=(lax.rem(me + k, ND),), device_id_type=MESH)
    pl.semaphore_wait(barrier, ND - 1)

    def tok_copy(c):
        return pltpu.make_async_remote_copy(
            src_ref=tok.at[pl.ds(c * CF, CF)], dst_ref=hbuf.at[me * NF + c], send_sem=tok_sem.at[c],
            recv_sem=recv_sem.at[me * NF + c], device_id=(0,), device_id_type=MESH)

    def tok_local(c):
        return pltpu.make_async_copy(tok.at[pl.ds(c * CF, CF)], hbuf.at[c], recv_sem.at[c])

    def len_copy(k):
        return pltpu.make_async_remote_copy(
            src_ref=ltile, dst_ref=lens.at[me], send_sem=len_ssem.at[k - 1], recv_sem=len_rsem.at[me],
            device_id=(lax.rem(me + k, ND),), device_id_type=MESH)

    def len_wait(m):
        pltpu.make_async_remote_copy(
            src_ref=ltile, dst_ref=lens.at[m], send_sem=len_ssem.at[0], recv_sem=len_rsem.at[m],
            device_id=(0,), device_id_type=MESH).wait_recv()

    def cot_copy(m, at, n):
        rows = pl.ds(at, n)
        return pltpu.make_async_remote_copy(
            src_ref=cot.at[rows], dst_ref=cot_all.at[m, rows], send_sem=cot_ssem.at[0], recv_sem=cot_rsem.at[m],
            device_id=(LAST,), device_id_type=MESH)

    def cot_local():
        return pltpu.make_async_copy(cot, cot_all.at[LAST], cot_ssem.at[0])

    def pass_copy(t, c):
        return pltpu.make_async_remote_copy(
            src_ref=o_s.at[c], dst_ref=hbuf.at[t], send_sem=send_sem.at[c], recv_sem=recv_sem.at[t],
            device_id=(lax.rem(me + 1, ND),), device_id_type=MESH)

    def y_copy(m, c):
        return pltpu.make_async_remote_copy(
            src_ref=o_s.at[c], dst_ref=y.at[pl.ds(c * CF, CF)], send_sem=send_sem.at[c],
            recv_sem=y_sem.at[c], device_id=(m,), device_id_type=MESH)

    def y_local(c):
        return pltpu.make_async_copy(o_s.at[c], y.at[pl.ds(c * CF, CF)], yl_sem.at[c])

    def saves(m, c):
        t, slot = m * NF + c, c % 2
        return [
            pltpu.make_async_copy(st.at[slot], sv_qkv.at[t], loc_sem.at[slot, 0]),
            pltpu.make_async_copy(hbuf.at[t], sv_h.at[t], loc_sem.at[slot, 1]),
            pltpu.make_async_copy(cx_s.at[slot], sv_cx.at[t], loc_sem.at[slot, 2]),
            pltpu.make_async_copy(u_s.at[slot], sv_u.at[t], loc_sem.at[slot, 3]),
            pltpu.make_async_copy(lse_s.at[slot], sv_lse.at[t], loc_sem.at[slot, 4]),
        ]

    def out_wait(m, c):
        @pl.when(me < LAST)
        def _():
            pass_copy(m * NF + c, c).wait_send()

        @pl.when(me == LAST)
        def _():
            @pl.when(m < LAST)
            def _():
                y_copy(m, c).wait_send()

            @pl.when(m == LAST)
            def _():
                y_local(c).wait()

    @pl.when(me == 0)
    def _():
        for c in range(NF):
            tok_local(c).start()

    @pl.when(me > 0)
    def _():
        for c in range(NF):
            tok_copy(c).start()

    turned = [pltpu.make_async_copy(a, b, wt_sem.at[i])
              for i, (a, b) in enumerate(((t1, wqkv_t), (t2, wo_t), (t3, w1_t), (t4, w2_t)))]

    def turn_weights():
        for src, dst in ((wqkv, t1), (wo, t2), (w1, t3), (w2, t4)):
            def block(i, carry, src=src, dst=dst):
                at = pl.ds(pl.multiple_of(i * W, W), W)
                dst[at] = src[:, at].T
                return carry
            lax.fori_loop(0, src.shape[1] // W, block, 0)
        for cp in turned:
            cp.start()

    for k in range(1, ND):
        len_copy(k).start()
    lens[me] = ltile[...]

    @pl.when(me == LAST)
    def _():
        cot_local().start()

    causal[...] = jnp.where(iota(C, C2, 0)
                            <= lax.rem(iota(C, C2, 1), C), 0.0, NEG)

    for cp in weights:
        cp.wait()

    @pl.when(me >= 4)
    def _():
        turn_weights()

    def step(m, c):
        t, slot = m * NF + c, c % 2

        if c == 0:
            @pl.when(m != me)
            def _():
                len_wait(m)

        @pl.when(jnp.logical_and(me == 0, m == 0))
        def _():
            tok_local(c).wait()

        @pl.when(jnp.logical_or(me > 0, m > 0))
        def _():
            pass_copy(t, c).wait_recv()

        @pl.when(m > 0)
        def _():
            out_wait(m - 1, c)

        def reuse(mm):
            for cp in saves(mm, (c - 2) % NF):
                cp.wait()

        if c < 2:
            @pl.when(m > 0)
            def _():
                reuse(m - 1)
        else:
            reuse(m)

        h = hbuf[t].astype(f32)
        a = rms(h, g1[...].astype(f32))
        q = jnp.dot(a, wqkv[:, :D], preferred_element_type=f32)
        kk = jnp.dot(a, wqkv[:, D:2 * D], preferred_element_type=f32).astype(bf16)
        vv = jnp.dot(a, wqkv[:, 2 * D:], preferred_element_type=f32).astype(bf16)
        q = (q * 0.125).astype(bf16)
        own = slice(c * CF, (c + 1) * CF)
        for p in range(NP):
            lanes = slice(p * W, (p + 1) * W)
            for j in range(HALVES):
                rows = slice(j * C, (j + 1) * C)
                st[slot, j, p] = q[rows, lanes]
                st[slot, j, NP + p] = kk[rows, lanes]
                st[slot, j, 2 * NP + p] = vv[rows, lanes]
            k_s[p, own] = kk[:, lanes]
            vt_s[p, :, own] = vv[:, lanes].T
        ln = lens[m][0:1, :]
        key = iota(CF, W, 0) + c * CF
        off = jnp.logical_and(key >= ln[:, :W], iota(CF, W, 1) == 0)
        mask_s[own] = jnp.where(off, NEG, 0.0).astype(bf16)

        half = iota(W, C, 0) < 64
        one = jnp.where(iota(W, C2, 0) == 0, 1.0, 0.0).astype(bf16)

        def attend(j):
            i = c * HALVES + j
            nk = (i + 1) * C

            def scores(p):
                qt = q[j * C:(j + 1) * C, p * W:(p + 1) * W].T
                zero = jnp.zeros_like(qt)
                qt = jnp.concatenate([jnp.where(half, qt, zero), jnp.where(half, zero, qt)], axis=1)
                qt = jnp.concatenate([qt, one], axis=0)
                top = None
                for b in range(i + 1):
                    ks = slice(b * C, (b + 1) * C)
                    s = jnp.dot(jnp.concatenate([k_s[p, ks], mask_s[ks]], axis=1), qt, preferred_element_type=f32)
                    if b == i:
                        s = s + causal[...]
                    mb = jnp.max(s.reshape(C // 8, 8, C2), axis=0)
                    top = mb if top is None else jnp.maximum(top, mb)
                    e_s[p, ks] = s
                return jnp.max(top, axis=0, keepdims=True)

            def exps(p, top):
                total = None
                top2 = top * LOG2E
                for b in range(i + 1):
                    ks = slice(b * C, (b + 1) * C)
                    e = jnp.exp2(e_s[p, ks] * LOG2E - top2)
                    sb = jnp.sum(e.reshape(C // 8, 8, C2), axis=0)
                    total = sb if total is None else total + sb
                    p_s[p, ks] = e.astype(bf16)
                total = row_sum(total)
                here = (lax.rem(iota(1, C2, 1), C) + i * C) < ln
                lse_s[slot, j, p:p + 1] = jnp.where(here, top + jnp.log(total), BIG)
                return 1.0 / total

            def context(p, inv):
                o = jnp.dot(vt_s[p, :, 0:nk], p_s[p, 0:nk], preferred_element_type=f32) * inv
                own = slice(j * C, (j + 1) * C)
                ct_s[p, 0:64, own] = o[0:64, 0:C].astype(bf16)
                ct_s[p, 64:, own] = o[64:, C:].astype(bf16)

            tops = [scores(p) for p in range(NP)]
            invs = [exps(p, tops[p]) for p in range(NP)]
            for p in range(NP):
                context(p, invs[p])

        for j in range(HALVES):
            attend(j)
        cx = jnp.concatenate([ct_s[p].T for p in range(NP)], axis=1)
        cx_s[slot] = cx
        u = (h + jnp.dot(cx, wo[...], preferred_element_type=f32)).astype(bf16)
        u_s[slot] = u
        u = u.astype(f32)
        a2 = rms(u, g2[...].astype(f32))
        z = gelu(jnp.dot(a2, w1[...], preferred_element_type=f32)).astype(bf16)
        o_s[c] = (u + jnp.dot(z, w2[...], preferred_element_type=f32)).astype(bf16)
        for cp in saves(m, c):
            cp.start()

        @pl.when(me < LAST)
        def _():
            pass_copy(t, c).start()
            piece = S // (ND * NF)
            cot_copy(me, pl.multiple_of(t * piece, piece), piece).start()

        @pl.when(me == LAST)
        def _():
            @pl.when(m < LAST)
            def _():
                y_copy(m, c).start()

            @pl.when(m == LAST)
            def _():
                y_local(c).start()

    def seq(m, carry):
        for c in range(NF):
            step(m, c)
        return carry

    lax.fori_loop(0, ND, seq, 0)

    @pl.when(me < 4)
    def _():
        turn_weights()

    for cp in turned:
        cp.wait()
    for m in range(ND):
        lens_o[m:m + 1] = lens[m][0:1, :W]
    for c in (NF - 2, NF - 1):
        for cp in saves(LAST, c):
            cp.wait()
    for c in range(NF):
        out_wait(LAST, c)
    for k in range(1, ND):
        len_copy(k).wait_send()

    @pl.when(me > 0)
    def _():
        for c in range(NF):
            tok_copy(c).wait_send()

    @pl.when(me < LAST)
    def _():
        cot_copy(me, 0, S).wait_send()
        for c in range(NF):
            y_copy(0, c).wait_recv()

    @pl.when(me == LAST)
    def _():
        cot_local().wait()
        for m in range(LAST):
            cot_copy(m, 0, S).wait_recv()


def forward(tok, cot, own_len, wqkv, wo, w1, w2, g1, g2):
    V = pl.BlockSpec(memory_space=pltpu.VMEM)
    A = pl.BlockSpec(memory_space=pltpu.HBM)
    dma = pltpu.SemaphoreType.DMA
    sd = jax.ShapeDtypeStruct
    return pl.pallas_call(
        fwd_kernel,
        out_shape=(sd((S, D), bf16), sd((ND, S, D), bf16), sd((ND, W), jnp.int32),
                   sd((ND * NF, HALVES, 3 * NP, C, W), bf16), sd((ND * NF, CF, D), bf16), sd((ND * NF, CF, D), bf16),
                   sd((ND * NF, CF, D), bf16), sd((ND * NF, HALVES, 2 * NP, C2), f32), sd((3 * D, D), bf16), sd((D, D), bf16), sd((F, D), bf16), sd((D, F), bf16)),
        in_specs=[A, V, pl.BlockSpec(memory_space=pltpu.SMEM)] + [A] * 4 + [V] * 2,
        out_specs=(A, A, V) + (A,) * 9,
        scratch_shapes=[
            pltpu.VMEM((ND * NF, CF, D), bf16), pltpu.VMEM((2, HALVES, 3 * NP, C, W), bf16), pltpu.VMEM((2, CF, D), bf16),
            pltpu.VMEM((2, CF, D), bf16), pltpu.VMEM((NF, CF, D), bf16), pltpu.VMEM((2, HALVES, 2 * NP, C2), f32),
            pltpu.VMEM((NP, S, W), bf16), pltpu.VMEM((NP, W, S), bf16), pltpu.VMEM((NP, W, CF), bf16),
            pltpu.VMEM((S, W), bf16), pltpu.VMEM((C, C2), f32), pltpu.VMEM((NP, S, C2), f32), pltpu.VMEM((NP, S, C2), bf16),
            pltpu.VMEM((3 * D, D), bf16), pltpu.VMEM((D, D), bf16), pltpu.VMEM((F, D), bf16), pltpu.VMEM((D, F), bf16),
            pltpu.VMEM((D, 3 * D), bf16), pltpu.VMEM((D, D), bf16), pltpu.VMEM((D, F), bf16), pltpu.VMEM((F, D), bf16),
            pltpu.VMEM((ND, C2), jnp.int32), pltpu.VMEM((ND, ND, C2), jnp.int32),
            dma((ND * NF,)), dma((NF,)), dma((NF,)), dma((ND - 1,)), dma((ND,)), dma((1,)), dma((ND,)), dma((NF,)),
            dma((2, 5)), dma((NF,)), dma((4,)), dma((4,))],
        compiler_params=params(56, collective_id=0, has_side_effects=True),
        cost_estimate=cost(80, 100),
    )(tok, cot, own_len, wqkv, wo, w1, w2, g1, g2)

TN = (((0,), (0,)), ((), ()))
OUT = 4


def bwd_kernel(sizes, un, cot_all, sv_qkv, sv_h, sv_u, sv_lse, wqkv_h, wo_h, w1_h, w1t_h, w2_h, g1, g2,
               z_o, dpre_o, d16_o, a2_o, a_o, dmid_o, dqkv_o, gg1_o, gg2_o,
               dbuf, cbuf, qkv_b, h_b, u_b, lse_b, kt_s, dk_s, dv_s,
               z_s, dpre_s, d16_s, a2_s, a_s, dmid_s, dqkv_s, o_s, qm_s, qt_s, dm_s, dt_s, p_s, dp_s, dsum_s, dqt_s, sh_s, r1_s,
               w2_t, w1, w1_t, wo_t, wqkv_t, recv_sem, send_sem, ld_sem, st_sem, w_sem):
    me = lax.axis_index('stage')
    weights = [pltpu.make_async_copy(a, b, w_sem.at[i]) for i, (a, b) in enumerate(
        ((w2_h, w2_t), (w1_h, w1), (w1t_h, w1_t), (wo_h, wo_t), (wqkv_h, wqkv_t)))]
    for cp in weights:
        cp.start()
    barrier = pltpu.get_barrier_semaphore()
    pl.semaphore_signal(barrier, inc=1, device_id=(lax.rem(me + 1, ND),), device_id_type=MESH)
    pl.semaphore_wait(barrier, 1)
    starts = [sum(sizes[:i]) for i in range(len(sizes))]
    total = sum(sizes)

    def loads(r, par):
        dst, src = pl.ds(0, sizes[r]), pl.ds(starts[r], sizes[r])
        pairs = [(sv_qkv, qkv_b), (sv_h, h_b), (sv_u, u_b), (sv_lse, lse_b), (cot_all, cbuf)]
        return [pltpu.make_async_copy(a.at[src], b.at[par, dst], ld_sem.at[par, i]) for i, (a, b) in enumerate(pairs)]

    def stores(row, slot):
        rows = pl.ds(row, C)
        pairs = [(z_s, z_o), (dpre_s, dpre_o), (d16_s, d16_o), (a2_s, a2_o), (a_s, a_o), (dmid_s, dmid_o), (dqkv_s, dqkv_o)]
        return [pltpu.make_async_copy(s.at[slot], o.at[rows], st_sem.at[slot, i]) for i, (s, o) in enumerate(pairs)]

    def send(t, slot):
        return pltpu.make_async_remote_copy(
            src_ref=o_s.at[slot], dst_ref=dbuf.at[t], send_sem=send_sem.at[slot], recv_sem=recv_sem.at[t],
            device_id=(lax.rem(me + ND - 1, ND),), device_id_type=MESH)

    for cp in loads(0, 0):
        cp.start()
    gg1_o[...] = jnp.zeros_like(gg1_o)
    gg2_o[...] = jnp.zeros_like(gg2_o)
    dk_s[...] = jnp.zeros_like(dk_s)
    dv_s[...] = jnp.zeros_like(dv_s)
    causal = iota(C, C2, 0) <= lax.rem(iota(C, C2, 1), C)
    lane = iota(C, W, 1) < 64

    def stack(x):
        zero = jnp.zeros_like(x)
        return jnp.concatenate([jnp.where(lane, x, zero), jnp.where(lane, zero, x)], axis=0)

    def step(t, carry):
        r, n, first = 0, sizes[0], 0
        for i in range(1, len(sizes)):
            past = (t + 1024 - starts[i]) // 1024
            r = r + past
            n = n + past * (sizes[i] - sizes[i - 1])
            first = first + past * (starts[i] - starts[i - 1])
        c = n - 1 - (t - first)
        par, slot, out = lax.rem(r, 2), lax.rem(t, 2), lax.rem(t, OUT)
        row0 = pl.multiple_of((first + c) * C, C)
        rows = pl.ds(pl.multiple_of(c * C, C), C)

        for i in range(len(sizes)):
            @pl.when(t == starts[i])
            def _(i=i):
                for cp in loads(i, i % 2):
                    cp.wait()
                if i + 1 < len(sizes):
                    for cp in loads(i + 1, (i + 1) % 2):
                        cp.start()

        @pl.when(t == first)
        def _():
            def turn(j, carry):
                at = pl.ds(pl.multiple_of(j * C, C), C)
                for p in range(NP):
                    kt_s[p, :, at] = qkv_b[par, j, NP + p].T
                return carry
            lax.fori_loop(0, n, turn, 0)

        @pl.when(t >= 2)
        def _():
            for cp in stores(0, slot):
                cp.wait()

        @pl.when(jnp.logical_and(t >= OUT, me > 0))
        def _():
            send(t, out).wait_send()

        @pl.when(me == LAST)
        def _():
            dbuf[t] = cbuf[par, c].astype(f32)

        @pl.when(me < LAST)
        def _():
            send(t, out).wait_recv()

        d = dbuf[t]
        d16 = d.astype(bf16)
        d16_s[slot] = d16
        u = u_b[par, c].astype(f32)
        gm2 = g2[...].astype(f32)
        r2 = lax.rsqrt(row_mean(u * u) + EPS)
        su = u * r2
        a2 = (su * gm2).astype(bf16)
        a2_s[slot] = a2
        FB = 256

        def ups(fb):
            cols = slice(fb * FB, (fb + 1) * FB)
            dz = jnp.dot(d16, w2_t[:, cols], preferred_element_type=f32)
            return jnp.dot(a2, w1[:, cols], preferred_element_type=f32), dz

        ahead = [ups(0)]
        for fb in range(F // FB):
            cols = slice(fb * FB, (fb + 1) * FB)
            if fb + 1 < F // FB:
                ahead.append(ups(fb + 1))
            x, dz = ahead[fb]
            x2 = x * x
            sg = 0.5 + 0.5 * jnp.tanh(x * (K0 + K1 * x2))
            zz = x * sg
            z_s[slot, :, cols] = zz.astype(bf16)
            gp = sg + (zz - zz * sg) * (2.0 * K0 + 6.0 * K1 * x2)
            dpre_s[slot, :, cols] = (dz * gp).astype(bf16)
        da2 = jnp.dot(dpre_s[slot], w1_t[...], preferred_element_type=f32)
        for p in range(NP):
            qm = stack(qkv_b[par, c, p])
            qm_s[p] = qm
            qt_s[p] = qm.T
        h = h_b[par, c].astype(f32)
        gm1 = g1[...].astype(f32)
        r1 = lax.rsqrt(row_mean(h * h) + EPS)
        sh = h * r1
        sh_s[...] = sh
        r1_s[...] = jnp.broadcast_to(r1, (C, W))
        a_s[slot] = (sh * gm1).astype(bf16)
        gg2_o[...] += jnp.sum((da2 * su).reshape(C // 8, 8, D), axis=0)
        gd = da2 * gm2
        dmid = d + r2 * (gd - su * row_mean(gd * su))
        dmid16 = dmid.astype(bf16)
        dmid_s[slot] = dmid16
        o_s[out] = dmid
        dc = jnp.dot(dmid16, wo_t[...], preferred_element_type=f32).astype(bf16)
        for p in range(NP):
            dm = stack(dc[:, p * W:(p + 1) * W])
            dm_s[p] = dm
            dt_s[p] = dm.T
        dsum_s[...] = jnp.zeros_like(dsum_s)
        dqt_s[...] = jnp.zeros_like(dqt_s)

        def scores(b, diagonal):
            for p in range(NP):
                s = jnp.dot(qkv_b[par, b, NP + p], qt_s[p], preferred_element_type=f32) * LOG2E - lse_b[par, c, p:p + 1] * LOG2E
                if diagonal:
                    s = jnp.where(causal, s, NEG)
                pr = jnp.exp2(s)
                dp = jnp.dot(qkv_b[par, b, 2 * NP + p], dt_s[p], preferred_element_type=f32)
                dsum_s[p] += jnp.sum((pr * dp).reshape(C // 8, 8, C2), axis=0)
                p_s[b, p] = pr
                dp_s[b, p] = dp

        def grads(b):
            ks = pl.ds(pl.multiple_of(b * C, C), C)
            for p in range(NP):
                pr = p_s[b, p]
                ds = (pr * (dp_s[b, p] - row_sum(dsum_s[p]))).astype(bf16)
                dv_s[p, ks] += jnp.dot(pr.astype(bf16), dm_s[p], preferred_element_type=f32)
                dk_s[p, ks] += jnp.dot(ds, qm_s[p], preferred_element_type=f32)
                dqt = jnp.dot(kt_s[p, :, ks], ds, preferred_element_type=f32)
                dqt_s[p, 0:64] += dqt[0:64, 0:C]
                dqt_s[p, 64:W] += dqt[64:W, C:C2]

        def group(what):
            def run(b, carry):
                for i in range(un):
                    what(un * b + i)
                return carry
            lax.fori_loop(0, c // un, run, 0)

        def rest(k):
            def run():
                for i in range(k):
                    scores(c - k + i, False)
                scores(c, True)
                grads(c)
                for i in range(k):
                    grads(c - k + i)
            return run

        group(lambda b: scores(b, False))
        for k in range(un):
            pl.when(lax.rem(c, un) == k)(rest(k))
        group(grads)

        for p in range(NP):
            for i, val in enumerate((dqt_s[p].T * 0.125, dk_s[p, rows], dv_s[p, rows])):
                dqkv_s[slot, :, i * D + p * W:i * D + (p + 1) * W] = val.astype(bf16)
            dk_s[p, rows] = jnp.zeros((C, W), f32)
            dv_s[p, rows] = jnp.zeros((C, W), f32)
        da = jnp.dot(dqkv_s[slot], wqkv_t[...], preferred_element_type=f32)
        gm1 = g1[...].astype(f32)
        sh, r1 = sh_s[...], r1_s[:, 0:1]
        gg1_o[...] += jnp.sum((da * sh).reshape(C // 8, 8, D), axis=0)
        gd = da * gm1
        o_s[out] += r1 * (gd - sh * row_mean(gd * sh))
        for cp in stores(row0, slot):
            cp.start()

        @pl.when(me > 0)
        def _():
            send(t, out).start()
        return carry

    for cp in weights:
        cp.wait()
    lax.fori_loop(0, total, step, 0)
    for t in (total - 2, total - 1):
        for cp in stores(0, t % 2):
            cp.wait()

    @pl.when(me > 0)
    def _():
        for t in range(total - OUT, total):
            send(t, t % OUT).wait_send()


def backward(sizes, un, cid, cot_all, sv_qkv, sv_h, sv_u, sv_lse, wqkv_t, wo_t, w1, w1_t, w2_t, g1, g2):
    V = pl.BlockSpec(memory_space=pltpu.VMEM)
    A = pl.BlockSpec(memory_space=pltpu.HBM)
    dma = pltpu.SemaphoreType.DMA
    sd = jax.ShapeDtypeStruct
    T = sum(sizes)
    R = NT_ALL * C
    VM = pltpu.VMEM
    return pl.pallas_call(
        functools.partial(bwd_kernel, sizes, un),
        out_shape=(sd((R, F), bf16), sd((R, F), bf16), sd((R, D), bf16), sd((R, D), bf16), sd((R, D), bf16), sd((R, D), bf16),
                   sd((R, 3 * D), bf16), sd((8, D), f32), sd((8, D), f32)),
        in_specs=[A] * 10 + [V] * 2,
        out_specs=(A,) * 7 + (V, V),
        scratch_shapes=[
            VM((T, C, D), f32), VM((2, NC, C, D), bf16), VM((2, NC, 3 * NP, C, W), bf16), VM((2, NC, C, D), bf16), VM((2, NC, C, D), bf16),
            VM((2, NC, 2 * NP, C2), f32), VM((NP, W, S), bf16), VM((NP, S, W), f32), VM((NP, S, W), f32),
            VM((2, C, F), bf16), VM((2, C, F), bf16), VM((2, C, D), bf16), VM((2, C, D), bf16), VM((2, C, D), bf16),
            VM((2, C, D), bf16), VM((2, C, 3 * D), bf16), VM((OUT, C, D), f32),
            VM((NP, C2, W), bf16), VM((NP, W, C2), bf16), VM((NP, C2, W), bf16), VM((NP, W, C2), bf16),
            VM((NC, NP, C, C2), f32), VM((NC, NP, C, C2), f32), VM((NP, 8, C2), f32), VM((NP, W, C), f32),
            VM((C, D), f32), VM((C, W), f32),
            VM((D, F), bf16), VM((D, F), bf16), VM((F, D), bf16), VM((D, D), bf16), VM((3 * D, D), bf16),
            dma((T,)), dma((OUT,)), dma((2, 5)), dma((2, 7)), dma((5,))],
        compiler_params=params(60, collective_id=cid, has_side_effects=True),
        cost_estimate=cost(60, 100),
    )(cot_all, sv_qkv, sv_h, sv_u, sv_lse, wqkv_t, wo_t, w1, w1_t, w2_t, g1, g2)


def pack_kernel(plans, lens, qkv, h, u, lse, cot, pick_o, src, live, qkv_o, h_o, u_o, lse_o, cot_o,
                qkv_b, h_b, u_b, lse_b, cot_b, order, ld_sem, st_sem):
    for m in range(ND):
        rank = 0
        for k in range(ND):
            longer = lens[k, 0] > lens[m, 0] if k >= m else lens[k, 0] >= lens[m, 0]
            rank = rank + jnp.where(longer, 1, 0)
        order[rank] = m
    largest, *others = sorted(range(len(plans)), key=lambda i: -sum(plans[i]))
    pick = largest
    for i in others:
        fits = True
        for r in range(ND):
            fits = jnp.logical_and(fits, lens[order[r], 0] <= plans[i][r] * C)
        pick = jnp.where(fits, i, pick)
    pick_o[0] = pick
    count = 0
    for r in range(ND):
        n = 0
        for i, plan in enumerate(plans):
            n = n + jnp.where(pick == i, plan[r], 0)

        def put(j, carry, count=count, r=r):
            src[count + j] = order[r] * NC + j
            return carry
        lax.fori_loop(0, n, put, 0)
        count = count + n
    used = 0
    start = 0
    for r in range(ND):
        n = 0
        for i, plan in enumerate(plans):
            n = n + jnp.where(pick == i, plan[r], 0)
        k = (lens[order[r], 0] + C - 1) // C

        def mark(j, carry, used=used, start=start):
            live[used + j] = start + j
            return carry
        lax.fori_loop(0, k, mark, 0)
        used = used + k
        start = start + n
    pick_o[1] = used
    arrays = ((qkv, qkv_b, qkv_o), (h, h_b, h_o), (u, u_b, u_o), (lse, lse_b, lse_o), (cot, cot_b, cot_o))

    def load(t):
        s = lax.rem(t, RING)
        return [pltpu.make_async_copy(a.at[src[t]], b.at[s], ld_sem.at[s, i]) for i, (a, b, _) in enumerate(arrays)]

    def store(t):
        s = lax.rem(t, RING)
        return [pltpu.make_async_copy(b.at[s], o.at[t], st_sem.at[s, i]) for i, (_, b, o) in enumerate(arrays)]

    lag = RING // 2

    def go(t, carry):
        @pl.when(t < count)
        def _():
            @pl.when(t >= RING)
            def _():
                for cp in store(t - RING):
                    cp.wait()
            for cp in load(t):
                cp.start()

        @pl.when(t >= lag)
        def _():
            for cp in load(t - lag):
                cp.wait()
            for cp in store(t - lag):
                cp.start()
        return carry

    lax.fori_loop(0, count + lag, go, 0)

    def drain(t, carry):
        for cp in store(t):
            cp.wait()
        return carry

    lax.fori_loop(jnp.maximum(count - RING, 0), count, drain, 0)


RING = 16


def pack(plans, lens, *arrays):
    A = pl.BlockSpec(memory_space=pltpu.HBM)
    SM = pl.BlockSpec(memory_space=pltpu.SMEM)
    sd = jax.ShapeDtypeStruct
    return pl.pallas_call(
        functools.partial(pack_kernel, plans),
        out_shape=(sd((2,), jnp.int32), sd((NT_ALL,), jnp.int32), sd((NT_ALL,), jnp.int32)) + tuple(sd(a.shape, a.dtype) for a in arrays),
        in_specs=[SM] + [A] * 5,
        out_specs=(SM, SM, SM) + (A,) * 5,
        scratch_shapes=[pltpu.VMEM((RING,) + a.shape[1:], a.dtype) for a in arrays] + [
            pltpu.SMEM((ND,), jnp.int32), pltpu.SemaphoreType.DMA((RING, 5)), pltpu.SemaphoreType.DMA((RING, 5))],
        compiler_params=params(60),
        cost_estimate=cost(1, 50),
    )(lens, *arrays)


def wgrad_kernel(pick, src, live, y, a, cx, a2, z, dqkv, dmid, dpre, d16, gg1, gg2,
                 y_o, g_qkv, g_out, g_up, g_down, g_g1, g_g2,
                 a_b, cx_b, a2_b, z_b, dqkv_b, dmid_b, dpre_b, d16_b, s_qkv, s_out, s_up, s_down, y_b, ld_sem, st_sem, y_sem):
    count = pick[1]
    blocks = (count + WB - 1) // WB
    bufs = ((z, z_b), (d16, d16_b), (a2, a2_b), (dpre, dpre_b), (a, a_b), (dqkv, dqkv_b), (dmid, dmid_b))

    def load(i, j, par):
        t = live[WB * i + j]
        rows = pl.ds(j * C, C)
        cps = [pltpu.make_async_copy(x.at[pl.ds(pl.multiple_of(t * C, C), C)], b.at[par, rows], ld_sem.at[par, j, k])
               for k, (x, b) in enumerate(bufs)]
        return cps + [pltpu.make_async_copy(cx.at[src[t]], cx_b.at[par, rows], ld_sem.at[par, j, len(bufs)])]

    def each(i, par, what):
        for j in range(WB):
            @pl.when(WB * i + j < count)
            def _(j=j):
                for cp in load(i, j, par):
                    what(cp)

    each(0, 0, lambda cp: cp.start())
    y_in, y_out = pltpu.make_async_copy(y, y_b, y_sem.at[0]), pltpu.make_async_copy(y_b, y_o, y_sem.at[1])
    y_in.start()
    g_g1[...] = row_sum(gg1[...])
    g_g2[...] = row_sum(gg2[...])
    work = ((z_b, d16_b, s_down, g_down), (a2_b, dpre_b, s_up, g_up), (a_b, dqkv_b, s_qkv, g_qkv), (cx_b, dmid_b, s_out, g_out))
    for _, _, acc, _ in work:
        acc[...] = jnp.zeros_like(acc)

    def block(i, carry):
        par = lax.rem(i, 2)

        @pl.when(i + 1 < blocks)
        def _():
            each(i + 1, 1 - par, lambda cp: cp.start())
        each(i, par, lambda cp: cp.wait())
        for j in range(1, WB):
            @pl.when(WB * i + j >= count)
            def _(j=j):
                rows = slice(j * C, (j + 1) * C)
                for x, y, _, _ in work:
                    x[par, rows] = jnp.zeros((C, x.shape[2]), bf16)
                    y[par, rows] = jnp.zeros((C, y.shape[2]), bf16)
        for k, (x, y, acc, out) in enumerate(work):
            for m in range(0, acc.shape[0], WM):
                xt = x[par, :, m:m + WM].T
                for n in range(0, acc.shape[1], 512):
                    acc[m:m + WM, n:n + 512] += jnp.dot(xt, y[par, :, n:n + 512], preferred_element_type=f32)

            @pl.when(i + 1 == blocks)
            def _():
                pltpu.make_async_copy(acc, out, st_sem.at[k]).start()
        return carry

    y_in.wait()
    y_out.start()
    lax.fori_loop(0, blocks, block, 0)
    y_out.wait()
    for k, (_, _, acc, out) in enumerate(work):
        pltpu.make_async_copy(acc, out, st_sem.at[k]).wait()


WB = 2
WM = 512


def wgrad(pick, src, live, y, a, cx, a2, z, dqkv, dmid, dpre, d16, gg1, gg2):
    A = pl.BlockSpec(memory_space=pltpu.HBM)
    SM = pl.BlockSpec(memory_space=pltpu.SMEM)
    V = pl.BlockSpec(memory_space=pltpu.VMEM)
    sd = jax.ShapeDtypeStruct
    VM = pltpu.VMEM
    widths = (D, D, D, F, 3 * D, D, F, D)
    shapes = ((D, 3 * D), (D, D), (D, F), (F, D))
    return pl.pallas_call(
        wgrad_kernel,
        out_shape=(sd(y.shape, bf16),) + tuple(sd(s, f32) for s in shapes) + (sd((1, D), f32),) * 2,
        in_specs=[SM] * 3 + [A] * 9 + [V] * 2,
        out_specs=(A,) * 5 + (V, V),
        scratch_shapes=[VM((2, WB * C, w), bf16) for w in widths] + [VM(s, f32) for s in shapes] + [VM(y.shape, bf16),
            pltpu.SemaphoreType.DMA((2, WB, 8)), pltpu.SemaphoreType.DMA((4,)), pltpu.SemaphoreType.DMA((2,))],
        compiler_params=params(60),
        cost_estimate=cost(25, 70),
    )(pick, src, live, y, a, cx, a2, z, dqkv, dmid, dpre, d16, gg1, gg2)


PLANS = ((8, 8, 7, 4, 4, 3, 2, 2), (8, 6, 4, 3, 2, 2, 2, 1), (8, 8, 5, 4, 3, 2, 2, 1), (8, 8, 8, 7, 5, 4, 3, 2), (NC,) * ND)
GROUPS = (4, 4, 4, 2, 1)


def solution(mesh):
    def per_device(tokens, seq_lens, cot, wqkv, wo, w1, w2, g1, g2):
        wqkv, wo, w1, w2 = wqkv[0], wo[0], w1[0], w2[0]
        y, cot_all, lens, qkv, h, cx, u, lse, wqkv_t, wo_t, w1_t, w2_t = forward(tokens[0], cot[0], seq_lens, wqkv, wo, w1, w2, g1, g2)
        qkv, lse = qkv.reshape(NT_ALL, 3 * NP, C, 128), lse.reshape(NT_ALL, 2 * NP, C2)
        h, cx, u, cot_all = (x.reshape(NT_ALL, C, D) for x in (h, cx, u, cot_all))
        pick, src, live, *packed = pack(PLANS, lens, qkv, h, u, lse, cot_all)

        def branch(i):
            def run(qkv, h, u, lse, cot_all, wqkv_t, wo_t, w1, w1_t, w2_t, g1, g2):
                return backward(PLANS[i], GROUPS[i], i + 1, cot_all, qkv, h, u, lse, wqkv_t, wo_t, w1, w1_t, w2_t, g1, g2)
            return run

        z, dpre, d16, a2, a, dmid, dqkv, gg1, gg2 = lax.switch(
            pick[0], [branch(i) for i in range(len(PLANS))], *packed, wqkv_t, wo_t, w1, w1_t, w2_t, g1, g2)
        y, g_qkv, g_out, g_up, g_down, g_g1, g_g2 = wgrad(pick, src, live, y, a, cx, a2, z, dqkv, dmid, dpre, d16, gg1, gg2)
        return y[None], g_qkv[None], g_out[None], g_up[None], g_down[None], g_g1, g_g2

    spec = P('stage')
    return jax.shard_map(per_device, mesh=mesh, in_specs=(spec,) * 9, out_specs=(spec,) * 7, check_vma=False)
```

```python
import functools
import jax
import jax.numpy as jnp
from jax import lax
from jax.experimental import pallas as pl
from jax.experimental.pallas import tpu as pltpu
from jax.sharding import PartitionSpec as P

bf16, f32 = jnp.bfloat16, jnp.float32
EPS = 1e-5
K0 = 0.7978845608028654
K1 = K0 * 0.044715
W = 128
NEG = -1e30
BIG = 1e30
NT = (((1,), (1,)), ((), ()))
MESH = pl.DeviceIdType.MESH
S, D, F, NH = 1024, 512, 2048, 8
C = W
C2 = 2 * C
NC = S // C
NP = 4
KB = W
ND = 8
LAST = ND - 1
NT_ALL = ND * NC
CF = 256
NF = S // CF
HALVES = CF // C
LOG2E = 1.4426950408889634


def row_sum(x):
    return jnp.sum(x, axis=0, keepdims=True)


def cost(gflops, mbytes):
    return pl.CostEstimate(flops=gflops * 10 ** 9, bytes_accessed=mbytes * 10 ** 6, transcendentals=0)


def row_mean(x):
    return jnp.mean(x, axis=-1, keepdims=True)


def params(mib, **kw):
    return pltpu.CompilerParams(vmem_limit_bytes=mib * 2 ** 20, **kw)


def iota(rows, cols, dim):
    return lax.broadcasted_iota(jnp.int32, (rows, cols), dim)


def rms(h, g):
    r = lax.rsqrt(row_mean(h * h) + EPS)
    return (h * r * g).astype(bf16)


def gelu(x):
    return x * (0.5 + 0.5 * jnp.tanh(x * (K0 + K1 * (x * x))))


def fwd_kernel(tok, cot, own_len, wqkv_h, wo_h, w1_h, w2_h, g1, g2,
               y, cot_all, lens_o, sv_qkv, sv_h, sv_cx, sv_u, sv_lse, wqkv_t, wo_t, w1_t, w2_t,
               hbuf, st, cx_s, u_s, o_s, lse_s, k_s, vt_s, ct_s, mask_s, causal, e_s, p_s, t1, t2, t3, t4, wqkv, wo, w1, w2, ltile, lens,
               recv_sem, send_sem, tok_sem, len_ssem, len_rsem, cot_ssem, cot_rsem, y_sem, loc_sem, yl_sem, wt_sem, w_sem):
    me = lax.axis_index('stage')
    weights = [pltpu.make_async_copy(a, b, w_sem.at[i])
               for i, (a, b) in enumerate(((wqkv_h, wqkv), (wo_h, wo), (w1_h, w1), (w2_h, w2)))]
    for cp in weights:
        cp.start()
    ltile[...] = jnp.full(ltile.shape, own_len[0], jnp.int32)

    barrier = pltpu.get_barrier_semaphore()
    for k in range(1, ND):
        pl.semaphore_signal(barrier, inc=1, device_id=(lax.rem(me + k, ND),), device_id_type=MESH)
    pl.semaphore_wait(barrier, ND - 1)

    def tok_copy(c):
        return pltpu.make_async_remote_copy(
            src_ref=tok.at[pl.ds(c * CF, CF)], dst_ref=hbuf.at[me * NF + c], send_sem=tok_sem.at[c],
            recv_sem=recv_sem.at[me * NF + c], device_id=(0,), device_id_type=MESH)

    def tok_local(c):
        return pltpu.make_async_copy(tok.at[pl.ds(c * CF, CF)], hbuf.at[c], recv_sem.at[c])

    def len_copy(k):
        return pltpu.make_async_remote_copy(
            src_ref=ltile, dst_ref=lens.at[me], send_sem=len_ssem.at[k - 1], recv_sem=len_rsem.at[me],
            device_id=(lax.rem(me + k, ND),), device_id_type=MESH)

    def len_wait(m):
        pltpu.make_async_remote_copy(
            src_ref=ltile, dst_ref=lens.at[m], send_sem=len_ssem.at[0], recv_sem=len_rsem.at[m],
            device_id=(0,), device_id_type=MESH).wait_recv()

    def cot_copy(m, at, n):
        rows = pl.ds(at, n)
        return pltpu.make_async_remote_copy(
            src_ref=cot.at[rows], dst_ref=cot_all.at[m, rows], send_sem=cot_ssem.at[0], recv_sem=cot_rsem.at[m],
            device_id=(LAST,), device_id_type=MESH)

    def cot_local():
        return pltpu.make_async_copy(cot, cot_all.at[LAST], cot_ssem.at[0])

    def pass_copy(t, c):
        return pltpu.make_async_remote_copy(
            src_ref=o_s.at[c], dst_ref=hbuf.at[t], send_sem=send_sem.at[c], recv_sem=recv_sem.at[t],
            device_id=(lax.rem(me + 1, ND),), device_id_type=MESH)

    def y_copy(m, c):
        return pltpu.make_async_remote_copy(
            src_ref=o_s.at[c], dst_ref=y.at[pl.ds(c * CF, CF)], send_sem=send_sem.at[c],
            recv_sem=y_sem.at[c], device_id=(m,), device_id_type=MESH)

    def y_local(c):
        return pltpu.make_async_copy(o_s.at[c], y.at[pl.ds(c * CF, CF)], yl_sem.at[c])

    def saves(m, c):
        t, slot = m * NF + c, c % 2
        return [
            pltpu.make_async_copy(st.at[slot], sv_qkv.at[t], loc_sem.at[slot, 0]),
            pltpu.make_async_copy(hbuf.at[t], sv_h.at[t], loc_sem.at[slot, 1]),
            pltpu.make_async_copy(cx_s.at[slot], sv_cx.at[t], loc_sem.at[slot, 2]),
            pltpu.make_async_copy(u_s.at[slot], sv_u.at[t], loc_sem.at[slot, 3]),
            pltpu.make_async_copy(lse_s.at[slot], sv_lse.at[t], loc_sem.at[slot, 4]),
        ]

    def out_wait(m, c):
        @pl.when(me < LAST)
        def _():
            pass_copy(m * NF + c, c).wait_send()

        @pl.when(me == LAST)
        def _():
            @pl.when(m < LAST)
            def _():
                y_copy(m, c).wait_send()

            @pl.when(m == LAST)
            def _():
                y_local(c).wait()

    @pl.when(me == 0)
    def _():
        for c in range(NF):
            tok_local(c).start()

    @pl.when(me > 0)
    def _():
        for c in range(NF):
            tok_copy(c).start()

    turned = [pltpu.make_async_copy(a, b, wt_sem.at[i])
              for i, (a, b) in enumerate(((t1, wqkv_t), (t2, wo_t), (t3, w1_t), (t4, w2_t)))]

    def turn_weights():
        for src, dst in ((wqkv, t1), (wo, t2), (w1, t3), (w2, t4)):
            def block(i, carry, src=src, dst=dst):
                at = pl.ds(pl.multiple_of(i * W, W), W)
                dst[at] = src[:, at].T
                return carry
            lax.fori_loop(0, src.shape[1] // W, block, 0)
        for cp in turned:
            cp.start()

    for k in range(1, ND):
        len_copy(k).start()
    lens[me] = ltile[...]

    @pl.when(me == LAST)
    def _():
        cot_local().start()

    causal[...] = jnp.where(iota(C, C2, 0)
                            <= lax.rem(iota(C, C2, 1), C), 0.0, NEG)

    for cp in weights:
        cp.wait()

    @pl.when(me >= 4)
    def _():
        turn_weights()

    def step(m, c):
        t, slot = m * NF + c, c % 2

        if c == 0:
            @pl.when(m != me)
            def _():
                len_wait(m)

        @pl.when(jnp.logical_and(me == 0, m == 0))
        def _():
            tok_local(c).wait()

        @pl.when(jnp.logical_or(me > 0, m > 0))
        def _():
            pass_copy(t, c).wait_recv()

        @pl.when(m > 0)
        def _():
            out_wait(m - 1, c)

        def reuse(mm):
            for cp in saves(mm, (c - 2) % NF):
                cp.wait()

        if c < 2:
            @pl.when(m > 0)
            def _():
                reuse(m - 1)
        else:
            reuse(m)

        h = hbuf[t].astype(f32)
        a = rms(h, g1[...].astype(f32))
        q = jnp.dot(a, wqkv[:, :D], preferred_element_type=f32)
        kk = jnp.dot(a, wqkv[:, D:2 * D], preferred_element_type=f32).astype(bf16)
        vv = jnp.dot(a, wqkv[:, 2 * D:], preferred_element_type=f32).astype(bf16)
        q = (q * 0.125).astype(bf16)
        own = slice(c * CF, (c + 1) * CF)
        for p in range(NP):
            lanes = slice(p * W, (p + 1) * W)
            for j in range(HALVES):
                rows = slice(j * C, (j + 1) * C)
                st[slot, j, p] = q[rows, lanes]
                st[slot, j, NP + p] = kk[rows, lanes]
                st[slot, j, 2 * NP + p] = vv[rows, lanes]
            k_s[p, own] = kk[:, lanes]
            vt_s[p, :, own] = vv[:, lanes].T
        ln = lens[m][0:1, :]
        key = iota(CF, W, 0) + c * CF
        off = jnp.logical_and(key >= ln[:, :W], iota(CF, W, 1) == 0)
        mask_s[own] = jnp.where(off, NEG, 0.0).astype(bf16)

        half = iota(W, C, 0) < 64
        one = jnp.where(iota(W, C2, 0) == 0, 1.0, 0.0).astype(bf16)

        def attend(j):
            i = c * HALVES + j
            nk = (i + 1) * C

            def scores(p):
                qt = q[j * C:(j + 1) * C, p * W:(p + 1) * W].T
                zero = jnp.zeros_like(qt)
                qt = jnp.concatenate([jnp.where(half, qt, zero), jnp.where(half, zero, qt)], axis=1)
                qt = jnp.concatenate([qt, one], axis=0)
                top = None
                for b in range(i + 1):
                    ks = slice(b * C, (b + 1) * C)
                    s = jnp.dot(jnp.concatenate([k_s[p, ks], mask_s[ks]], axis=1), qt, preferred_element_type=f32)
                    if b == i:
                        s = s + causal[...]
                    mb = jnp.max(s.reshape(C // 8, 8, C2), axis=0)
                    top = mb if top is None else jnp.maximum(top, mb)
                    e_s[p, ks] = s
                return jnp.max(top, axis=0, keepdims=True)

            def exps(p, top):
                total = None
                top2 = top * LOG2E
                for b in range(i + 1):
                    ks = slice(b * C, (b + 1) * C)
                    e = jnp.exp2(e_s[p, ks] * LOG2E - top2)
                    sb = jnp.sum(e.reshape(C // 8, 8, C2), axis=0)
                    total = sb if total is None else total + sb
                    p_s[p, ks] = e.astype(bf16)
                total = row_sum(total)
                here = (lax.rem(iota(1, C2, 1), C) + i * C) < ln
                lse_s[slot, j, p:p + 1] = jnp.where(here, top + jnp.log(total), BIG)
                return 1.0 / total

            def context(p, inv):
                o = jnp.dot(vt_s[p, :, 0:nk], p_s[p, 0:nk], preferred_element_type=f32) * inv
                own = slice(j * C, (j + 1) * C)
                ct_s[p, 0:64, own] = o[0:64, 0:C].astype(bf16)
                ct_s[p, 64:, own] = o[64:, C:].astype(bf16)

            tops = [scores(p) for p in range(NP)]
            invs = [exps(p, tops[p]) for p in range(NP)]
            for p in range(NP):
                context(p, invs[p])

        for j in range(HALVES):
            attend(j)
        cx = jnp.concatenate([ct_s[p].T for p in range(NP)], axis=1)
        cx_s[slot] = cx
        u = (h + jnp.dot(cx, wo[...], preferred_element_type=f32)).astype(bf16)
        u_s[slot] = u
        u = u.astype(f32)
        a2 = rms(u, g2[...].astype(f32))
        z = gelu(jnp.dot(a2, w1[...], preferred_element_type=f32)).astype(bf16)
        o_s[c] = (u + jnp.dot(z, w2[...], preferred_element_type=f32)).astype(bf16)
        for cp in saves(m, c):
            cp.start()

        @pl.when(me < LAST)
        def _():
            pass_copy(t, c).start()
            piece = S // (ND * NF)
            cot_copy(me, pl.multiple_of(t * piece, piece), piece).start()

        @pl.when(me == LAST)
        def _():
            @pl.when(m < LAST)
            def _():
                y_copy(m, c).start()

            @pl.when(m == LAST)
            def _():
                y_local(c).start()

    def seq(m, carry):
        for c in range(NF):
            step(m, c)
        return carry

    lax.fori_loop(0, ND, seq, 0)

    @pl.when(me < 4)
    def _():
        turn_weights()

    for cp in turned:
        cp.wait()
    for m in range(ND):
        lens_o[m:m + 1] = lens[m][0:1, :W]
    for c in (NF - 2, NF - 1):
        for cp in saves(LAST, c):
            cp.wait()
    for c in range(NF):
        out_wait(LAST, c)
    for k in range(1, ND):
        len_copy(k).wait_send()

    @pl.when(me > 0)
    def _():
        for c in range(NF):
            tok_copy(c).wait_send()

    @pl.when(me < LAST)
    def _():
        cot_copy(me, 0, S).wait_send()
        for c in range(NF):
            y_copy(0, c).wait_recv()

    @pl.when(me == LAST)
    def _():
        cot_local().wait()
        for m in range(LAST):
            cot_copy(m, 0, S).wait_recv()


def forward(tok, cot, own_len, wqkv, wo, w1, w2, g1, g2):
    V = pl.BlockSpec(memory_space=pltpu.VMEM)
    A = pl.BlockSpec(memory_space=pltpu.HBM)
    dma = pltpu.SemaphoreType.DMA
    sd = jax.ShapeDtypeStruct
    return pl.pallas_call(
        fwd_kernel,
        out_shape=(sd((S, D), bf16), sd((ND, S, D), bf16), sd((ND, W), jnp.int32),
                   sd((ND * NF, HALVES, 3 * NP, C, W), bf16), sd((ND * NF, CF, D), bf16), sd((ND * NF, CF, D), bf16),
                   sd((ND * NF, CF, D), bf16), sd((ND * NF, HALVES, 2 * NP, C2), f32), sd((3 * D, D), bf16), sd((D, D), bf16), sd((F, D), bf16), sd((D, F), bf16)),
        in_specs=[A, V, pl.BlockSpec(memory_space=pltpu.SMEM)] + [A] * 4 + [V] * 2,
        out_specs=(A, A, V) + (A,) * 9,
        scratch_shapes=[
            pltpu.VMEM((ND * NF, CF, D), bf16), pltpu.VMEM((2, HALVES, 3 * NP, C, W), bf16), pltpu.VMEM((2, CF, D), bf16),
            pltpu.VMEM((2, CF, D), bf16), pltpu.VMEM((NF, CF, D), bf16), pltpu.VMEM((2, HALVES, 2 * NP, C2), f32),
            pltpu.VMEM((NP, S, W), bf16), pltpu.VMEM((NP, W, S), bf16), pltpu.VMEM((NP, W, CF), bf16),
            pltpu.VMEM((S, W), bf16), pltpu.VMEM((C, C2), f32), pltpu.VMEM((NP, S, C2), f32), pltpu.VMEM((NP, S, C2), bf16),
            pltpu.VMEM((3 * D, D), bf16), pltpu.VMEM((D, D), bf16), pltpu.VMEM((F, D), bf16), pltpu.VMEM((D, F), bf16),
            pltpu.VMEM((D, 3 * D), bf16), pltpu.VMEM((D, D), bf16), pltpu.VMEM((D, F), bf16), pltpu.VMEM((F, D), bf16),
            pltpu.VMEM((ND, C2), jnp.int32), pltpu.VMEM((ND, ND, C2), jnp.int32),
            dma((ND * NF,)), dma((NF,)), dma((NF,)), dma((ND - 1,)), dma((ND,)), dma((1,)), dma((ND,)), dma((NF,)),
            dma((2, 5)), dma((NF,)), dma((4,)), dma((4,))],
        compiler_params=params(56, collective_id=0, has_side_effects=True),
        cost_estimate=cost(80, 100),
    )(tok, cot, own_len, wqkv, wo, w1, w2, g1, g2)

TN = (((0,), (0,)), ((), ()))
OUT = 4


def bwd_kernel(sizes, un, cot_all, sv_qkv, sv_h, sv_u, sv_lse, wqkv_h, wo_h, w1_h, w1t_h, w2_h, g1, g2,
               z_o, dpre_o, d16_o, a2_o, a_o, dmid_o, dqkv_o, gg1_o, gg2_o,
               dbuf, cbuf, qkv_b, h_b, u_b, lse_b, kt_s, dk_s, dv_s,
               z_s, dpre_s, d16_s, a2_s, a_s, dmid_s, dqkv_s, o_s, qm_s, qt_s, dm_s, dt_s, p_s, dp_s, dsum_s, dqt_s, sh_s, r1_s,
               w2_t, w1, w1_t, wo_t, wqkv_t, recv_sem, send_sem, ld_sem, st_sem, w_sem):
    me = lax.axis_index('stage')
    weights = [pltpu.make_async_copy(a, b, w_sem.at[i]) for i, (a, b) in enumerate(
        ((w2_h, w2_t), (w1_h, w1), (w1t_h, w1_t), (wo_h, wo_t), (wqkv_h, wqkv_t)))]
    for cp in weights:
        cp.start()
    barrier = pltpu.get_barrier_semaphore()
    pl.semaphore_signal(barrier, inc=1, device_id=(lax.rem(me + 1, ND),), device_id_type=MESH)
    pl.semaphore_wait(barrier, 1)
    starts = [sum(sizes[:i]) for i in range(len(sizes))]
    total = sum(sizes)

    def loads(r, par):
        dst, src = pl.ds(0, sizes[r]), pl.ds(starts[r], sizes[r])
        pairs = [(sv_qkv, qkv_b), (sv_h, h_b), (sv_u, u_b), (sv_lse, lse_b), (cot_all, cbuf)]
        return [pltpu.make_async_copy(a.at[src], b.at[par, dst], ld_sem.at[par, i]) for i, (a, b) in enumerate(pairs)]

    def stores(row, slot):
        rows = pl.ds(row, C)
        pairs = [(z_s, z_o), (dpre_s, dpre_o), (d16_s, d16_o), (a2_s, a2_o), (a_s, a_o), (dmid_s, dmid_o), (dqkv_s, dqkv_o)]
        return [pltpu.make_async_copy(s.at[slot], o.at[rows], st_sem.at[slot, i]) for i, (s, o) in enumerate(pairs)]

    def send(t, slot):
        return pltpu.make_async_remote_copy(
            src_ref=o_s.at[slot], dst_ref=dbuf.at[t], send_sem=send_sem.at[slot], recv_sem=recv_sem.at[t],
            device_id=(lax.rem(me + ND - 1, ND),), device_id_type=MESH)

    for cp in loads(0, 0):
        cp.start()
    gg1_o[...] = jnp.zeros_like(gg1_o)
    gg2_o[...] = jnp.zeros_like(gg2_o)
    dk_s[...] = jnp.zeros_like(dk_s)
    dv_s[...] = jnp.zeros_like(dv_s)
    causal = iota(C, C2, 0) <= lax.rem(iota(C, C2, 1), C)
    lane = iota(C, W, 1) < 64

    def stack(x):
        zero = jnp.zeros_like(x)
        return jnp.concatenate([jnp.where(lane, x, zero), jnp.where(lane, zero, x)], axis=0)

    def step(t, carry):
        r, n, first = 0, sizes[0], 0
        for i in range(1, len(sizes)):
            past = (t + 1024 - starts[i]) // 1024
            r = r + past
            n = n + past * (sizes[i] - sizes[i - 1])
            first = first + past * (starts[i] - starts[i - 1])
        c = n - 1 - (t - first)
        par, slot, out = lax.rem(r, 2), lax.rem(t, 2), lax.rem(t, OUT)
        row0 = pl.multiple_of((first + c) * C, C)
        rows = pl.ds(pl.multiple_of(c * C, C), C)

        for i in range(len(sizes)):
            @pl.when(t == starts[i])
            def _(i=i):
                for cp in loads(i, i % 2):
                    cp.wait()
                if i + 1 < len(sizes):
                    for cp in loads(i + 1, (i + 1) % 2):
                        cp.start()

        @pl.when(t == first)
        def _():
            def turn(j, carry):
                at = pl.ds(pl.multiple_of(j * C, C), C)
                for p in range(NP):
                    kt_s[p, :, at] = qkv_b[par, j, NP + p].T
                return carry
            lax.fori_loop(0, n, turn, 0)

        @pl.when(t >= 2)
        def _():
            for cp in stores(0, slot):
                cp.wait()

        @pl.when(jnp.logical_and(t >= OUT, me > 0))
        def _():
            send(t, out).wait_send()

        @pl.when(me == LAST)
        def _():
            dbuf[t] = cbuf[par, c].astype(f32)

        @pl.when(me < LAST)
        def _():
            send(t, out).wait_recv()

        d = dbuf[t]
        d16 = d.astype(bf16)
        d16_s[slot] = d16
        u = u_b[par, c].astype(f32)
        gm2 = g2[...].astype(f32)
        r2 = lax.rsqrt(row_mean(u * u) + EPS)
        su = u * r2
        a2 = (su * gm2).astype(bf16)
        a2_s[slot] = a2
        FB = 256

        def ups(fb):
            cols = slice(fb * FB, (fb + 1) * FB)
            dz = jnp.dot(d16, w2_t[:, cols], preferred_element_type=f32)
            return jnp.dot(a2, w1[:, cols], preferred_element_type=f32), dz

        ahead = [ups(0)]
        for fb in range(F // FB):
            cols = slice(fb * FB, (fb + 1) * FB)
            if fb + 1 < F // FB:
                ahead.append(ups(fb + 1))
            x, dz = ahead[fb]
            x2 = x * x
            sg = 0.5 + 0.5 * jnp.tanh(x * (K0 + K1 * x2))
            zz = x * sg
            z_s[slot, :, cols] = zz.astype(bf16)
            gp = sg + (zz - zz * sg) * (2.0 * K0 + 6.0 * K1 * x2)
            dpre_s[slot, :, cols] = (dz * gp).astype(bf16)
        da2 = jnp.dot(dpre_s[slot], w1_t[...], preferred_element_type=f32)
        for p in range(NP):
            qm = stack(qkv_b[par, c, p])
            qm_s[p] = qm
            qt_s[p] = qm.T
        h = h_b[par, c].astype(f32)
        gm1 = g1[...].astype(f32)
        r1 = lax.rsqrt(row_mean(h * h) + EPS)
        sh = h * r1
        sh_s[...] = sh
        r1_s[...] = jnp.broadcast_to(r1, (C, W))
        a_s[slot] = (sh * gm1).astype(bf16)
        gg2_o[...] += jnp.sum((da2 * su).reshape(C // 8, 8, D), axis=0)
        gd = da2 * gm2
        dmid = d + r2 * (gd - su * row_mean(gd * su))
        dmid16 = dmid.astype(bf16)
        dmid_s[slot] = dmid16
        o_s[out] = dmid
        dc = jnp.dot(dmid16, wo_t[...], preferred_element_type=f32).astype(bf16)
        for p in range(NP):
            dm = stack(dc[:, p * W:(p + 1) * W])
            dm_s[p] = dm
            dt_s[p] = dm.T
        dsum_s[...] = jnp.zeros_like(dsum_s)
        dqt_s[...] = jnp.zeros_like(dqt_s)

        def scores(b, diagonal):
            for p in range(NP):
                s = jnp.dot(qkv_b[par, b, NP + p], qt_s[p], preferred_element_type=f32) * LOG2E - lse_b[par, c, p:p + 1] * LOG2E
                if diagonal:
                    s = jnp.where(causal, s, NEG)
                pr = jnp.exp2(s)
                dp = jnp.dot(qkv_b[par, b, 2 * NP + p], dt_s[p], preferred_element_type=f32)
                dsum_s[p] += jnp.sum((pr * dp).reshape(C // 8, 8, C2), axis=0)
                p_s[b, p] = pr
                dp_s[b, p] = dp

        def grads(b):
            ks = pl.ds(pl.multiple_of(b * C, C), C)
            for p in range(NP):
                pr = p_s[b, p]
                ds = (pr * (dp_s[b, p] - row_sum(dsum_s[p]))).astype(bf16)
                dv_s[p, ks] += jnp.dot(pr.astype(bf16), dm_s[p], preferred_element_type=f32)
                dk_s[p, ks] += jnp.dot(ds, qm_s[p], preferred_element_type=f32)
                dqt = jnp.dot(kt_s[p, :, ks], ds, preferred_element_type=f32)
                dqt_s[p, 0:64] += dqt[0:64, 0:C]
                dqt_s[p, 64:W] += dqt[64:W, C:C2]

        def group(what):
            def run(b, carry):
                for i in range(un):
                    what(un * b + i)
                return carry
            lax.fori_loop(0, c // un, run, 0)

        def rest(k):
            def run():
                for i in range(k):
                    scores(c - k + i, False)
                scores(c, True)
                grads(c)
                for i in range(k):
                    grads(c - k + i)
            return run

        group(lambda b: scores(b, False))
        for k in range(un):
            pl.when(lax.rem(c, un) == k)(rest(k))
        group(grads)

        for p in range(NP):
            for i, val in enumerate((dqt_s[p].T * 0.125, dk_s[p, rows], dv_s[p, rows])):
                dqkv_s[slot, :, i * D + p * W:i * D + (p + 1) * W] = val.astype(bf16)
            dk_s[p, rows] = jnp.zeros((C, W), f32)
            dv_s[p, rows] = jnp.zeros((C, W), f32)
        da = jnp.dot(dqkv_s[slot], wqkv_t[...], preferred_element_type=f32)
        gm1 = g1[...].astype(f32)
        sh, r1 = sh_s[...], r1_s[:, 0:1]
        gg1_o[...] += jnp.sum((da * sh).reshape(C // 8, 8, D), axis=0)
        gd = da * gm1
        o_s[out] += r1 * (gd - sh * row_mean(gd * sh))
        for cp in stores(row0, slot):
            cp.start()

        @pl.when(me > 0)
        def _():
            send(t, out).start()
        return carry

    for cp in weights:
        cp.wait()
    lax.fori_loop(0, total, step, 0)
    for t in (total - 2, total - 1):
        for cp in stores(0, t % 2):
            cp.wait()

    @pl.when(me > 0)
    def _():
        for t in range(total - OUT, total):
            send(t, t % OUT).wait_send()


def backward(sizes, un, cid, cot_all, sv_qkv, sv_h, sv_u, sv_lse, wqkv_t, wo_t, w1, w1_t, w2_t, g1, g2):
    V = pl.BlockSpec(memory_space=pltpu.VMEM)
    A = pl.BlockSpec(memory_space=pltpu.HBM)
    dma = pltpu.SemaphoreType.DMA
    sd = jax.ShapeDtypeStruct
    T = sum(sizes)
    R = NT_ALL * C
    VM = pltpu.VMEM
    return pl.pallas_call(
        functools.partial(bwd_kernel, sizes, un),
        out_shape=(sd((R, F), bf16), sd((R, F), bf16), sd((R, D), bf16), sd((R, D), bf16), sd((R, D), bf16), sd((R, D), bf16),
                   sd((R, 3 * D), bf16), sd((8, D), f32), sd((8, D), f32)),
        in_specs=[A] * 10 + [V] * 2,
        out_specs=(A,) * 7 + (V, V),
        scratch_shapes=[
            VM((T, C, D), f32), VM((2, NC, C, D), bf16), VM((2, NC, 3 * NP, C, W), bf16), VM((2, NC, C, D), bf16), VM((2, NC, C, D), bf16),
            VM((2, NC, 2 * NP, C2), f32), VM((NP, W, S), bf16), VM((NP, S, W), f32), VM((NP, S, W), f32),
            VM((2, C, F), bf16), VM((2, C, F), bf16), VM((2, C, D), bf16), VM((2, C, D), bf16), VM((2, C, D), bf16),
            VM((2, C, D), bf16), VM((2, C, 3 * D), bf16), VM((OUT, C, D), f32),
            VM((NP, C2, W), bf16), VM((NP, W, C2), bf16), VM((NP, C2, W), bf16), VM((NP, W, C2), bf16),
            VM((NC, NP, C, C2), f32), VM((NC, NP, C, C2), f32), VM((NP, 8, C2), f32), VM((NP, W, C), f32),
            VM((C, D), f32), VM((C, W), f32),
            VM((D, F), bf16), VM((D, F), bf16), VM((F, D), bf16), VM((D, D), bf16), VM((3 * D, D), bf16),
            dma((T,)), dma((OUT,)), dma((2, 5)), dma((2, 7)), dma((5,))],
        compiler_params=params(60, collective_id=cid, has_side_effects=True),
        cost_estimate=cost(60, 100),
    )(cot_all, sv_qkv, sv_h, sv_u, sv_lse, wqkv_t, wo_t, w1, w1_t, w2_t, g1, g2)


def pack_kernel(plans, lens, qkv, h, u, lse, cot, pick_o, src, live, qkv_o, h_o, u_o, lse_o, cot_o,
                qkv_b, h_b, u_b, lse_b, cot_b, order, ld_sem, st_sem):
    for m in range(ND):
        rank = 0
        for k in range(ND):
            longer = lens[k, 0] > lens[m, 0] if k >= m else lens[k, 0] >= lens[m, 0]
            rank = rank + jnp.where(longer, 1, 0)
        order[rank] = m
    largest, *others = sorted(range(len(plans)), key=lambda i: -sum(plans[i]))
    pick = largest
    for i in others:
        fits = True
        for r in range(ND):
            fits = jnp.logical_and(fits, lens[order[r], 0] <= plans[i][r] * C)
        pick = jnp.where(fits, i, pick)
    pick_o[0] = pick
    count = 0
    for r in range(ND):
        n = 0
        for i, plan in enumerate(plans):
            n = n + jnp.where(pick == i, plan[r], 0)

        def put(j, carry, count=count, r=r):
            src[count + j] = order[r] * NC + j
            return carry
        lax.fori_loop(0, n, put, 0)
        count = count + n
    used = 0
    start = 0
    for r in range(ND):
        n = 0
        for i, plan in enumerate(plans):
            n = n + jnp.where(pick == i, plan[r], 0)
        k = (lens[order[r], 0] + C - 1) // C

        def mark(j, carry, used=used, start=start):
            live[used + j] = start + j
            return carry
        lax.fori_loop(0, k, mark, 0)
        used = used + k
        start = start + n
    pick_o[1] = used
    arrays = ((qkv, qkv_b, qkv_o), (h, h_b, h_o), (u, u_b, u_o), (lse, lse_b, lse_o), (cot, cot_b, cot_o))

    def load(t):
        s = lax.rem(t, RING)
        return [pltpu.make_async_copy(a.at[src[t]], b.at[s], ld_sem.at[s, i]) for i, (a, b, _) in enumerate(arrays)]

    def store(t):
        s = lax.rem(t, RING)
        return [pltpu.make_async_copy(b.at[s], o.at[t], st_sem.at[s, i]) for i, (_, b, o) in enumerate(arrays)]

    lag = RING // 2

    def go(t, carry):
        @pl.when(t < count)
        def _():
            @pl.when(t >= RING)
            def _():
                for cp in store(t - RING):
                    cp.wait()
            for cp in load(t):
                cp.start()

        @pl.when(t >= lag)
        def _():
            for cp in load(t - lag):
                cp.wait()
            for cp in store(t - lag):
                cp.start()
        return carry

    lax.fori_loop(0, count + lag, go, 0)

    def drain(t, carry):
        for cp in store(t):
            cp.wait()
        return carry

    lax.fori_loop(jnp.maximum(count - RING, 0), count, drain, 0)


RING = 16


def pack(plans, lens, *arrays):
    A = pl.BlockSpec(memory_space=pltpu.HBM)
    SM = pl.BlockSpec(memory_space=pltpu.SMEM)
    sd = jax.ShapeDtypeStruct
    return pl.pallas_call(
        functools.partial(pack_kernel, plans),
        out_shape=(sd((2,), jnp.int32), sd((NT_ALL,), jnp.int32), sd((NT_ALL,), jnp.int32)) + tuple(sd(a.shape, a.dtype) for a in arrays),
        in_specs=[SM] + [A] * 5,
        out_specs=(SM, SM, SM) + (A,) * 5,
        scratch_shapes=[pltpu.VMEM((RING,) + a.shape[1:], a.dtype) for a in arrays] + [
            pltpu.SMEM((ND,), jnp.int32), pltpu.SemaphoreType.DMA((RING, 5)), pltpu.SemaphoreType.DMA((RING, 5))],
        compiler_params=params(60),
        cost_estimate=cost(1, 50),
    )(lens, *arrays)


def wgrad_kernel(pick, src, live, y, a, cx, a2, z, dqkv, dmid, dpre, d16, gg1, gg2,
                 y_o, g_qkv, g_out, g_up, g_down, g_g1, g_g2,
                 a_b, cx_b, a2_b, z_b, dqkv_b, dmid_b, dpre_b, d16_b, s_qkv, s_out, s_up, s_down, y_b, ld_sem, st_sem, y_sem):
    count = pick[1]
    blocks = (count + WB - 1) // WB
    bufs = ((z, z_b), (d16, d16_b), (a2, a2_b), (dpre, dpre_b), (a, a_b), (dqkv, dqkv_b), (dmid, dmid_b))

    def load(i, j, par):
        t = live[WB * i + j]
        rows = pl.ds(j * C, C)
        cps = [pltpu.make_async_copy(x.at[pl.ds(pl.multiple_of(t * C, C), C)], b.at[par, rows], ld_sem.at[par, j, k])
               for k, (x, b) in enumerate(bufs)]
        return cps + [pltpu.make_async_copy(cx.at[src[t]], cx_b.at[par, rows], ld_sem.at[par, j, len(bufs)])]

    def each(i, par, what):
        for j in range(WB):
            @pl.when(WB * i + j < count)
            def _(j=j):
                for cp in load(i, j, par):
                    what(cp)

    each(0, 0, lambda cp: cp.start())
    y_in, y_out = pltpu.make_async_copy(y, y_b, y_sem.at[0]), pltpu.make_async_copy(y_b, y_o, y_sem.at[1])
    y_in.start()
    g_g1[...] = row_sum(gg1[...])
    g_g2[...] = row_sum(gg2[...])
    work = ((z_b, d16_b, s_down, g_down), (a2_b, dpre_b, s_up, g_up), (a_b, dqkv_b, s_qkv, g_qkv), (cx_b, dmid_b, s_out, g_out))
    for _, _, acc, _ in work:
        acc[...] = jnp.zeros_like(acc)

    def block(i, carry):
        par = lax.rem(i, 2)

        @pl.when(i + 1 < blocks)
        def _():
            each(i + 1, 1 - par, lambda cp: cp.start())
        each(i, par, lambda cp: cp.wait())
        for j in range(1, WB):
            @pl.when(WB * i + j >= count)
            def _(j=j):
                rows = slice(j * C, (j + 1) * C)
                for x, y, _, _ in work:
                    x[par, rows] = jnp.zeros((C, x.shape[2]), bf16)
                    y[par, rows] = jnp.zeros((C, y.shape[2]), bf16)
        for k, (x, y, acc, out) in enumerate(work):
            for m in range(0, acc.shape[0], WM):
                xt = x[par, :, m:m + WM].T
                for n in range(0, acc.shape[1], 512):
                    acc[m:m + WM, n:n + 512] += jnp.dot(xt, y[par, :, n:n + 512], preferred_element_type=f32)

            @pl.when(i + 1 == blocks)
            def _():
                pltpu.make_async_copy(acc, out, st_sem.at[k]).start()
        return carry

    y_in.wait()
    y_out.start()
    lax.fori_loop(0, blocks, block, 0)
    y_out.wait()
    for k, (_, _, acc, out) in enumerate(work):
        pltpu.make_async_copy(acc, out, st_sem.at[k]).wait()


WB = 2
WM = 512


def wgrad(pick, src, live, y, a, cx, a2, z, dqkv, dmid, dpre, d16, gg1, gg2):
    A = pl.BlockSpec(memory_space=pltpu.HBM)
    SM = pl.BlockSpec(memory_space=pltpu.SMEM)
    V = pl.BlockSpec(memory_space=pltpu.VMEM)
    sd = jax.ShapeDtypeStruct
    VM = pltpu.VMEM
    widths = (D, D, D, F, 3 * D, D, F, D)
    shapes = ((D, 3 * D), (D, D), (D, F), (F, D))
    return pl.pallas_call(
        wgrad_kernel,
        out_shape=(sd(y.shape, bf16),) + tuple(sd(s, f32) for s in shapes) + (sd((1, D), f32),) * 2,
        in_specs=[SM] * 3 + [A] * 9 + [V] * 2,
        out_specs=(A,) * 5 + (V, V),
        scratch_shapes=[VM((2, WB * C, w), bf16) for w in widths] + [VM(s, f32) for s in shapes] + [VM(y.shape, bf16),
            pltpu.SemaphoreType.DMA((2, WB, 8)), pltpu.SemaphoreType.DMA((4,)), pltpu.SemaphoreType.DMA((2,))],
        compiler_params=params(60),
        cost_estimate=cost(25, 70),
    )(pick, src, live, y, a, cx, a2, z, dqkv, dmid, dpre, d16, gg1, gg2)


PLANS = ((8, 8, 7, 4, 4, 3, 2, 2), (8, 6, 4, 3, 2, 2, 2, 1), (8, 8, 5, 4, 3, 2, 2, 1), (8, 8, 8, 7, 6, 4, 4, 2), (NC,) * ND)
GROUPS = (4, 4, 4, 2, 2)


def solution(mesh):
    def per_device(tokens, seq_lens, cot, wqkv, wo, w1, w2, g1, g2):
        wqkv, wo, w1, w2 = wqkv[0], wo[0], w1[0], w2[0]
        y, cot_all, lens, qkv, h, cx, u, lse, wqkv_t, wo_t, w1_t, w2_t = forward(tokens[0], cot[0], seq_lens, wqkv, wo, w1, w2, g1, g2)
        qkv, lse = qkv.reshape(NT_ALL, 3 * NP, C, 128), lse.reshape(NT_ALL, 2 * NP, C2)
        h, cx, u, cot_all = (x.reshape(NT_ALL, C, D) for x in (h, cx, u, cot_all))
        pick, src, live, *packed = pack(PLANS, lens, qkv, h, u, lse, cot_all)

        def branch(i):
            def run(qkv, h, u, lse, cot_all, wqkv_t, wo_t, w1, w1_t, w2_t, g1, g2):
                return backward(PLANS[i], GROUPS[i], i + 1, cot_all, qkv, h, u, lse, wqkv_t, wo_t, w1, w1_t, w2_t, g1, g2)
            return run

        z, dpre, d16, a2, a, dmid, dqkv, gg1, gg2 = lax.switch(
            pick[0], [branch(i) for i in range(len(PLANS))], *packed, wqkv_t, wo_t, w1, w1_t, w2_t, g1, g2)
        y, g_qkv, g_out, g_up, g_down, g_g1, g_g2 = wgrad(pick, src, live, y, a, cx, a2, z, dqkv, dmid, dpre, d16, gg1, gg2)
        return y[None], g_qkv[None], g_out[None], g_up[None], g_down[None], g_g1, g_g2

    spec = P('stage')
    return jax.shard_map(per_device, mesh=mesh, in_specs=(spec,) * 9, out_specs=(spec,) * 7, check_vma=False)
```
